32 devices in a mesh: seq: 16 (over z, y, x), rep: 2 (over core).
Axes of the slice: x: 2, y: 2, z: 4, core: 2. Of those that a mesh axis runs over, the one named last changes fastest.
Arguments:
- q_lin: bfloat16 [2, 2048, 4096], P('rep', 'seq'), may hold values from -90 to 90, as said below
- k_lin: bfloat16 [2, 2048, 512], P('rep', 'seq'), may hold values from -4 to 4
- value_projection: bfloat16 [2, 2048, 512], P('rep', 'seq'), may hold values from -6 to 6
- grad_out: bfloat16 [2, 2048, 4096], P('rep', 'seq'), may hold values from -6 to 6
- q_bias: float32 [4096], replicated, may hold values from -3 to 3
- block_lists: int32 [32, 16, 2], replicated, may hold values from 0 to 15, as said below
- block_counts: int32 [32, 16], replicated, may hold values from 1 to 2, as said below
Outputs:
- dq: bfloat16 [2, 2048, 4096], P('rep', 'seq')
- dk: bfloat16 [2, 2048, 512], P('rep', 'seq')
- dv: bfloat16 [2, 2048, 512], P('rep', 'seq')
- dbq: float32 [4096], replicated
The draws below stay inside these ranges and needn't reach their ends.
Inputs may be any that keep to these rules, and one draw needn't show every extreme that they name: `q_lin`: in the shown and hidden draws alike the entries stay within the stated range. `block_lists`: entry 0 of every list is the query block itself; the 2 entries of a list are distinct; entries past block_counts are ignored. `block_counts`: some head has 2 for every query block.
All inputs are finite; a program needn't handle non-finite values.
Results may differ from the reference program's by a relative error of at most 0.008.
Values may be sent and summed in bfloat16 or wider, within the bound.
A program may use at most 128 MiB of HBM per device.

```python
import jax
import jax.numpy as jnp
from jax import lax

QUERY_HEADS = 32
KEY_VALUE_HEADS = 4
HEAD_WIDTH = 128
BLOCK = 128
SEL = 2
SEQUENCE_LENGTH = 2048
BATCH_COUNT = 2
QBLOCKS = 16
GROUP_SIZE = 8


def query_key_pair(key):
    base = jax.random.fold_in(key, 11)
    key_query, key_random_keys = jax.random.split(base, 2)
    gathered_keys = jnp.clip(jax.random.normal(key_random_keys, (BATCH_COUNT, SEQUENCE_LENGTH, KEY_VALUE_HEADS, HEAD_WIDTH), jnp.float32), -4.0, 4.0)
    query_rows = jnp.clip(jax.random.normal(key_query, (BATCH_COUNT, SEQUENCE_LENGTH, QUERY_HEADS, HEAD_WIDTH), jnp.float32), -4.0, 4.0)
    return (query_rows.reshape(BATCH_COUNT, SEQUENCE_LENGTH, QUERY_HEADS * HEAD_WIDTH), gathered_keys.reshape(BATCH_COUNT, SEQUENCE_LENGTH, KEY_VALUE_HEADS * HEAD_WIDTH))


def draw_q_lin(key, part):
    return query_key_pair(key)[0].astype(jnp.bfloat16)


def draw_k_lin(key, part):
    return query_key_pair(key)[1].astype(jnp.bfloat16)


def mask_tables(key):
    base = jax.random.fold_in(key, 7)
    key_levels, key_heavy, key_shift, key_picks = jax.random.split(base, 4)
    levels = jax.random.randint(key_levels, (QUERY_HEADS,), 1, SEL + 1)
    heavy = jax.random.randint(key_heavy, (), 0, QUERY_HEADS)
    shifts = jax.random.randint(key_shift, (QUERY_HEADS, QBLOCKS), 0, 2)
    counts = jnp.clip(levels[:, None] - shifts, 1, SEL)
    counts = counts.at[heavy].set(SEL)
    row_keys = jax.random.split(key_picks, QUERY_HEADS * QBLOCKS)
    others = jax.vmap(lambda row_key: jax.random.permutation(row_key, QBLOCKS - 1)[:SEL - 1])(row_keys)
    others = others.reshape(QUERY_HEADS, QBLOCKS, SEL - 1)
    own = jnp.broadcast_to(jnp.arange(QBLOCKS, dtype=jnp.int32)[None, :, None], (QUERY_HEADS, QBLOCKS, 1))
    others = (own + 1 + others) % QBLOCKS
    chosen = jnp.concatenate([own, others.astype(jnp.int32)], axis=2)
    return (chosen.astype(jnp.int32), counts.astype(jnp.int32))


def draw_block_lists(key, part):
    return mask_tables(key)[0]


def draw_block_counts(key, part):
    return mask_tables(key)[1]


def block_scale(own_key, extent, shards, low, top_value):
    def one(position, parts):
        draws = jax.random.uniform(jax.random.fold_in(jax.random.fold_in(own_key, 6), position), (parts,), jnp.float32, low / len(shards), top_value / len(shards))
        return jnp.repeat(jnp.exp(draws), extent[position] // parts).reshape((-1,) + (1,) * (len(extent) - position - 1))

    factor_of = one(*shards[0])
    for cut in shards[1:]:
        factor_of = factor_of * one(*cut)
    return factor_of


def normal_values(key, dims, width, most, cuts=(), kind=jnp.bfloat16):
    gain = block_scale(key, dims, cuts, -0.22, 0.18) if cuts else 1.0
    drawn = jax.random.normal(key, dims, jnp.float32) * width * gain
    return jnp.minimum(jnp.maximum(drawn, -most), most).astype(kind)


def setup_inputs(seed: int = 0) -> dict:
    keys = jax.random.split(jax.random.key(seed), 8)
    return {
        "q_lin": draw_q_lin(jax.random.fold_in(keys[7], 71), 0),
        "k_lin": draw_k_lin(jax.random.fold_in(keys[7], 71), 0),
        "value_projection": normal_values(keys[2], (BATCH_COUNT, SEQUENCE_LENGTH, KEY_VALUE_HEADS * HEAD_WIDTH), 1.0, 6.0, ((0, 2), (1, 16))),
        "grad_out": normal_values(keys[3], (BATCH_COUNT, SEQUENCE_LENGTH, QUERY_HEADS * HEAD_WIDTH), 1.0, 6.0, ((0, 2), (1, 16))),
        "q_bias": normal_values(keys[4], (QUERY_HEADS * HEAD_WIDTH,), 0.5, 3.0, (), jnp.float32),
        "block_lists": draw_block_lists(jax.random.fold_in(keys[7], 71), 0),
        "block_counts": draw_block_counts(jax.random.fold_in(keys[7], 71), 0),
    }


def rounded(values_in):
    return lax.optimization_barrier(values_in.astype(jnp.bfloat16)).astype(jnp.float32)


def head_pass(query_rows, key_rows, value_rows, grads, chosen, counts):
    scaling = HEAD_WIDTH ** -0.5
    q_blocks = query_rows.reshape(QBLOCKS, BLOCK, HEAD_WIDTH).astype(jnp.float32)
    key_sel = key_rows.reshape(QBLOCKS, BLOCK, HEAD_WIDTH)[chosen].reshape(QBLOCKS, SEL * BLOCK, HEAD_WIDTH).astype(jnp.float32)
    value_sel = value_rows.reshape(QBLOCKS, BLOCK, HEAD_WIDTH)[chosen].reshape(QBLOCKS, SEL * BLOCK, HEAD_WIDTH).astype(jnp.float32)
    g_blocks = grads.reshape(QBLOCKS, BLOCK, HEAD_WIDTH).astype(jnp.float32)
    active = jnp.repeat(jnp.arange(SEL, dtype=jnp.int32)[None, :] < counts[:, None], BLOCK, axis=1)
    scores = jnp.einsum("qrd,qkd->qrk", q_blocks, key_sel) * scaling
    scores = jnp.where(active[:, None, :], scores, -1.0e30)
    weights = jax.nn.softmax(scores, axis=-1)
    weights_half = rounded(weights)
    attn_out = jnp.einsum("qrk,qkd->qrd", weights_half, value_sel)
    row_dots = jnp.sum(g_blocks * attn_out, axis=-1)
    weight_grads = jnp.einsum("qrd,qkd->qrk", g_blocks, value_sel)
    score_grads = rounded(weights * (weight_grads - row_dots[..., None]))
    grad_q = scaling * jnp.einsum("qrk,qkd->qrd", score_grads, key_sel)
    dk_sel = scaling * jnp.einsum("qrk,qrd->qkd", score_grads, q_blocks)
    dv_sel = jnp.einsum("qrk,qrd->qkd", weights_half, g_blocks)
    empty = jnp.zeros((QBLOCKS, BLOCK, HEAD_WIDTH), jnp.float32)
    key_gradient = empty.at[chosen].add(dk_sel.reshape(QBLOCKS, SEL, BLOCK, HEAD_WIDTH))
    value_gradient = empty.at[chosen].add(dv_sel.reshape(QBLOCKS, SEL, BLOCK, HEAD_WIDTH))
    return grad_q.reshape(SEQUENCE_LENGTH, HEAD_WIDTH), key_gradient.reshape(SEQUENCE_LENGTH, HEAD_WIDTH), value_gradient.reshape(SEQUENCE_LENGTH, HEAD_WIDTH)


def reference(q_lin, k_lin, value_projection, grad_out, q_bias, block_lists, block_counts):
    query_rows = (q_lin.astype(jnp.float32) + q_bias).astype(jnp.bfloat16)
    group_of = jnp.arange(QUERY_HEADS, dtype=jnp.int32) // GROUP_SIZE

    def per_sequence(members):
        q_seq, key_sequence, value_sequence, g_seq = members
        q_heads = jnp.transpose(q_seq.reshape(SEQUENCE_LENGTH, QUERY_HEADS, HEAD_WIDTH), (1, 0, 2))
        g_heads = jnp.transpose(g_seq.reshape(SEQUENCE_LENGTH, QUERY_HEADS, HEAD_WIDTH), (1, 0, 2))
        key_head_rows = jnp.transpose(key_sequence.reshape(SEQUENCE_LENGTH, KEY_VALUE_HEADS, HEAD_WIDTH), (1, 0, 2))
        value_head_rows = jnp.transpose(value_sequence.reshape(SEQUENCE_LENGTH, KEY_VALUE_HEADS, HEAD_WIDTH), (1, 0, 2))

        def per_head(inner):
            q_one, g_one, chosen, counts, group = inner
            key_rows = lax.dynamic_index_in_dim(key_head_rows, group, 0, keepdims=False)
            value_rows = lax.dynamic_index_in_dim(value_head_rows, group, 0, keepdims=False)
            return head_pass(q_one, key_rows, value_rows, g_one, chosen, counts)

        grad_q, key_gradient, value_gradient = lax.map(per_head, (q_heads, g_heads, block_lists, block_counts, group_of))
        bias_part = jnp.sum(grad_q, axis=1)
        dq_seq = jnp.transpose(grad_q, (1, 0, 2)).reshape(SEQUENCE_LENGTH, QUERY_HEADS * HEAD_WIDTH).astype(jnp.bfloat16)
        key_gradient_sequence = jnp.sum(key_gradient.reshape(KEY_VALUE_HEADS, GROUP_SIZE, SEQUENCE_LENGTH, HEAD_WIDTH), axis=1)
        value_gradient_sequence = jnp.sum(value_gradient.reshape(KEY_VALUE_HEADS, GROUP_SIZE, SEQUENCE_LENGTH, HEAD_WIDTH), axis=1)
        key_gradient_sequence = jnp.transpose(key_gradient_sequence, (1, 0, 2)).reshape(SEQUENCE_LENGTH, KEY_VALUE_HEADS * HEAD_WIDTH).astype(jnp.bfloat16)
        value_gradient_sequence = jnp.transpose(value_gradient_sequence, (1, 0, 2)).reshape(SEQUENCE_LENGTH, KEY_VALUE_HEADS * HEAD_WIDTH).astype(jnp.bfloat16)
        return dq_seq, key_gradient_sequence, value_gradient_sequence, bias_part

    dq, dk, dv, bias_parts = lax.map(per_sequence, (query_rows, k_lin, value_projection, grad_out))
    return dq, dk, dv, jnp.sum(bias_parts, axis=0).reshape(QUERY_HEADS * HEAD_WIDTH)
```

```python
import functools

import jax
import jax.numpy as jnp
from jax import lax
from jax.experimental import pallas as pl
from jax.experimental.pallas import tpu as pltpu
from jax.sharding import PartitionSpec as P

NT = (((1,), (1,)), ((), ()))
TN = (((0,), (0,)), ((), ()))
NN = (((1,), (0,)), ((), ()))
MESH = pl.DeviceIdType.MESH
PLANE = 4
UNROLL = 4


def dot(a, b, dims):
    return lax.dot_general(a, b, dims, preferred_element_type=jnp.float32)


def fused_kernel(
    group, scaling,
    lists_ref, count_ref, bias_ref, q_ref, g_ref, k_ref, v_ref,
    dq_ref, dk_ref, dv_ref, dbq_ref,
    kall, vall, qbuf, gbuf, dqbuf, weights_buf, chain_k, chain_v, own_k, own_v,
    rs_send, rs_recv, final, bias_acc, rep_slots, z_slots, bias_sums,
    enc_ref, prev_ref, last_ref,
    local_sem, plane_send, plane_recv, rows_send, rows_recv, z_send, z_recv,
    dq_local, dq_send, dq_recv, rs_send_sem, rs_recv_sem,
    out_local, out_send, out_recv, rep_send, rep_recv, zb_send, zb_recv, pb_send, pb_recv,
):
    me = lax.axis_index("seq")
    n = lax.axis_size("seq")
    reps, rep = lax.axis_size("rep"), lax.axis_index("rep")
    lines = n // PLANE
    z, p = me // PLANE, me % PLANE
    rows, width = kall.shape[1:]
    halves = group // UNROLL
    steps = PLANE * halves
    piece = UNROLL * width
    pairs = PLANE * group

    def near(s):
        return (p // 2 + s // 2) % 2 * 2 + (p % 2 + s % 2) % 2

    def seq(zz, pp):
        return {"seq": zz * PLANE + pp}

    def remote(src, dst, send, recv, target):
        return pltpu.make_async_remote_copy(
            src_ref=src, dst_ref=dst, send_sem=send, recv_sem=recv,
            device_id=target, device_id_type=MESH,
        )

    def cols(start, size):
        return pl.ds(pl.multiple_of(start * width, width), size * width)

    own_kv = [
        pltpu.make_async_copy(src.at[:, cols(p, 1)], dst.at[me], local_sem.at[a])
        for a, (src, dst) in enumerate([(k_ref, kall), (v_ref, vall)])
    ]
    own_rows = [
        pltpu.make_async_copy(
            src.at[:, cols(p * group + hb * UNROLL, UNROLL)], dst.at[hb],
            local_sem.at[2 + a * halves + hb],
        )
        for a, (src, dst) in enumerate([(q_ref, qbuf), (g_ref, gbuf)])
        for hb in range(halves)
    ]
    for copy in own_kv + own_rows:
        copy.start()

    barrier = pltpu.get_barrier_semaphore()
    z_others = [lax.rem(z + d, lines) for d in range(1, lines)]
    rep_others = [lax.rem(rep + d, reps) for d in range(1, reps)]
    for s in range(1, PLANE):
        pl.semaphore_signal(barrier, inc=1, device_id=seq(z, near(s)), device_id_type=MESH)
    for zz in z_others:
        pl.semaphore_signal(barrier, inc=1, device_id=seq(zz, p), device_id_type=MESH)
    for rr in rep_others:
        pl.semaphore_signal(barrier, inc=1, device_id={"rep": rr}, device_id_type=MESH)
    pl.semaphore_wait(barrier, PLANE - 1 + lines - 1 + reps - 1)

    def plane_copy(a, s):
        src, dst = [(k_ref, kall), (v_ref, vall)][a]
        return remote(
            src.at[:, cols(near(s), 1)], dst.at[me],
            plane_send.at[a, s - 1], plane_recv.at[a, s - 1], seq(z, near(s)),
        )

    for a in range(2):
        for s in range(1, PLANE):
            plane_copy(a, s).start()

    def rows_copy(a, it):
        s, hb = it // halves, it % halves
        src, dst = [(q_ref, qbuf), (g_ref, gbuf)][a]
        return remote(
            src.at[:, cols(near(s) * group + hb * UNROLL, UNROLL)], dst.at[it],
            rows_send.at[a, it], rows_recv.at[a, it], seq(z, near(s)),
        )

    for a in range(2):
        for it in range(halves, steps):
            rows_copy(a, it).start()

    def z_copy(a, way, d):
        dst = [kall, vall][a]
        block = dst.at[pl.ds((z - d if way == 0 else z + d) * PLANE, PLANE)]
        return remote(
            block, block, z_send.at[a, way, d], z_recv.at[a, way, d],
            seq(z + 1 if way == 0 else z - 1, p),
        )

    def z_start(a, d):
        @pl.when((z + 1 < lines) & (z - d >= 0))
        def _():
            z_copy(a, 0, d).start()

        @pl.when((z - 1 >= 0) & (z + d < lines))
        def _():
            z_copy(a, 1, d).start()

    def z_arrive(a, d):
        dst = [kall, vall][a]

        def arrived(way, where):
            block = dst.at[pl.ds(where * PLANE, PLANE)]
            remote(
                block, block, z_send.at[a, way, d - 1], z_recv.at[a, way, d - 1], seq(z, p)
            ).wait_recv()

        @pl.when(z - d >= 0)
        def _():
            arrived(0, z - d)

        @pl.when(z + d < lines)
        def _():
            arrived(1, z + d)

    def z_open(a):
        own_kv[a].wait()
        for s in range(1, PLANE):
            plane_copy(a, s).wait_recv()
        z_start(a, 0)

    def z_relay(a, d):
        z_arrive(a, d)
        if d < lines - 1:
            z_start(a, d)

    def read_table(t, _):
        s, h = t // group, t % group
        position = z * PLANE + near(s)
        head = p * group + h
        other = jnp.clip(lists_ref[position, 1, head], 0, n - 1)
        enc_ref[t] = jnp.where(count_ref[position, head] != 1, other, n)
        return 0

    lax.fori_loop(0, pairs, read_table, 0)

    z_open(0)

    def link_pair(t, _):
        code = enc_ref[t]
        found = jnp.int32(0)
        for u in range(pairs):
            same = (enc_ref[u] == code) & (u < t)
            found = jnp.where(same, u + 1, found)
        prev_ref[t] = found
        return 0

    lax.fori_loop(0, pairs, link_pair, 0)
    z_open(1)

    def link_block(j, _):
        found = jnp.int32(0)
        for u in range(pairs):
            found = jnp.where(enc_ref[u] == j, u + 1, found)
        last_ref[j] = found
        return 0

    lax.fori_loop(0, n, link_block, 0)

    chain_k[0] = jnp.zeros((rows, width), jnp.float32)
    chain_v[0] = jnp.zeros((rows, width), jnp.float32)
    own_k[...] = jnp.zeros_like(own_k)
    own_v[...] = jnp.zeros_like(own_v)
    bias_acc[...] = jnp.zeros_like(bias_acc)

    for d in range(1, lines):
        z_relay(0, d)
    for copy in own_rows:
        copy.wait()

    def both(ref, it, u):
        t = it * UNROLL + u
        code = enc_ref[t]
        other = jnp.where(code < n, code, 0)
        position = z * PLANE + near(it // halves)
        return jnp.concatenate([ref[position], ref[other]], axis=0), code

    def soften(it, _):
        @pl.when(it >= halves)
        def _():
            rows_copy(0, it).wait_recv()

        for u in range(UNROLL):
            lanes = slice(u * width, (u + 1) * width)
            head = p * group + (it % halves) * UNROLL + u
            queries = (
                qbuf[it, :, lanes].astype(jnp.float32) + bias_ref[pl.ds(head, 1), :]
            ).astype(jnp.bfloat16)
            qbuf[it, :, lanes] = queries
            keys, code = both(kall, it, u)
            scores = dot(keys, queries, NT) * scaling
            first = scores[:rows]
            second = scores[rows:] + jnp.where(code < n, 0.0, -1.0e30)
            top = jnp.maximum(
                jnp.max(first, axis=0, keepdims=True), jnp.max(second, axis=0, keepdims=True)
            )
            first, second = jnp.exp(first - top), jnp.exp(second - top)
            total = jnp.sum(first, axis=0, keepdims=True) + jnp.sum(second, axis=0, keepdims=True)
            scale_to = 1.0 / total
            weights_buf[it * UNROLL + u, :rows] = first * scale_to
            weights_buf[it * UNROLL + u, rows:] = second * scale_to
        return 0

    def dq_copy(it):
        s, hb = it // halves, it % halves
        return remote(
            dqbuf.at[it], dq_ref.at[:, cols(p * group + hb * UNROLL, UNROLL)],
            dq_send.at[it], dq_recv.at[it], seq(z, near(s)),
        )

    def dq_stay(it):
        return pltpu.make_async_copy(
            dqbuf.at[it], dq_ref.at[:, cols(p * group + it * UNROLL, UNROLL)], dq_local.at[it]
        )

    def dq_arrive(it):
        s, hb = it // halves, it % halves
        return remote(
            dqbuf.at[it], dq_ref.at[:, cols(near(s) * group + hb * UNROLL, UNROLL)],
            dq_send.at[it], dq_recv.at[it], seq(z, near(s)),
        )

    def differentiate(it, _):
        s = it // halves

        @pl.when(it >= halves)
        def _():
            rows_copy(1, it).wait_recv()

        more_k = more_v = None
        for u in range(UNROLL):
            t = it * UNROLL + u
            lanes = slice(u * width, (u + 1) * width)
            head = (it % halves) * UNROLL + u
            queries, grads = qbuf[it, :, lanes], gbuf[it, :, lanes]
            keys, _ = both(kall, it, u)
            values, _ = both(vall, it, u)
            weights = weights_buf[t]
            half = weights.astype(jnp.bfloat16)
            weight_grads = dot(values, grads, NT)
            row_dots = jnp.sum(half.astype(jnp.float32) * weight_grads, axis=0, keepdims=True)
            score_grads = (weights * (weight_grads - row_dots)).astype(jnp.bfloat16)
            grad_q = scaling * dot(score_grads, keys, TN)
            dqbuf[it, :, lanes] = grad_q.astype(jnp.bfloat16)
            bias_acc[pl.ds(head, 1), :] += jnp.sum(grad_q, axis=0, keepdims=True)
            part_k, part_v = dot(score_grads, queries, NN), dot(half, grads, NN)
            before = prev_ref[t]
            chain_k[t + 1] = part_k[rows:] + chain_k[before]
            chain_v[t + 1] = part_v[rows:] + chain_v[before]
            more_k = part_k[:rows] if more_k is None else more_k + part_k[:rows]
            more_v = part_v[:rows] if more_v is None else more_v + part_v[:rows]
        position = near(s)
        own_k[position] += more_k
        own_v[position] += more_v

        @pl.when(it < halves)
        def _():
            dq_stay(it).start()

        @pl.when(it >= halves)
        def _():
            dq_copy(it).start()

        return 0

    share = [steps * d // lines for d in range(lines + 1)]
    for d in range(lines):
        if d:
            z_relay(1, d)
        lax.fori_loop(share[d], share[d + 1], soften, 0)
    lax.fori_loop(0, steps, differentiate, 0)

    rep_slots[rep] = bias_acc[...]

    def rep_copy(d):
        return remote(
            bias_acc, rep_slots.at[rep], rep_send.at[d - 1], rep_recv.at[d - 1],
            {"rep": rep_others[d - 1]},
        )

    for d in range(1, reps):
        rep_copy(d).start()

    factors = [scaling, 1.0]
    chains = [chain_k, chain_v]
    owns = [own_k, own_v]

    def rs_copy(a, way, d):
        return remote(
            rs_send.at[a, way, d - 1], rs_recv.at[a, way, d - 1],
            rs_send_sem.at[a, way, d - 1], rs_recv_sem.at[a, way, d - 1],
            seq(z + 1 if way == 0 else z - 1, p),
        )

    def rs_step(a, way, d):
        target = z + d if way == 0 else z - d
        inside = target < lines if way == 0 else target >= 0
        inner = z >= 1 if way == 0 else z + 1 < lines

        def part(j):
            return chains[a][last_ref[target * PLANE + j]] * factors[a]

        if d < lines - 1:
            @pl.when(inside & inner)
            def _():
                rs_copy(a, way, d + 1).wait_recv()
                for j in range(PLANE):
                    rs_send[a, way, d - 1, j] = (
                        part(j) + rs_recv[a, way, d, j].astype(jnp.float32)
                    ).astype(jnp.bfloat16)
                rs_copy(a, way, d).start()

            inside = inside & jnp.logical_not(inner)

        @pl.when(inside)
        def _():
            for j in range(PLANE):
                rs_send[a, way, d - 1, j] = part(j).astype(jnp.bfloat16)
            rs_copy(a, way, d).start()

    rs_step(1, 0, lines - 1)
    rs_step(1, 1, lines - 1)

    for d in range(1, reps):
        rep_copy(d).wait_recv()
    summed = rep_slots[0]
    for d in range(1, reps):
        summed = summed + rep_slots[d]
    bias_sums[0] = summed
    z_slots[z] = summed

    def zb_copy(d):
        return remote(
            bias_sums.at[0], z_slots.at[z], zb_send.at[d - 1], zb_recv.at[d - 1],
            seq(z_others[d - 1], p),
        )

    for d in range(1, lines):
        zb_copy(d).start()

    for a in (1, 0):
        for d in range(lines - 1, 0, -1):
            if a == 0 or d < lines - 1:
                rs_step(a, 0, d)
                rs_step(a, 1, d)

    def out_copy(a, s):
        return remote(
            final.at[a, near(s)], [dk_ref, dv_ref][a].at[:, cols(p, 1)],
            out_send.at[a, s - 1], out_recv.at[a, s - 1], seq(z, near(s)),
        )

    def out_arrive(a, s):
        return remote(
            final.at[a, near(s)], [dk_ref, dv_ref][a].at[:, cols(near(s), 1)],
            out_send.at[a, s - 1], out_recv.at[a, s - 1], seq(z, near(s)),
        )

    def out_stay(a):
        return pltpu.make_async_copy(
            final.at[a, p], [dk_ref, dv_ref][a].at[:, cols(p, 1)], out_local.at[a]
        )

    for a in (1, 0):
        base = []
        for j in range(PLANE):
            owns[a][j] = (owns[a][j] + chains[a][last_ref[z * PLANE + j]]) * factors[a]

        for way, inner in ((0, z >= 1), (1, z + 1 < lines)):
            @pl.when(inner)
            def _():
                rs_copy(a, way, 1).wait_recv()
                for j in range(PLANE):
                    owns[a][j] += rs_recv[a, way, 0, j].astype(jnp.float32)

        for j in range(PLANE):
            final[a, j] = owns[a][j].astype(jnp.bfloat16)
        for s in (3, 1, 2):
            out_copy(a, s).start()
        out_stay(a).start()

    for d in range(1, lines):
        zb_copy(d).wait_recv()
    summed = z_slots[0]
    for d in range(1, lines):
        summed = summed + z_slots[d]
    bias_sums[1] = summed
    mine = pl.ds(pl.multiple_of(p * group, group), group)
    dbq_ref[mine, :] = summed

    def pb_copy(s):
        return remote(
            bias_sums.at[1], dbq_ref.at[mine], pb_send.at[s - 1], pb_recv.at[s - 1],
            seq(z, near(s)),
        )

    def pb_arrive(s):
        return remote(
            bias_sums.at[1],
            dbq_ref.at[pl.ds(pl.multiple_of(near(s) * group, group), group)],
            pb_send.at[s - 1], pb_recv.at[s - 1], seq(z, near(s)),
        )

    for s in range(1, PLANE):
        pb_copy(s).start()

    for a in range(2):
        for s in range(1, PLANE):
            plane_copy(a, s).wait_send()
        for it in range(halves, steps):
            rows_copy(a, it).wait_send()
        for way in range(2):
            for d in range(lines - 1):
                ahead = z + 1 < lines if way == 0 else z >= 1
                behind = z - d >= 0 if way == 0 else z + d < lines

                @pl.when(ahead & behind)
                def _():
                    z_copy(a, way, d).wait_send()

            for d in range(1, lines):
                @pl.when(z + d < lines if way == 0 else z - d >= 0)
                def _():
                    rs_copy(a, way, d).wait_send()
    for it in range(halves):
        dq_stay(it).wait()
    for it in range(halves, steps):
        dq_copy(it).wait_send()
        dq_arrive(it).wait_recv()
    for d in range(1, reps):
        rep_copy(d).wait_send()
    for d in range(1, lines):
        zb_copy(d).wait_send()
    for a in range(2):
        out_stay(a).wait()
        for s in range(1, PLANE):
            out_copy(a, s).wait_send()
            out_arrive(a, s).wait_recv()
    for s in range(1, PLANE):
        pb_copy(s).wait_send()
        pb_arrive(s).wait_recv()


def fused(lists, counts, bias, q, g, k, v):
    n, reps = lax.axis_size("seq"), lax.axis_size("rep")
    rows, total = q.shape
    heads, width = bias.shape
    kv_count = k.shape[1] // width
    group = heads // kv_count
    assert n % PLANE == 0 and kv_count == PLANE and group % UNROLL == 0
    lines = n // PLANE
    halves = group // UNROLL
    steps = PLANE * halves
    pairs = PLANE * group
    half, full = jnp.bfloat16, jnp.float32
    smem = pl.BlockSpec(memory_space=pltpu.SMEM)
    vmem = pl.BlockSpec(memory_space=pltpu.VMEM)
    free = pl.BlockSpec(memory_space=pl.ANY)
    dma = pltpu.SemaphoreType.DMA
    return pl.pallas_call(
        functools.partial(fused_kernel, group, width ** (-0.5)),
        in_specs=[smem, smem, vmem, free, free, free, free],
        out_specs=[free, free, free, vmem],
        out_shape=[
            jax.ShapeDtypeStruct(q.shape, half),
            jax.ShapeDtypeStruct(k.shape, half),
            jax.ShapeDtypeStruct(v.shape, half),
            jax.ShapeDtypeStruct(bias.shape, full),
        ],
        scratch_shapes=[
            pltpu.VMEM((n, rows, width), half),
            pltpu.VMEM((n, rows, width), half),
            pltpu.VMEM((steps, rows, UNROLL * width), half),
            pltpu.VMEM((steps, rows, UNROLL * width), half),
            pltpu.VMEM((steps, rows, UNROLL * width), half),
            pltpu.VMEM((pairs, 2 * rows, rows), full),
            pltpu.VMEM((pairs + 1, rows, width), full),
            pltpu.VMEM((pairs + 1, rows, width), full),
            pltpu.VMEM((PLANE, rows, width), full),
            pltpu.VMEM((PLANE, rows, width), full),
            pltpu.VMEM((2, 2, lines - 1, PLANE, rows, width), half),
            pltpu.VMEM((2, 2, lines - 1, PLANE, rows, width), half),
            pltpu.VMEM((2, PLANE, rows, width), half),
            pltpu.VMEM((group, width), full),
            pltpu.VMEM((reps, group, width), full),
            pltpu.VMEM((lines, group, width), full),
            pltpu.VMEM((2, group, width), full),
            pltpu.SMEM((pairs,), jnp.int32),
            pltpu.SMEM((pairs,), jnp.int32),
            pltpu.SMEM((n,), jnp.int32),
            dma((2 + 2 * halves,)),
            dma((2, PLANE - 1)), dma((2, PLANE - 1)),
            dma((2, steps)), dma((2, steps)),
            dma((2, 2, lines - 1)), dma((2, 2, lines - 1)),
            dma((halves,)), dma((steps,)), dma((steps,)),
            dma((2, 2, lines - 1)), dma((2, 2, lines - 1)),
            dma((2,)), dma((2, PLANE - 1)), dma((2, PLANE - 1)),
            dma((reps - 1,)), dma((reps - 1,)),
            dma((lines - 1,)), dma((lines - 1,)),
            dma((PLANE - 1,)), dma((PLANE - 1,)),
        ],
        compiler_params=pltpu.CompilerParams(
            collective_id=1, has_side_effects=True, vmem_limit_bytes=60 * 1024 * 1024
        ),
        name="fused",
    )(lists, counts, bias, q, g, k, v)


def place_kernel(*refs):
    half = len(refs) // 2
    for src, dst in zip(refs[:half], refs[half:]):
        dst[...] = src[...]


def place(*arrays):
    spec = pl.BlockSpec(memory_space=pltpu.VMEM)
    return pl.pallas_call(
        place_kernel,
        in_specs=[spec] * len(arrays),
        out_specs=[spec] * len(arrays),
        out_shape=[jax.ShapeDtypeStruct(one.shape, one.dtype) for one in arrays],
        name="place",
    )(*arrays)


def body(q_lin, k_lin, value_projection, grad_out, q_bias, block_lists, block_counts):
    assert block_lists.shape[1] == lax.axis_size("seq") and block_lists.shape[2] == 2
    heads = block_lists.shape[0]
    dq, dk, dv, dbq = fused(
        jnp.transpose(block_lists, (1, 2, 0)), block_counts.T, q_bias.reshape(heads, -1),
        q_lin[0], grad_out[0], k_lin[0], value_projection[0],
    )
    dq, dk, dv, dbq = place(dq, dk, dv, dbq)
    return (dq[None], dk[None], dv[None], dbq.reshape(-1))


def solution(mesh):
    placed = (P("rep", "seq", None),) * 4 + (P(),) * 3
    return jax.shard_map(
        body,
        mesh=mesh,
        in_specs=placed,
        out_specs=(P("rep", "seq", None),) * 3 + (P(),),
        check_vma=False,
    )
```

```python
import functools

import jax
import jax.numpy as jnp
from jax import lax
from jax.experimental import pallas as pl
from jax.experimental.pallas import tpu as pltpu
from jax.sharding import PartitionSpec as P

NT = (((1,), (1,)), ((), ()))
TN = (((0,), (0,)), ((), ()))
NN = (((1,), (0,)), ((), ()))
MESH = pl.DeviceIdType.MESH
PLANE = 4
UNROLL = 4


def dot(a, b, dims):
    return lax.dot_general(a, b, dims, preferred_element_type=jnp.float32)


def fused_kernel(
    group, scaling,
    lists_ref, count_ref, bias_ref, q_ref, g_ref, k_ref, v_ref,
    dq_ref, dk_ref, dv_ref, dbq_ref,
    lists_smem, count_smem, bias_buf,
    kall, vall, qbuf, gbuf, dqbuf, weights_buf, chain_k, chain_v, own_k, own_v,
    rs_send, rs_recv, final, bias_acc, rep_slots, z_slots, bias_sums,
    enc_ref, prev_ref, last_ref,
    table_sem, local_sem, plane_send, plane_recv, rows_send, rows_recv, z_send, z_recv,
    dq_local, dq_send, dq_recv, rs_send_sem, rs_recv_sem,
    out_local, out_send, out_recv, rep_send, rep_recv, zb_send, zb_recv, pb_send, pb_recv,
):
    me = lax.axis_index("seq")
    n = lax.axis_size("seq")
    reps, rep = lax.axis_size("rep"), lax.axis_index("rep")
    lines = n // PLANE
    z, p = me // PLANE, me % PLANE
    rows, width = kall.shape[1:]
    halves = group // UNROLL
    steps = PLANE * halves
    piece = UNROLL * width
    pairs = PLANE * group

    def near(s):
        return (p // 2 + s // 2) % 2 * 2 + (p % 2 + s % 2) % 2

    def seq(zz, pp):
        return {"seq": zz * PLANE + pp}

    def remote(src, dst, send, recv, target):
        return pltpu.make_async_remote_copy(
            src_ref=src, dst_ref=dst, send_sem=send, recv_sem=recv,
            device_id=target, device_id_type=MESH,
        )

    def cols(start, size):
        return pl.ds(pl.multiple_of(start * width, width), size * width)

    barrier = pltpu.get_barrier_semaphore()
    z_others = [lax.rem(z + d, lines) for d in range(1, lines)]
    rep_others = [lax.rem(rep + d, reps) for d in range(1, reps)]
    for s in range(1, PLANE):
        pl.semaphore_signal(barrier, inc=1, device_id=seq(z, near(s)), device_id_type=MESH)
    for zz in z_others:
        pl.semaphore_signal(barrier, inc=1, device_id=seq(zz, p), device_id_type=MESH)
    for rr in rep_others:
        pl.semaphore_signal(barrier, inc=1, device_id={"rep": rr}, device_id_type=MESH)
    own_kv = [
        pltpu.make_async_copy(src.at[:, cols(p, 1)], dst.at[me], local_sem.at[a])
        for a, (src, dst) in enumerate([(k_ref, kall), (v_ref, vall)])
    ]
    own_rows = [
        pltpu.make_async_copy(
            src.at[:, cols(p * group + hb * UNROLL, UNROLL)], dst.at[hb],
            local_sem.at[2 + a * halves + hb],
        )
        for a, (src, dst) in enumerate([(q_ref, qbuf), (g_ref, gbuf)])
        for hb in range(halves)
    ]
    tables = [
        pltpu.make_async_copy(lists_ref, lists_smem, table_sem.at[0]),
        pltpu.make_async_copy(count_ref, count_smem, table_sem.at[1]),
    ]
    bias_copy = pltpu.make_async_copy(bias_ref, bias_buf, table_sem.at[2])
    for copy in own_kv + tables + own_rows + [bias_copy]:
        copy.start()

    pl.semaphore_wait(barrier, PLANE - 1 + lines - 1 + reps - 1)

    def plane_copy(a, s):
        src, dst = [(k_ref, kall), (v_ref, vall)][a]
        return remote(
            src.at[:, cols(near(s), 1)], dst.at[me],
            plane_send.at[a, s - 1], plane_recv.at[a, s - 1], seq(z, near(s)),
        )

    for a in range(2):
        for s in range(1, PLANE):
            plane_copy(a, s).start()

    def rows_copy(a, it):
        s, hb = it // halves, it % halves
        src, dst = [(q_ref, qbuf), (g_ref, gbuf)][a]
        return remote(
            src.at[:, cols(near(s) * group + hb * UNROLL, UNROLL)], dst.at[it],
            rows_send.at[a, it], rows_recv.at[a, it], seq(z, near(s)),
        )

    for a in range(2):
        for it in range(halves, steps):
            rows_copy(a, it).start()

    def z_block(a, place, s):
        return [kall, vall][a].at[place * PLANE + near(s)]

    def z_copy(a, way, d, s):
        block = z_block(a, z - d if way == 0 else z + d, s)
        return remote(
            block, block, z_send.at[a, way, d, s], z_recv.at[a, way, d, s],
            seq(z + 1 if way == 0 else z - 1, p),
        )

    def goes(way, d):
        if way == 0:
            return (z + 1 < lines) & (z - d >= 0)
        return (z - 1 >= 0) & (z + d < lines)

    def goes_any(way):
        return goes(way, 1)

    def z_start(a, d, s):
        for way in range(2):
            @pl.when(goes(way, d))
            def _():
                z_copy(a, way, d, s).start()

    def z_relay(a, d):
        for s in range(PLANE):
            for way in range(2):
                @pl.when(z - d >= 0 if way == 0 else z + d < lines)
                def _():
                    block = z_block(a, z - d if way == 0 else z + d, s)
                    remote(
                        block, block, z_send.at[a, way, d - 1, s], z_recv.at[a, way, d - 1, s],
                        seq(z, p),
                    ).wait_recv()

            if d < lines - 1:
                z_start(a, d, s)

    own_kv[0].wait()
    z_start(0, 0, 0)

    for copy in tables:
        copy.wait()

    def read_table(t, _):
        position = z * PLANE + near(t // group)
        head = p * group + t % group
        other = jnp.clip(lists_smem[position, 1, head], 0, n - 1)
        enc_ref[t] = jnp.where(count_smem[position, head] != 1, other, n)
        return 0

    lax.fori_loop(0, pairs, read_table, 0)

    def link_pair(t, _):
        code = enc_ref[t]
        found = jnp.int32(0)
        for u in range(pairs):
            same = (enc_ref[u] == code) & (u < t)
            found = jnp.where(same, u + 1, found)
        prev_ref[t] = found
        return 0

    def link_block(j, _):
        found = jnp.int32(0)
        for u in range(pairs):
            found = jnp.where(enc_ref[u] == j, u + 1, found)
        last_ref[j] = found
        return 0

    for s in range(1, PLANE):
        plane_copy(0, s).wait_recv()
        z_start(0, 0, s)
    lax.fori_loop(0, pairs, link_pair, 0)
    own_kv[1].wait()
    for s in range(PLANE):
        if s:
            plane_copy(1, s).wait_recv()
        for way in range(2):
            @pl.when(goes(way, 0) & jnp.logical_not(goes_any(way)))
            def _():
                z_copy(1, way, 0, s).start()

    lax.fori_loop(0, n, link_block, 0)
    chain_k[0] = jnp.zeros((rows, width), jnp.float32)
    chain_v[0] = jnp.zeros((rows, width), jnp.float32)
    own_k[...] = jnp.zeros_like(own_k)
    own_v[...] = jnp.zeros_like(own_v)
    bias_acc[...] = jnp.zeros_like(bias_acc)

    for d in range(1, lines):
        z_relay(0, d)
    for s in range(PLANE):
        for way in range(2):
            @pl.when(goes(way, 0) & goes_any(way))
            def _():
                z_copy(1, way, 0, s).start()

    for copy in own_rows:
        copy.wait()
    bias_copy.wait()

    def both(ref, it, u):
        t = it * UNROLL + u
        code = enc_ref[t]
        other = jnp.where(code < n, code, 0)
        position = z * PLANE + near(it // halves)
        return jnp.concatenate([ref[position], ref[other]], axis=0), code

    def soften(it, _):
        @pl.when(it >= halves)
        def _():
            rows_copy(0, it).wait_recv()

        for u in range(UNROLL):
            lanes = slice(u * width, (u + 1) * width)
            head = p * group + (it % halves) * UNROLL + u
            queries = (
                qbuf[it, :, lanes].astype(jnp.float32) + bias_buf[pl.ds(head, 1), :]
            ).astype(jnp.bfloat16)
            qbuf[it, :, lanes] = queries
            keys, code = both(kall, it, u)
            scores = dot(keys, queries, NT) * scaling
            first = scores[:rows]
            second = scores[rows:] + jnp.where(code < n, 0.0, -1.0e30)
            top = jnp.maximum(
                jnp.max(first, axis=0, keepdims=True), jnp.max(second, axis=0, keepdims=True)
            )
            first, second = jnp.exp(first - top), jnp.exp(second - top)
            total = jnp.sum(first, axis=0, keepdims=True) + jnp.sum(second, axis=0, keepdims=True)
            scale_to = 1.0 / total
            weights_buf[it * UNROLL + u, :rows] = first * scale_to
            weights_buf[it * UNROLL + u, rows:] = second * scale_to
        return 0

    def dq_copy(it):
        s, hb = it // halves, it % halves
        return remote(
            dqbuf.at[it], dq_ref.at[:, cols(p * group + hb * UNROLL, UNROLL)],
            dq_send.at[it], dq_recv.at[it], seq(z, near(s)),
        )

    def dq_stay(it):
        return pltpu.make_async_copy(
            dqbuf.at[it], dq_ref.at[:, cols(p * group + it * UNROLL, UNROLL)], dq_local.at[it]
        )

    def dq_arrive(it):
        s, hb = it // halves, it % halves
        return remote(
            dqbuf.at[it], dq_ref.at[:, cols(near(s) * group + hb * UNROLL, UNROLL)],
            dq_send.at[it], dq_recv.at[it], seq(z, near(s)),
        )

    def differentiate(it, _):
        s = it // halves

        @pl.when(it >= halves)
        def _():
            rows_copy(1, it).wait_recv()

        more_k = more_v = None
        for u in range(UNROLL):
            t = it * UNROLL + u
            lanes = slice(u * width, (u + 1) * width)
            head = (it % halves) * UNROLL + u
            queries, grads = qbuf[it, :, lanes], gbuf[it, :, lanes]
            keys, _ = both(kall, it, u)
            values, _ = both(vall, it, u)
            weights = weights_buf[t]
            half = weights.astype(jnp.bfloat16)
            weight_grads = dot(values, grads, NT)
            row_dots = jnp.sum(half.astype(jnp.float32) * weight_grads, axis=0, keepdims=True)
            score_grads = (weights * (weight_grads - row_dots)).astype(jnp.bfloat16)
            grad_q = scaling * dot(score_grads, keys, TN)
            dqbuf[it, :, lanes] = grad_q.astype(jnp.bfloat16)
            bias_acc[pl.ds(head, 1), :] += jnp.sum(grad_q, axis=0, keepdims=True)
            part_k, part_v = dot(score_grads, queries, NN), dot(half, grads, NN)
            before = prev_ref[t]
            chain_k[t + 1] = part_k[rows:] + chain_k[before]
            chain_v[t + 1] = part_v[rows:] + chain_v[before]
            more_k = part_k[:rows] if more_k is None else more_k + part_k[:rows]
            more_v = part_v[:rows] if more_v is None else more_v + part_v[:rows]
        position = near(s)
        own_k[position] += more_k
        own_v[position] += more_v

        @pl.when(it < halves)
        def _():
            dq_stay(it).start()

        @pl.when(it >= halves)
        def _():
            dq_copy(it).start()

        return 0

    share = [steps * d // lines for d in range(lines + 1)]
    for d in range(lines):
        if d:
            z_relay(1, d)
        lax.fori_loop(share[d], share[d + 1], soften, 0)
    lax.fori_loop(0, steps, differentiate, 0)

    rep_slots[rep] = bias_acc[...]

    def rep_copy(d):
        return remote(
            bias_acc, rep_slots.at[rep], rep_send.at[d - 1], rep_recv.at[d - 1],
            {"rep": rep_others[d - 1]},
        )

    for d in range(1, reps):
        rep_copy(d).start()

    factors = [scaling, 1.0]
    chains = [chain_k, chain_v]
    owns = [own_k, own_v]
    order = [3, 1, 2, 0]

    def rs_copy(a, way, d, s):
        return remote(
            rs_send.at[a, way, d - 1, s], rs_recv.at[a, way, d - 1, s],
            rs_send_sem.at[a, way, d - 1, s], rs_recv_sem.at[a, way, d - 1, s],
            seq(z + 1 if way == 0 else z - 1, p),
        )

    def rs_inner(way):
        return z >= 1 if way == 0 else z + 1 < lines

    def rs_step(a, way, d, s):
        target = z + d if way == 0 else z - d
        inside = target < lines if way == 0 else target >= 0

        def part():
            return chains[a][last_ref[target * PLANE + near(s)]] * factors[a]

        if d < lines - 1:
            @pl.when(inside & rs_inner(way))
            def _():
                rs_copy(a, way, d + 1, s).wait_recv()
                rs_send[a, way, d - 1, s] = (
                    part() + rs_recv[a, way, d, s].astype(jnp.float32)
                ).astype(jnp.bfloat16)
                rs_copy(a, way, d, s).start()

            inside = inside & jnp.logical_not(rs_inner(way))

        @pl.when(inside)
        def _():
            rs_send[a, way, d - 1, s] = part().astype(jnp.bfloat16)
            rs_copy(a, way, d, s).start()

    def out_copy(a, s):
        return remote(
            final.at[a, s], [dk_ref, dv_ref][a].at[:, cols(p, 1)],
            out_send.at[a, s - 1], out_recv.at[a, s - 1], seq(z, near(s)),
        )

    def out_arrive(a, s):
        return remote(
            final.at[a, s], [dk_ref, dv_ref][a].at[:, cols(near(s), 1)],
            out_send.at[a, s - 1], out_recv.at[a, s - 1], seq(z, near(s)),
        )

    def out_stay(a):
        return pltpu.make_async_copy(
            final.at[a, 0], [dk_ref, dv_ref][a].at[:, cols(p, 1)], out_local.at[a]
        )

    def zb_copy(d):
        return remote(
            bias_sums.at[0], z_slots.at[z], zb_send.at[d - 1], zb_recv.at[d - 1],
            seq(z_others[d - 1], p),
        )

    for d in range(lines - 1, 0, -1):
        for a in (1, 0):
            for s in order:
                rs_step(a, 0, d, s)
                rs_step(a, 1, d, s)
        if d == lines - 1:
            for e in range(1, reps):
                rep_copy(e).wait_recv()
            summed = rep_slots[0]
            for e in range(1, reps):
                summed = summed + rep_slots[e]
            bias_sums[0] = summed
            z_slots[z] = summed
            for e in range(1, lines):
                zb_copy(e).start()

    def finish(a, s):
        j = near(s)
        owns[a][j] = (owns[a][j] + chains[a][last_ref[z * PLANE + j]]) * factors[a]
        for way in range(2):
            @pl.when(rs_inner(way))
            def _():
                rs_copy(a, way, 1, s).wait_recv()
                owns[a][j] += rs_recv[a, way, 0, s].astype(jnp.float32)

        final[a, s] = owns[a][j].astype(jnp.bfloat16)
        if s:
            out_copy(a, s).start()
        else:
            out_stay(a).start()

    for s in order:
        finish(1, s)

    for d in range(1, lines):
        zb_copy(d).wait_recv()
    summed = z_slots[0]
    for d in range(1, lines):
        summed = summed + z_slots[d]
    bias_sums[1] = summed

    def bias_rows(chip):
        return dbq_ref.at[pl.ds(pl.multiple_of(chip * group, group), group)]

    bias_stay = pltpu.make_async_copy(bias_sums.at[1], bias_rows(p), table_sem.at[0])
    bias_stay.start()

    def pb_copy(s):
        return remote(
            bias_sums.at[1], bias_rows(p), pb_send.at[s - 1], pb_recv.at[s - 1], seq(z, near(s))
        )

    def pb_arrive(s):
        return remote(
            bias_sums.at[1], bias_rows(near(s)), pb_send.at[s - 1], pb_recv.at[s - 1],
            seq(z, near(s)),
        )

    for s in range(1, PLANE):
        pb_copy(s).start()

    for s in order:
        finish(0, s)

    for a in range(2):
        for s in range(1, PLANE):
            plane_copy(a, s).wait_send()
        for it in range(halves, steps):
            rows_copy(a, it).wait_send()
        for way in range(2):
            for d in range(lines - 1):
                @pl.when(goes(way, d))
                def _():
                    for s in range(PLANE):
                        z_copy(a, way, d, s).wait_send()

            for d in range(1, lines):
                @pl.when(z + d < lines if way == 0 else z - d >= 0)
                def _():
                    for s in range(PLANE):
                        rs_copy(a, way, d, s).wait_send()
    for it in range(halves):
        dq_stay(it).wait()
    for it in range(halves, steps):
        dq_copy(it).wait_send()
        dq_arrive(it).wait_recv()
    for d in range(1, reps):
        rep_copy(d).wait_send()
    for d in range(1, lines):
        zb_copy(d).wait_send()
    for a in range(2):
        out_stay(a).wait()
        for s in range(1, PLANE):
            out_copy(a, s).wait_send()
            out_arrive(a, s).wait_recv()
    bias_stay.wait()
    for s in range(1, PLANE):
        pb_copy(s).wait_send()
        pb_arrive(s).wait_recv()


def fused(lists, counts, bias, q, g, k, v):
    n, reps = lax.axis_size("seq"), lax.axis_size("rep")
    rows, total = q.shape
    heads, width = bias.shape
    kv_count = k.shape[1] // width
    group = heads // kv_count
    assert n % PLANE == 0 and kv_count == PLANE and group % UNROLL == 0
    lines = n // PLANE
    halves = group // UNROLL
    steps = PLANE * halves
    pairs = PLANE * group
    half, full = jnp.bfloat16, jnp.float32
    free = pl.BlockSpec(memory_space=pl.ANY)
    dma = pltpu.SemaphoreType.DMA
    block = rows * width
    need = 2 * block * (2 * n + 3 * pairs + 32 * (lines - 1) + 8)
    need += 4 * block * (2 * pairs + 2 * (pairs + 1) + 2 * PLANE)
    need += 8 * heads * width * (reps + lines)
    return pl.pallas_call(
        functools.partial(fused_kernel, group, width ** (-0.5)),
        in_specs=[pl.BlockSpec(memory_space=pltpu.HBM)] * 7,
        out_specs=[free] * 4,
        out_shape=[
            jax.ShapeDtypeStruct(q.shape, half),
            jax.ShapeDtypeStruct(k.shape, half),
            jax.ShapeDtypeStruct(v.shape, half),
            jax.ShapeDtypeStruct(bias.shape, full),
        ],
        scratch_shapes=[
            pltpu.SMEM(lists.shape, lists.dtype),
            pltpu.SMEM(counts.shape, counts.dtype),
            pltpu.VMEM(bias.shape, full),
            pltpu.VMEM((n, rows, width), half),
            pltpu.VMEM((n, rows, width), half),
            pltpu.VMEM((steps, rows, UNROLL * width), half),
            pltpu.VMEM((steps, rows, UNROLL * width), half),
            pltpu.VMEM((steps, rows, UNROLL * width), half),
            pltpu.VMEM((pairs, 2 * rows, rows), full),
            pltpu.VMEM((pairs + 1, rows, width), full),
            pltpu.VMEM((pairs + 1, rows, width), full),
            pltpu.VMEM((PLANE, rows, width), full),
            pltpu.VMEM((PLANE, rows, width), full),
            pltpu.VMEM((2, 2, lines - 1, PLANE, rows, width), half),
            pltpu.VMEM((2, 2, lines - 1, PLANE, rows, width), half),
            pltpu.VMEM((2, PLANE, rows, width), half),
            pltpu.VMEM((group, width), full),
            pltpu.VMEM((reps, group, width), full),
            pltpu.VMEM((lines, group, width), full),
            pltpu.VMEM((2, group, width), full),
            pltpu.SMEM((pairs,), jnp.int32),
            pltpu.SMEM((pairs,), jnp.int32),
            pltpu.SMEM((n,), jnp.int32),
            dma((3,)), dma((2 + 2 * halves,)),
            dma((2, PLANE - 1)), dma((2, PLANE - 1)),
            dma((2, steps)), dma((2, steps)),
            dma((2, 2, lines - 1, PLANE)), dma((2, 2, lines - 1, PLANE)),
            dma((halves,)), dma((steps,)), dma((steps,)),
            dma((2, 2, lines - 1, PLANE)), dma((2, 2, lines - 1, PLANE)),
            dma((2,)), dma((2, PLANE - 1)), dma((2, PLANE - 1)),
            dma((reps - 1,)), dma((reps - 1,)),
            dma((lines - 1,)), dma((lines - 1,)),
            dma((PLANE - 1,)), dma((PLANE - 1,)),
        ],
        compiler_params=pltpu.CompilerParams(
            collective_id=1, has_side_effects=True, vmem_limit_bytes=need + 4 * 2**20
        ),
        name="fused",
    )(lists, counts, bias, q, g, k, v)


def place_kernel(*refs):
    count = len(refs) // 2
    sem = refs[-1]
    copies = [
        pltpu.make_async_copy(refs[a], refs[count + a], sem.at[a]) for a in range(count)
    ]
    for copy in copies:
        copy.start()
    for copy in copies:
        copy.wait()


def place(*arrays):
    spec = pl.BlockSpec(memory_space=pl.ANY)
    return pl.pallas_call(
        place_kernel,
        in_specs=[spec] * len(arrays),
        out_specs=[spec] * len(arrays),
        out_shape=[jax.ShapeDtypeStruct(one.shape, one.dtype) for one in arrays],
        scratch_shapes=[pltpu.SemaphoreType.DMA((len(arrays),))],
        compiler_params=pltpu.CompilerParams(vmem_limit_bytes=2**20),
        name="place",
    )(*arrays)


def body(q_lin, k_lin, value_projection, grad_out, q_bias, block_lists, block_counts):
    assert block_lists.shape[1] == lax.axis_size("seq") and block_lists.shape[2] == 2
    heads = block_lists.shape[0]
    args = (jnp.transpose(block_lists, (1, 2, 0)), block_counts.T, q_bias.reshape(heads, -1),
        q_lin[0], grad_out[0], k_lin[0], value_projection[0])
    args = [pltpu.with_memory_space_constraint(a, pltpu.HBM) for a in args]
    dq, dk, dv, dbq = fused(*args)
    dq, dk, dv, dbq = place(dq, dk, dv, dbq)
    return (dq[None], dk[None], dv[None], dbq.reshape(-1))


def solution(mesh):
    placed = (P("rep", "seq", None),) * 4 + (P(),) * 3
    return jax.shard_map(
        body,
        mesh=mesh,
        in_specs=placed,
        out_specs=(P("rep", "seq", None),) * 3 + (P(),),
        check_vma=False,
    )
```

```python
import functools

import jax
import jax.numpy as jnp
from jax import lax
from jax.experimental import pallas as pl
from jax.experimental.pallas import tpu as pltpu
from jax.sharding import PartitionSpec as P

NT = (((1,), (1,)), ((), ()))
TN = (((0,), (0,)), ((), ()))
NN = (((1,), (0,)), ((), ()))
MESH = pl.DeviceIdType.MESH
PLANE = 4
PAIR = 2


def dot(a, b, dims):
    return lax.dot_general(a, b, dims, preferred_element_type=jnp.float32)


def fused_kernel(
    group, scaling,
    lists_ref, count_ref, bias_ref, q_ref, g_ref, k_ref, v_ref,
    dq_ref, dk_ref, dv_ref, dbq_ref,
    lists_smem, count_smem, bias_buf,
    kall, vall, qbuf, gbuf, dqbuf, weights_buf, chain_k, chain_v, own_k, own_v,
    rs_send, rs_recv, final, bias_acc, rep_slots, z_slots, bias_sums,
    enc_ref, prev_ref, last_ref,
    table_sem, local_sem, plane_send, plane_recv, rows_send, rows_recv, z_send, z_recv,
    rs_sem, dq_sem, out_sem, rep_send, rep_recv, zb_sem, pb_sem,
):
    me = lax.axis_index("seq")
    n = lax.axis_size("seq")
    reps, rep = lax.axis_size("rep"), lax.axis_index("rep")
    lines = n // PLANE
    z, p = me // PLANE, me % PLANE
    rows, width = kall.shape[1:]
    pairs = PLANE * group

    def near(s):
        return (p // 2 + s // 2) % 2 * 2 + (p % 2 + s % 2) % 2

    def seq(zz, pp):
        return {"seq": zz * PLANE + pp}

    def remote(src, dst, send, recv, target):
        return pltpu.make_async_remote_copy(
            src_ref=src, dst_ref=dst, send_sem=send, recv_sem=recv,
            device_id=target, device_id_type=MESH,
        )

    def cols(start, size):
        return pl.ds(pl.multiple_of(start * width, width), size * width)

    barrier = pltpu.get_barrier_semaphore()
    z_others = [lax.rem(z + d, lines) for d in range(1, lines)]
    rep_others = [lax.rem(rep + d, reps) for d in range(1, reps)]
    for s in range(1, PLANE):
        pl.semaphore_signal(barrier, inc=1, device_id=seq(z, near(s)), device_id_type=MESH)
    for zz in z_others:
        pl.semaphore_signal(barrier, inc=1, device_id=seq(zz, p), device_id_type=MESH)
    for rr in rep_others:
        pl.semaphore_signal(barrier, inc=1, device_id={"rep": rr}, device_id_type=MESH)
    own_kv = [
        pltpu.make_async_copy(src.at[:, cols(p, 1)], dst.at[me], local_sem.at[a])
        for a, (src, dst) in enumerate([(k_ref, kall), (v_ref, vall)])
    ]
    own_rows = [
        pltpu.make_async_copy(src.at[:, cols(p * group, group)], dst.at[0], local_sem.at[2 + a])
        for a, (src, dst) in enumerate([(q_ref, qbuf), (g_ref, gbuf)])
    ]
    tables = [
        pltpu.make_async_copy(lists_ref, lists_smem, table_sem.at[0]),
        pltpu.make_async_copy(count_ref, count_smem, table_sem.at[1]),
    ]
    bias_copy = pltpu.make_async_copy(bias_ref, bias_buf, table_sem.at[2])
    for copy in own_kv + tables + own_rows + [bias_copy]:
        copy.start()

    pl.semaphore_wait(barrier, PLANE - 1 + lines - 1 + reps - 1)

    def plane_copy(a, s):
        src, dst = [(k_ref, kall), (v_ref, vall)][a]
        return remote(
            src.at[:, cols(near(s), 1)], dst.at[me],
            plane_send.at[a], plane_recv.at[a, s - 1], seq(z, near(s)),
        )

    def plane_sent(a):
        blocks = [kall, vall][a].at[pl.ds(0, PLANE - 1)]
        return remote(blocks, blocks, plane_send.at[a], plane_recv.at[a, 0], seq(z, p))

    for a in range(2):
        for s in range(1, PLANE):
            plane_copy(a, s).start()

    def rows_copy(a, s, first=0, count=group):
        src, dst = [(q_ref, qbuf), (g_ref, gbuf)][a]
        which = s - 1 if first == 0 else PLANE - 1
        return remote(
            src.at[:, cols(near(s) * group + first, count)],
            dst.at[s, :, first * width : (first + count) * width],
            rows_send.at[a], rows_recv.at[a, which], seq(z, near(s)),
        )

    def rows_sent(a):
        rows_of = [qbuf, gbuf][a].at[pl.ds(1, PLANE - 1)]
        return remote(rows_of, rows_of, rows_send.at[a], rows_recv.at[a, 0], seq(z, p))

    half_group = group // 2
    last_rows = [(0, half_group), (half_group, group - half_group)]
    for s in range(1, PLANE - 1):
        rows_copy(0, s).start()
    for s in range(1, PLANE - 1):
        rows_copy(1, s).start()
    rows_copy(0, PLANE - 1).start()
    for first, count in last_rows:
        rows_copy(1, PLANE - 1, first, count).start()

    def z_block(a, place, s):
        return [kall, vall][a].at[place * PLANE + near(s)]

    def z_copy(a, way, d, s):
        block = z_block(a, z - d if way == 0 else z + d, s)
        return remote(
            block, block, z_send.at[a, way, d], z_recv.at[a, way, d, s],
            seq(z + 1 if way == 0 else z - 1, p),
        )

    def goes(way, d):
        if way == 0:
            return (z + 1 < lines) & (z - d >= 0)
        return (z - 1 >= 0) & (z + d < lines)

    def goes_any(way):
        return goes(way, 1)

    def z_start(a, d, s):
        for way in range(2):
            @pl.when(goes(way, d))
            def _():
                z_copy(a, way, d, s).start()

    def z_relay(a, d):
        for s in range(PLANE):
            for way in range(2):
                @pl.when(z - d >= 0 if way == 0 else z + d < lines)
                def _():
                    block = z_block(a, z - d if way == 0 else z + d, s)
                    remote(
                        block, block, z_send.at[a, way, d - 1], z_recv.at[a, way, d - 1, s],
                        seq(z, p),
                    ).wait_recv()

            if d < lines - 1:
                z_start(a, d, s)

    own_kv[0].wait()
    z_start(0, 0, 0)

    for copy in tables:
        copy.wait()

    def read_table(t, _):
        position = z * PLANE + near(t // group)
        head = p * group + t % group
        other = jnp.clip(lists_smem[position, 1, head], 0, n - 1)
        enc_ref[t] = jnp.where(count_smem[position, head] != 1, other, n)
        return 0

    lax.fori_loop(0, pairs, read_table, 0)

    def link_pair(t, _):
        code = enc_ref[t]
        found = jnp.int32(0)
        for u in range(pairs):
            same = (enc_ref[u] == code) & (u < t)
            found = jnp.where(same, u + 1, found)
        prev_ref[t] = found
        return 0

    def link_block(j, _):
        found = jnp.int32(0)
        for u in range(pairs):
            found = jnp.where(enc_ref[u] == j, u + 1, found)
        last_ref[j] = found
        return 0

    for s in range(1, PLANE):
        plane_copy(0, s).wait_recv()
        z_start(0, 0, s)
    lax.fori_loop(0, pairs, link_pair, 0)
    own_kv[1].wait()
    for s in range(PLANE):
        if s:
            plane_copy(1, s).wait_recv()
        for way in range(2):
            @pl.when(goes(way, 0) & jnp.logical_not(goes_any(way)))
            def _():
                z_copy(1, way, 0, s).start()

    lax.fori_loop(0, n, link_block, 0)
    chain_k[0] = jnp.zeros((rows, width), jnp.float32)
    chain_v[0] = jnp.zeros((rows, width), jnp.float32)
    own_k[...] = jnp.zeros_like(own_k)
    own_v[...] = jnp.zeros_like(own_v)
    bias_acc[...] = jnp.zeros_like(bias_acc)

    for d in range(1, lines):
        z_relay(0, d)
    for s in range(PLANE):
        for way in range(2):
            @pl.when(goes(way, 0) & goes_any(way))
            def _():
                z_copy(1, way, 0, s).start()

    for copy in own_rows:
        copy.wait()
    bias_copy.wait()

    def both(ref, s, t):
        code = enc_ref[t]
        other = jnp.where(code < n, code, 0)
        return jnp.concatenate([ref[z * PLANE + near(s)], ref[other]], axis=0), code

    def lanes_of(h):
        return slice(h * width, (h + 1) * width)

    def soften(s):
        for h in range(group):
            t, lanes = s * group + h, lanes_of(h)
            queries = (
                qbuf[s, :, lanes].astype(jnp.float32) + bias_buf[pl.ds(p * group + h, 1), :]
            ).astype(jnp.bfloat16)
            qbuf[s, :, lanes] = queries
            keys, code = both(kall, s, t)
            scores = dot(keys, queries, NT) * scaling
            first = scores[:rows]
            second = scores[rows:] + jnp.where(code < n, 0.0, -1.0e30)
            top = jnp.maximum(
                jnp.max(first, axis=0, keepdims=True), jnp.max(second, axis=0, keepdims=True)
            )
            first, second = jnp.exp(first - top), jnp.exp(second - top)
            total = jnp.sum(first, axis=0, keepdims=True) + jnp.sum(second, axis=0, keepdims=True)
            scale_to = 1.0 / total
            weights_buf[t, :rows] = first * scale_to
            weights_buf[t, rows:] = second * scale_to

    def dq_copy(s):
        return remote(
            dqbuf.at[s], dq_ref.at[:, cols(p * group, group)],
            dq_sem.at[0], dq_sem.at[1], seq(z, near(s)),
        )

    dq_stay = pltpu.make_async_copy(dqbuf.at[0], dq_ref.at[:, cols(p * group, group)], dq_sem.at[2])
    others = dqbuf.at[pl.ds(1, PLANE - 1)]
    dq_all = remote(others, others, dq_sem.at[0], dq_sem.at[1], seq(z, p))

    def grad_values(s, heads):
        more_v = None
        for h in heads:
            t = s * group + h
            part_v = dot(weights_buf[t].astype(jnp.bfloat16), gbuf[s, :, lanes_of(h)], NN)
            chain_v[t + 1] = part_v[rows:] + chain_v[prev_ref[t]]
            more_v = part_v[:rows] if more_v is None else more_v + part_v[:rows]
        own_v[s] += more_v

    def grad_keys(s, heads):
        more_k = None
        held = []
        for h in heads:
            values, _ = both(vall, s, s * group + h)
            held.append(dot(values, gbuf[s, :, lanes_of(h)], NT))
        for h, weight_grads in zip(heads, held):
            t, lanes = s * group + h, lanes_of(h)
            keys, _ = both(kall, s, t)
            weights = weights_buf[t]
            half = weights.astype(jnp.bfloat16)
            row_dots = jnp.sum(half.astype(jnp.float32) * weight_grads, axis=0, keepdims=True)
            score_grads = (weights * (weight_grads - row_dots)).astype(jnp.bfloat16)
            grad_q = scaling * dot(score_grads, keys, TN)
            dqbuf[s, :, lanes] = grad_q.astype(jnp.bfloat16)
            bias_acc[h : h + 1, :] += jnp.sum(grad_q, axis=0, keepdims=True)
            part_k = dot(score_grads, qbuf[s, :, lanes], NN)
            chain_k[t + 1] = part_k[rows:] + chain_k[prev_ref[t]]
            more_k = part_k[:rows] if more_k is None else more_k + part_k[:rows]
        own_k[s] += more_k

    every = list(range(group))
    early = []
    for s in range(PLANE - 1):
        early.append((0, s))
        early.append((1, s))
    early.append((0, PLANE - 1))
    cut = [len(early) * d // lines for d in range(lines + 1)]

    def run(kind, s):
        if s:
            rows_copy(kind, s).wait_recv()
        if kind == 0:
            soften(s)
        else:
            grad_values(s, every)

    for d in range(lines):
        if d:
            z_relay(1, d)
        for kind, s in early[cut[d] : cut[d + 1]]:
            run(kind, s)
    for s in range(PLANE - 1):
        grad_keys(s, every)
        if s:
            dq_copy(s).start()
        else:
            dq_stay.start()
    for first, count in last_rows:
        heads = list(range(first, first + count))
        rows_copy(1, PLANE - 1, first, count).wait_recv()
        grad_values(PLANE - 1, heads)
        grad_keys(PLANE - 1, heads)
    dq_copy(PLANE - 1).start()

    rep_slots[rep] = bias_acc[...]

    def sent(a, way, d):
        blocks = [kall, vall][a].at[pl.ds(0, PLANE)]
        return remote(blocks, blocks, z_send.at[a, way, d], z_recv.at[a, way, d, 0], seq(z, p))

    for a in range(2):
        for way in range(2):
            for d in range(lines - 1):
                @pl.when(goes(way, d))
                def _():
                    sent(a, way, d).wait_send()

    def rep_copy(d):
        return remote(
            bias_acc, rep_slots.at[rep], rep_send.at[d - 1], rep_recv.at[d - 1],
            {"rep": rep_others[d - 1]},
        )

    for d in range(1, reps):
        rep_copy(d).start()

    factors = [scaling, 1.0]
    chains = [chain_k, chain_v]
    owns = [own_k, own_v]
    order = range(PLANE - PAIR, -1, -PAIR)

    def rs_copy(a, way, d, first):
        pair = pl.ds(first, PAIR)
        return remote(
            rs_send.at[a, way, d - 1, pair], rs_recv.at[a, way, d - 1, pair],
            z_send.at[a, way, d - 1], rs_sem.at[a, way, d - 1, first // PAIR],
            seq(z + 1 if way == 0 else z - 1, p),
        )

    def rs_inner(way):
        return z >= 1 if way == 0 else z + 1 < lines

    def rs_step(a, way, d, first):
        target = z + d if way == 0 else z - d
        inside = target < lines if way == 0 else target >= 0

        def part(s):
            return chains[a][last_ref[target * PLANE + near(s)]] * factors[a]

        if d < lines - 1:
            @pl.when(inside & rs_inner(way))
            def _():
                rs_copy(a, way, d + 1, first).wait_recv()
                for s in range(first, first + PAIR):
                    rs_send[a, way, d - 1, s] = (
                        part(s) + rs_recv[a, way, d, s].astype(jnp.float32)
                    ).astype(jnp.bfloat16)
                rs_copy(a, way, d, first).start()

            inside = inside & jnp.logical_not(rs_inner(way))

        @pl.when(inside)
        def _():
            for s in range(first, first + PAIR):
                rs_send[a, way, d - 1, s] = part(s).astype(jnp.bfloat16)
            rs_copy(a, way, d, first).start()

    def out_copy(a, s):
        return remote(
            final.at[a, s], [dk_ref, dv_ref][a].at[:, cols(p, 1)],
            out_sem.at[0, a], out_sem.at[1, a], seq(z, near(s)),
        )

    def out_all(a):
        blocks = final.at[a, pl.ds(1, PLANE - 1)]
        return remote(blocks, blocks, out_sem.at[0, a], out_sem.at[1, a], seq(z, p))

    def out_stay(a):
        return pltpu.make_async_copy(
            final.at[a, 0], [dk_ref, dv_ref][a].at[:, cols(p, 1)], out_sem.at[2, a]
        )

    def zb_copy(d):
        return remote(
            bias_sums.at[0], z_slots.at[z], zb_sem.at[0], zb_sem.at[1],
            seq(z_others[d - 1], p),
        )

    slots = z_slots.at[pl.ds(0, lines - 1)]
    zb_all = remote(slots, slots, zb_sem.at[0], zb_sem.at[1], seq(z, p))

    for d in range(lines - 1, 0, -1):
        for a in (1, 0):
            for first in order:
                rs_step(a, 0, d, first)
                rs_step(a, 1, d, first)
        if d == lines - 1:
            for e in range(1, reps):
                rep_copy(e).wait_recv()
            summed = rep_slots[0]
            for e in range(1, reps):
                summed = summed + rep_slots[e]
            bias_sums[0] = summed
            z_slots[z] = summed
            for e in range(1, lines):
                zb_copy(e).start()

    def finish(a, first):
        block = range(first, first + PAIR)
        for s in block:
            owns[a][s] = (owns[a][s] + chains[a][last_ref[z * PLANE + near(s)]]) * factors[a]
        for way in range(2):
            @pl.when(rs_inner(way))
            def _():
                rs_copy(a, way, 1, first).wait_recv()
                for s in block:
                    owns[a][s] += rs_recv[a, way, 0, s].astype(jnp.float32)

        for s in reversed(block):
            final[a, s] = owns[a][s].astype(jnp.bfloat16)
            if s:
                out_copy(a, s).start()
            else:
                out_stay(a).start()

    for s in order:
        finish(1, s)

    zb_all.wait_recv()
    summed = z_slots[0]
    for d in range(1, lines):
        summed = summed + z_slots[d]
    bias_sums[1] = summed

    def bias_rows(chip):
        return dbq_ref.at[pl.ds(pl.multiple_of(chip * group, group), group)]

    bias_stay = pltpu.make_async_copy(bias_sums.at[1], bias_rows(p), table_sem.at[0])
    bias_stay.start()

    def pb_copy(s):
        return remote(
            bias_sums.at[1], bias_rows(p), pb_sem.at[0], pb_sem.at[1], seq(z, near(s))
        )

    shares = bias_buf.at[pl.ds(0, (PLANE - 1) * group)]
    pb_all = remote(shares, shares, pb_sem.at[0], pb_sem.at[1], seq(z, p))
    for s in range(1, PLANE):
        pb_copy(s).start()

    for s in order:
        finish(0, s)

    for a in range(2):
        plane_sent(a).wait_send()
        rows_sent(a).wait_send()
        for way in range(2):
            for d in range(1, lines):
                @pl.when(z + d < lines if way == 0 else z - d >= 0)
                def _():
                    sent(a, way, d - 1).wait_send()
    dq_stay.wait()
    dq_all.wait()
    for d in range(1, reps):
        rep_copy(d).wait_send()
    zb_all.wait_send()
    for a in range(2):
        out_stay(a).wait()
        out_all(a).wait()
    bias_stay.wait()
    pb_all.wait()


def fused(lists, counts, bias, q, g, k, v):
    n, reps = lax.axis_size("seq"), lax.axis_size("rep")
    rows, total = q.shape
    heads, width = bias.shape
    kv_count = k.shape[1] // width
    group = heads // kv_count
    assert n % PLANE == 0 and kv_count == PLANE and group % 2 == 0
    lines = n // PLANE
    pairs = PLANE * group
    half, full = jnp.bfloat16, jnp.float32
    free = pl.BlockSpec(memory_space=pl.ANY)
    dma = pltpu.SemaphoreType.DMA
    block = rows * width
    need = 2 * block * (2 * n + 3 * pairs + 32 * (lines - 1) + 8)
    need += 4 * block * (2 * pairs + 2 * (pairs + 1) + 2 * PLANE)
    need += 8 * heads * width * (reps + lines)
    return pl.pallas_call(
        functools.partial(fused_kernel, group, width ** (-0.5)),
        in_specs=[pl.BlockSpec(memory_space=pltpu.HBM)] * 7,
        out_specs=[free] * 4,
        out_shape=[
            jax.ShapeDtypeStruct(q.shape, half),
            jax.ShapeDtypeStruct(k.shape, half),
            jax.ShapeDtypeStruct(v.shape, half),
            jax.ShapeDtypeStruct(bias.shape, full),
        ],
        scratch_shapes=[
            pltpu.SMEM(lists.shape, lists.dtype),
            pltpu.SMEM(counts.shape, counts.dtype),
            pltpu.VMEM(bias.shape, full),
            pltpu.VMEM((n, rows, width), half),
            pltpu.VMEM((n, rows, width), half),
            pltpu.VMEM((PLANE, rows, group * width), half),
            pltpu.VMEM((PLANE, rows, group * width), half),
            pltpu.VMEM((PLANE, rows, group * width), half),
            pltpu.VMEM((pairs, 2 * rows, rows), full),
            pltpu.VMEM((pairs + 1, rows, width), full),
            pltpu.VMEM((pairs + 1, rows, width), full),
            pltpu.VMEM((PLANE, rows, width), full),
            pltpu.VMEM((PLANE, rows, width), full),
            pltpu.VMEM((2, 2, lines - 1, PLANE, rows, width), half),
            pltpu.VMEM((2, 2, lines - 1, PLANE, rows, width), half),
            pltpu.VMEM((2, PLANE, rows, width), half),
            pltpu.VMEM((group, width), full),
            pltpu.VMEM((reps, group, width), full),
            pltpu.VMEM((lines, group, width), full),
            pltpu.VMEM((2, group, width), full),
            pltpu.SMEM((pairs,), jnp.int32),
            pltpu.SMEM((pairs,), jnp.int32),
            pltpu.SMEM((n,), jnp.int32),
            dma((3,)), dma((4,)),
            dma((2,)), dma((2, PLANE - 1)),
            dma((2,)), dma((2, PLANE)),
            dma((2, 2, lines - 1)), dma((2, 2, lines - 1, PLANE)),
            dma((2, 2, lines - 1, PLANE // PAIR)), dma((3,)), dma((3, 2)),
            dma((reps - 1,)), dma((reps - 1,)),
            dma((2,)), dma((2,)),
        ],
        compiler_params=pltpu.CompilerParams(
            collective_id=1, has_side_effects=True, vmem_limit_bytes=need + 4 * 2**20
        ),
        name="fused",
    )(lists, counts, bias, q, g, k, v)


def place_kernel(*refs):
    count = len(refs) // 2
    sem = refs[-1]
    copies = [
        pltpu.make_async_copy(refs[a], refs[count + a], sem.at[a]) for a in range(count)
    ]
    for copy in copies:
        copy.start()
    for copy in copies:
        copy.wait()


def place(*arrays):
    spec = pl.BlockSpec(memory_space=pl.ANY)
    return pl.pallas_call(
        place_kernel,
        in_specs=[spec] * len(arrays),
        out_specs=[spec] * len(arrays),
        out_shape=[jax.ShapeDtypeStruct(one.shape, one.dtype) for one in arrays],
        scratch_shapes=[pltpu.SemaphoreType.DMA((len(arrays),))],
        compiler_params=pltpu.CompilerParams(vmem_limit_bytes=2**20),
        name="place",
    )(*arrays)


def body(q_lin, k_lin, value_projection, grad_out, q_bias, block_lists, block_counts):
    assert block_lists.shape[1] == lax.axis_size("seq") and block_lists.shape[2] == 2
    heads = block_lists.shape[0]
    args = (jnp.transpose(block_lists, (1, 2, 0)), block_counts.T, q_bias.reshape(heads, -1),
        q_lin[0], grad_out[0], k_lin[0], value_projection[0])
    args = [pltpu.with_memory_space_constraint(a, pltpu.HBM) for a in args]
    dq, dk, dv, dbq = fused(*args)
    dq, dk, dv, dbq = place(dq, dk, dv, dbq)
    return (dq[None], dk[None], dv[None], dbq.reshape(-1))


def solution(mesh):
    placed = (P("rep", "seq", None),) * 4 + (P(),) * 3
    return jax.shard_map(
        body,
        mesh=mesh,
        in_specs=placed,
        out_specs=(P("rep", "seq", None),) * 3 + (P(),),
        check_vma=False,
    )
```

```python
import functools

import jax
import jax.numpy as jnp
from jax import lax
from jax.experimental import pallas as pl
from jax.experimental.pallas import tpu as pltpu
from jax.sharding import PartitionSpec as P

NT = (((1,), (1,)), ((), ()))
TN = (((0,), (0,)), ((), ()))
NN = (((1,), (0,)), ((), ()))
MESH = pl.DeviceIdType.MESH
PLANE = 4
PAIR = 2


def dot(a, b, dims):
    return lax.dot_general(a, b, dims, preferred_element_type=jnp.float32)


def fused_kernel(
    group, scaling,
    lists_ref, count_ref, bias_ref, q_ref, g_ref, k_ref, v_ref,
    dq_ref, dk_ref, dv_ref, dbq_ref,
    lists_smem, count_smem, bias_buf,
    kall, vall, qbuf, gbuf, dqbuf, weights_buf, chain_k, chain_v, own_k, own_v,
    rs_send, rs_recv, final, bias_acc, rep_slots, z_slots, bias_sums,
    enc_ref, prev_ref, last_ref,
    table_sem, local_sem, plane_send, plane_recv, rows_send, rows_recv, z_send, z_recv,
    gate, rs_sem, dq_sem, out_sem, rep_send, rep_recv, zb_sem, pb_sem,
):
    me = lax.axis_index("seq")
    n = lax.axis_size("seq")
    reps, rep = lax.axis_size("rep"), lax.axis_index("rep")
    lines = n // PLANE
    z, p = me // PLANE, me % PLANE
    rows, width = kall.shape[1:]
    pairs = PLANE * group

    def near(s):
        return (p // 2 + s // 2) % 2 * 2 + (p % 2 + s % 2) % 2

    def seq(zz, pp):
        return {"seq": zz * PLANE + pp}

    def remote(src, dst, send, recv, target):
        return pltpu.make_async_remote_copy(
            src_ref=src, dst_ref=dst, send_sem=send, recv_sem=recv,
            device_id=target, device_id_type=MESH,
        )

    def cols(start, size):
        return pl.ds(pl.multiple_of(start * width, width), size * width)

    barrier = pltpu.get_barrier_semaphore()
    z_others = [lax.rem(z + d, lines) for d in range(1, lines)]
    rep_others = [lax.rem(rep + d, reps) for d in range(1, reps)]
    for s in range(1, PLANE):
        pl.semaphore_signal(barrier, inc=1, device_id=seq(z, near(s)), device_id_type=MESH)
    for zz in z_others:
        pl.semaphore_signal(barrier, inc=1, device_id=seq(zz, p), device_id_type=MESH)
    for rr in rep_others:
        pl.semaphore_signal(barrier, inc=1, device_id={"rep": rr}, device_id_type=MESH)
    own_kv = [
        pltpu.make_async_copy(src.at[:, cols(p, 1)], dst.at[me], local_sem.at[a])
        for a, (src, dst) in enumerate([(k_ref, kall), (v_ref, vall)])
    ]
    own_rows = [
        pltpu.make_async_copy(src.at[:, cols(p * group, group)], dst.at[0], local_sem.at[2 + a])
        for a, (src, dst) in enumerate([(q_ref, qbuf), (g_ref, gbuf)])
    ]
    tables = [
        pltpu.make_async_copy(lists_ref, lists_smem, table_sem.at[0]),
        pltpu.make_async_copy(count_ref, count_smem, table_sem.at[1]),
    ]
    bias_copy = pltpu.make_async_copy(bias_ref, bias_buf, table_sem.at[2])
    for copy in own_kv + tables + own_rows + [bias_copy]:
        copy.start()

    pl.semaphore_wait(barrier, PLANE - 1 + lines - 1 + reps - 1)

    def plane_copy(a, s):
        src, dst = [(k_ref, kall), (v_ref, vall)][a]
        return remote(
            src.at[:, cols(near(s), 1)], dst.at[me],
            plane_send.at[a], plane_recv.at[a, s - 1], seq(z, near(s)),
        )

    def plane_sent(a):
        blocks = [kall, vall][a].at[pl.ds(0, PLANE - 1)]
        return remote(blocks, blocks, plane_send.at[a], plane_recv.at[a, 0], seq(z, p))

    lead = rep % 2 == 0
    follow = rep % 2 == 1

    def tell_partner():
        pl.semaphore_signal(
            gate, inc=1, device_id={"rep": rep // 2 * 2 + 1 - rep % 2}, device_id_type=MESH
        )

    def plane_start():
        for a in range(2):
            for s in range(1, PLANE):
                plane_copy(a, s).start()

    pl.when(lead)(plane_start)

    def rows_copy(a, s, first=0, count=group):
        src, dst = [(q_ref, qbuf), (g_ref, gbuf)][a]
        which = s - 1 if first == 0 else PLANE - 1
        return remote(
            src.at[:, cols(near(s) * group + first, count)],
            dst.at[s, :, first * width : (first + count) * width],
            rows_send.at[a if s < PLANE - 1 or a == 0 else 2], rows_recv.at[a, which],
            seq(z, near(s)),
        )

    def rows_sent(which):
        block = [
            qbuf.at[pl.ds(1, PLANE - 1)], gbuf.at[pl.ds(1, PLANE - 2)], gbuf.at[PLANE - 1]
        ][which]
        remote(block, block, rows_send.at[which], rows_recv.at[0, 0], seq(z, p)).wait_send()

    half_group = group // 2
    last_rows = [(0, half_group), (half_group, group - half_group)]
    def rows_start():
        for s in range(1, PLANE - 1):
            rows_copy(0, s).start()
        for s in range(1, PLANE - 1):
            rows_copy(1, s).start()
        rows_copy(0, PLANE - 1).start()
        for first, count in last_rows:
            rows_copy(1, PLANE - 1, first, count).start()

    def z_block(a, place, s):
        return [kall, vall][a].at[place * PLANE + near(s)]

    def z_copy(a, way, d, s):
        block = z_block(a, z - d if way == 0 else z + d, s)
        return remote(
            block, block, z_send.at[a, way, d], z_recv.at[a, way, d, s],
            seq(z + 1 if way == 0 else z - 1, p),
        )

    def goes(way, d):
        if way == 0:
            return (z + 1 < lines) & (z - d >= 0)
        return (z - 1 >= 0) & (z + d < lines)

    def z_start(a, d, s):
        for way in range(2):
            @pl.when(goes(way, d))
            def _():
                z_copy(a, way, d, s).start()

    def z_relay(a, d):
        for s in range(PLANE):
            for way in range(2):
                @pl.when(z - d >= 0 if way == 0 else z + d < lines)
                def _():
                    block = z_block(a, z - d if way == 0 else z + d, s)
                    remote(
                        block, block, z_send.at[a, way, d - 1], z_recv.at[a, way, d - 1, s],
                        seq(z, p),
                    ).wait_recv()

            if d < lines - 1:
                z_start(a, d, s)

    def z_own(a, s, who, which=None):
        for way in range(2):
            wanted = goes(way, 0) & who
            if which is not None:
                wanted = wanted & (goes(way, 1) if which else jnp.logical_not(goes(way, 1)))

            @pl.when(wanted)
            def _():
                z_copy(a, way, 0, s).start()

    own_kv[0].wait()
    z_own(0, 0, lead)

    for copy in tables:
        copy.wait()

    def read_table(t, _):
        position = z * PLANE + near(t // group)
        head = p * group + t % group
        other = jnp.clip(lists_smem[position, 1, head], 0, n - 1)
        enc_ref[t] = jnp.where(count_smem[position, head] != 1, other, n)
        return 0

    lax.fori_loop(0, pairs, read_table, 0)
    pl.when(lead)(rows_start)

    def link_pair(t, _):
        code = enc_ref[t]
        found = jnp.int32(0)
        for u in range(pairs):
            same = (enc_ref[u] == code) & (u < t)
            found = jnp.where(same, u + 1, found)
        prev_ref[t] = found
        return 0

    def link_block(j, _):
        found = jnp.int32(0)
        for u in range(pairs):
            found = jnp.where(enc_ref[u] == j, u + 1, found)
        last_ref[j] = found
        return 0

    lax.fori_loop(0, pairs, link_pair, 0)
    pl.when(follow)(plane_start)
    for s in range(1, PLANE):
        plane_copy(0, s).wait_recv()
        z_own(0, s, lead)
    own_kv[1].wait()
    for s in range(PLANE):
        if s:
            plane_copy(1, s).wait_recv()
        z_own(1, s, lead, False)
    lax.fori_loop(0, n, link_block, 0)
    chain_k[0] = jnp.zeros((rows, width), jnp.float32)
    chain_v[0] = jnp.zeros((rows, width), jnp.float32)
    own_k[...] = jnp.zeros_like(own_k)
    own_v[...] = jnp.zeros_like(own_v)
    bias_acc[...] = jnp.zeros_like(bias_acc)

    @pl.when(follow)
    def _():
        pl.semaphore_wait(gate, 1)
        rows_start()

    for s in range(PLANE):
        z_own(0, s, follow)
    for s in range(PLANE):
        z_own(1, s, follow, False)
    for d in range(1, lines):
        if d == lines - 1:
            @pl.when(lead)
            def _():
                rows_sent(0)
                rows_sent(1)
                tell_partner()

        z_relay(0, d)
        if d == 1:
            for s in range(PLANE):
                z_own(1, s, True, True)
        else:
            z_relay(1, d - 1)

    for copy in own_rows:
        copy.wait()
    bias_copy.wait()

    def both(ref, s, t):
        code = enc_ref[t]
        other = jnp.where(code < n, code, 0)
        return jnp.concatenate([ref[z * PLANE + near(s)], ref[other]], axis=0), code

    def lanes_of(h):
        return slice(h * width, (h + 1) * width)

    def soften(s):
        for h in range(group):
            t, lanes = s * group + h, lanes_of(h)
            queries = (
                qbuf[s, :, lanes].astype(jnp.float32) + bias_buf[pl.ds(p * group + h, 1), :]
            ).astype(jnp.bfloat16)
            qbuf[s, :, lanes] = queries
            keys, code = both(kall, s, t)
            scores = dot(keys, queries, NT) * scaling
            first = scores[:rows]
            second = scores[rows:] + jnp.where(code < n, 0.0, -1.0e30)
            top = jnp.maximum(
                jnp.max(first, axis=0, keepdims=True), jnp.max(second, axis=0, keepdims=True)
            )
            first, second = jnp.exp(first - top), jnp.exp(second - top)
            total = jnp.sum(first, axis=0, keepdims=True) + jnp.sum(second, axis=0, keepdims=True)
            scale_to = 1.0 / total
            weights_buf[t, :rows] = first * scale_to
            weights_buf[t, rows:] = second * scale_to

    def dq_copy(s):
        return remote(
            dqbuf.at[s], dq_ref.at[:, cols(p * group, group)],
            dq_sem.at[0], dq_sem.at[1], seq(z, near(s)),
        )

    dq_stay = pltpu.make_async_copy(dqbuf.at[0], dq_ref.at[:, cols(p * group, group)], dq_sem.at[2])
    others = dqbuf.at[pl.ds(1, PLANE - 1)]
    dq_all = remote(others, others, dq_sem.at[0], dq_sem.at[1], seq(z, p))

    def grad_values(s, heads):
        more_v = None
        for h in heads:
            t = s * group + h
            part_v = dot(weights_buf[t].astype(jnp.bfloat16), gbuf[s, :, lanes_of(h)], NN)
            chain_v[t + 1] = part_v[rows:] + chain_v[prev_ref[t]]
            more_v = part_v[:rows] if more_v is None else more_v + part_v[:rows]
        own_v[s] += more_v

    def grad_keys(s, heads):
        more_k = None
        held = []
        for h in heads:
            values, _ = both(vall, s, s * group + h)
            held.append(dot(values, gbuf[s, :, lanes_of(h)], NT))
        for h, weight_grads in zip(heads, held):
            t, lanes = s * group + h, lanes_of(h)
            keys, _ = both(kall, s, t)
            weights = weights_buf[t]
            half = weights.astype(jnp.bfloat16)
            row_dots = jnp.sum(half.astype(jnp.float32) * weight_grads, axis=0, keepdims=True)
            score_grads = (weights * (weight_grads - row_dots)).astype(jnp.bfloat16)
            grad_q = scaling * dot(score_grads, keys, TN)
            dqbuf[s, :, lanes] = grad_q.astype(jnp.bfloat16)
            bias_acc[h : h + 1, :] += jnp.sum(grad_q, axis=0, keepdims=True)
            part_k = dot(score_grads, qbuf[s, :, lanes], NN)
            chain_k[t + 1] = part_k[rows:] + chain_k[prev_ref[t]]
            more_k = part_k[:rows] if more_k is None else more_k + part_k[:rows]
        own_k[s] += more_k

    every = list(range(group))
    early = []
    for s in range(PLANE - 1):
        early.append((0, s))
        early.append((1, s))
    early.append((0, PLANE - 1))
    cut = len(early) // 2

    def run(kind, s):
        if s:
            rows_copy(kind, s).wait_recv()
        if kind == 0:
            soften(s)
        else:
            grad_values(s, every)

    for kind, s in early[:cut]:
        run(kind, s)
    z_relay(1, lines - 1)
    for kind, s in early[cut:]:
        run(kind, s)

    def dq_start(s):
        @pl.when(follow)
        def _():
            dq_copy(s).start()

    for s in range(PLANE - 1):
        grad_keys(s, every)
        if s:
            dq_start(s)
        else:
            dq_stay.start()
    for first, count in last_rows:
        heads = list(range(first, first + count))
        rows_copy(1, PLANE - 1, first, count).wait_recv()
        grad_values(PLANE - 1, heads)
        grad_keys(PLANE - 1, heads)
    dq_start(PLANE - 1)
    rows_sent(2)

    @pl.when(follow)
    def _():
        rows_sent(0)
        rows_sent(1)
        tell_partner()

    rep_slots[rep] = bias_acc[...]

    def sent(a, way, d):
        blocks = [kall, vall][a].at[pl.ds(0, PLANE)]
        return remote(blocks, blocks, z_send.at[a, way, d], z_recv.at[a, way, d, 0], seq(z, p))

    for a in range(2):
        for way in range(2):
            for d in range(lines - 1):
                @pl.when(goes(way, d))
                def _():
                    sent(a, way, d).wait_send()

    def rep_copy(d):
        return remote(
            bias_acc, rep_slots.at[rep], rep_send.at[d - 1], rep_recv.at[d - 1],
            {"rep": rep_others[d - 1]},
        )

    for d in range(1, reps):
        rep_copy(d).start()

    factors = [scaling, 1.0]
    chains = [chain_k, chain_v]
    owns = [own_k, own_v]
    order = range(PLANE - PAIR, -1, -PAIR)

    def rs_copy(a, way, d, first):
        pair = pl.ds(first, PAIR)
        return remote(
            rs_send.at[a, way, d - 1, pair], rs_recv.at[a, way, d - 1, pair],
            z_send.at[a, way, d - 1], rs_sem.at[a, way, d - 1, first // PAIR],
            seq(z + 1 if way == 0 else z - 1, p),
        )

    def rs_inner(way):
        return z >= 1 if way == 0 else z + 1 < lines

    def rs_step(a, way, d, first):
        target = z + d if way == 0 else z - d
        inside = target < lines if way == 0 else target >= 0

        def part(s):
            return chains[a][last_ref[target * PLANE + near(s)]] * factors[a]

        if d < lines - 1:
            @pl.when(inside & rs_inner(way))
            def _():
                rs_copy(a, way, d + 1, first).wait_recv()
                for s in range(first, first + PAIR):
                    rs_send[a, way, d - 1, s] = (
                        part(s) + rs_recv[a, way, d, s].astype(jnp.float32)
                    ).astype(jnp.bfloat16)
                rs_copy(a, way, d, first).start()

            inside = inside & jnp.logical_not(rs_inner(way))

        @pl.when(inside)
        def _():
            for s in range(first, first + PAIR):
                rs_send[a, way, d - 1, s] = part(s).astype(jnp.bfloat16)
            rs_copy(a, way, d, first).start()

    def out_copy(a, s):
        return remote(
            final.at[a, s], [dk_ref, dv_ref][a].at[:, cols(p, 1)],
            out_sem.at[0, a], out_sem.at[1, a], seq(z, near(s)),
        )

    def out_all(a):
        blocks = final.at[a, pl.ds(1, PLANE - 1)]
        return remote(blocks, blocks, out_sem.at[0, a], out_sem.at[1, a], seq(z, p))

    def out_stay(a):
        return pltpu.make_async_copy(
            final.at[a, 0], [dk_ref, dv_ref][a].at[:, cols(p, 1)], out_sem.at[2, a]
        )

    def zb_copy(d):
        return remote(
            bias_sums.at[0], z_slots.at[z], zb_sem.at[0], zb_sem.at[1],
            seq(z_others[d - 1], p),
        )

    slots = z_slots.at[pl.ds(0, lines - 1)]
    zb_all = remote(slots, slots, zb_sem.at[0], zb_sem.at[1], seq(z, p))

    for d in range(lines - 1, 0, -1):
        for a in (1, 0):
            for first in order:
                rs_step(a, 0, d, first)
                rs_step(a, 1, d, first)

    for e in range(1, reps):
        rep_copy(e).wait_recv()
    summed = rep_slots[0]
    for e in range(1, reps):
        summed = summed + rep_slots[e]
    bias_sums[0] = summed
    z_slots[z] = summed
    for e in range(1, lines):
        zb_copy(e).start()

    @pl.when(lead)
    def _():
        pl.semaphore_wait(gate, 1)
        for s in range(1, PLANE):
            dq_copy(s).start()

    def finish(a, first):
        block = range(first, first + PAIR)
        for s in block:
            owns[a][s] = (owns[a][s] + chains[a][last_ref[z * PLANE + near(s)]]) * factors[a]
        for way in range(2):
            @pl.when(rs_inner(way))
            def _():
                rs_copy(a, way, 1, first).wait_recv()
                for s in block:
                    owns[a][s] += rs_recv[a, way, 0, s].astype(jnp.float32)

        for s in reversed(block):
            final[a, s] = owns[a][s].astype(jnp.bfloat16)
            if s:
                out_copy(a, s).start()
            else:
                out_stay(a).start()

    for s in order:
        finish(1, s)

    zb_all.wait_recv()
    summed = z_slots[0]
    for d in range(1, lines):
        summed = summed + z_slots[d]
    bias_sums[1] = summed

    def bias_rows(chip):
        return dbq_ref.at[pl.ds(pl.multiple_of(chip * group, group), group)]

    bias_stay = pltpu.make_async_copy(bias_sums.at[1], bias_rows(p), table_sem.at[0])
    bias_stay.start()

    def pb_copy(s):
        return remote(
            bias_sums.at[1], bias_rows(p), pb_sem.at[0], pb_sem.at[1], seq(z, near(s))
        )

    shares = bias_buf.at[pl.ds(0, (PLANE - 1) * group)]
    pb_all = remote(shares, shares, pb_sem.at[0], pb_sem.at[1], seq(z, p))
    for s in range(1, PLANE):
        pb_copy(s).start()

    for s in order:
        finish(0, s)

    for a in range(2):
        plane_sent(a).wait_send()
        for way in range(2):
            for d in range(1, lines):
                @pl.when(z + d < lines if way == 0 else z - d >= 0)
                def _():
                    sent(a, way, d - 1).wait_send()
    dq_stay.wait()
    dq_all.wait()
    for d in range(1, reps):
        rep_copy(d).wait_send()
    zb_all.wait_send()
    for a in range(2):
        out_stay(a).wait()
        out_all(a).wait()
    bias_stay.wait()
    pb_all.wait()


def fused(lists, counts, bias, q, g, k, v):
    n, reps = lax.axis_size("seq"), lax.axis_size("rep")
    rows, total = q.shape
    heads, width = bias.shape
    kv_count = k.shape[1] // width
    group = heads // kv_count
    assert reps % 2 == 0 and n % PLANE == 0 and kv_count == PLANE and group % 2 == 0
    lines = n // PLANE
    pairs = PLANE * group
    half, full = jnp.bfloat16, jnp.float32
    free = pl.BlockSpec(memory_space=pl.ANY)
    dma = pltpu.SemaphoreType.DMA
    block = rows * width
    need = 2 * block * (2 * n + 3 * pairs + 32 * (lines - 1) + 8)
    need += 4 * block * (2 * pairs + 2 * (pairs + 1) + 2 * PLANE)
    need += 8 * heads * width * (reps + lines)
    return pl.pallas_call(
        functools.partial(fused_kernel, group, width ** (-0.5)),
        in_specs=[pl.BlockSpec(memory_space=pltpu.HBM)] * 7,
        out_specs=[free] * 4,
        out_shape=[
            jax.ShapeDtypeStruct(q.shape, half),
            jax.ShapeDtypeStruct(k.shape, half),
            jax.ShapeDtypeStruct(v.shape, half),
            jax.ShapeDtypeStruct(bias.shape, full),
        ],
        scratch_shapes=[
            pltpu.SMEM(lists.shape, lists.dtype),
            pltpu.SMEM(counts.shape, counts.dtype),
            pltpu.VMEM(bias.shape, full),
            pltpu.VMEM((n, rows, width), half),
            pltpu.VMEM((n, rows, width), half),
            pltpu.VMEM((PLANE, rows, group * width), half),
            pltpu.VMEM((PLANE, rows, group * width), half),
            pltpu.VMEM((PLANE, rows, group * width), half),
            pltpu.VMEM((pairs, 2 * rows, rows), full),
            pltpu.VMEM((pairs + 1, rows, width), full),
            pltpu.VMEM((pairs + 1, rows, width), full),
            pltpu.VMEM((PLANE, rows, width), full),
            pltpu.VMEM((PLANE, rows, width), full),
            pltpu.VMEM((2, 2, lines - 1, PLANE, rows, width), half),
            pltpu.VMEM((2, 2, lines - 1, PLANE, rows, width), half),
            pltpu.VMEM((2, PLANE, rows, width), half),
            pltpu.VMEM((group, width), full),
            pltpu.VMEM((reps, group, width), full),
            pltpu.VMEM((lines, group, width), full),
            pltpu.VMEM((2, group, width), full),
            pltpu.SMEM((pairs,), jnp.int32),
            pltpu.SMEM((pairs,), jnp.int32),
            pltpu.SMEM((n,), jnp.int32),
            dma((3,)), dma((4,)),
            dma((2,)), dma((2, PLANE - 1)),
            dma((3,)), dma((2, PLANE)),
            dma((2, 2, lines - 1)), dma((2, 2, lines - 1, PLANE)),
            pltpu.SemaphoreType.REGULAR,
            dma((2, 2, lines - 1, PLANE // PAIR)), dma((3,)), dma((3, 2)),
            dma((reps - 1,)), dma((reps - 1,)),
            dma((2,)), dma((2,)),
        ],
        compiler_params=pltpu.CompilerParams(
            collective_id=1, has_side_effects=True, vmem_limit_bytes=need + 4 * 2**20
        ),
        name="fused",
    )(lists, counts, bias, q, g, k, v)


def place_kernel(*refs):
    count = len(refs) // 2
    sem = refs[-1]
    copies = [
        pltpu.make_async_copy(refs[a], refs[count + a], sem.at[a]) for a in range(count)
    ]
    for copy in copies:
        copy.start()
    for copy in copies:
        copy.wait()


def place(*arrays):
    spec = pl.BlockSpec(memory_space=pl.ANY)
    return pl.pallas_call(
        place_kernel,
        in_specs=[spec] * len(arrays),
        out_specs=[spec] * len(arrays),
        out_shape=[jax.ShapeDtypeStruct(one.shape, one.dtype) for one in arrays],
        scratch_shapes=[pltpu.SemaphoreType.DMA((len(arrays),))],
        compiler_params=pltpu.CompilerParams(vmem_limit_bytes=2**20),
        name="place",
    )(*arrays)


def body(q_lin, k_lin, value_projection, grad_out, q_bias, block_lists, block_counts):
    assert block_lists.shape[1] == lax.axis_size("seq") and block_lists.shape[2] == 2
    heads = block_lists.shape[0]
    args = (jnp.transpose(block_lists, (1, 2, 0)), block_counts.T, q_bias.reshape(heads, -1),
        q_lin[0], grad_out[0], k_lin[0], value_projection[0])
    args = [pltpu.with_memory_space_constraint(a, pltpu.HBM) for a in args]
    dq, dk, dv, dbq = fused(*args)
    dq, dk, dv, dbq = place(dq, dk, dv, dbq)
    return (dq[None], dk[None], dv[None], dbq.reshape(-1))


def solution(mesh):
    placed = (P("rep", "seq", None),) * 4 + (P(),) * 3
    return jax.shard_map(
        body,
        mesh=mesh,
        in_specs=placed,
        out_specs=(P("rep", "seq", None),) * 3 + (P(),),
        check_vma=False,
    )
```

```python
import functools

import jax
import jax.numpy as jnp
from jax import lax
from jax.experimental import pallas as pl
from jax.experimental.pallas import tpu as pltpu
from jax.sharding import PartitionSpec as P

NT = (((1,), (1,)), ((), ()))
TN = (((0,), (0,)), ((), ()))
NN = (((1,), (0,)), ((), ()))
MESH = pl.DeviceIdType.MESH
PLANE = 4
PAIR = 2


def dot(a, b, dims):
    return lax.dot_general(a, b, dims, preferred_element_type=jnp.float32)


def fused_kernel(
    group, scaling,
    lists_ref, count_ref, bias_ref, q_ref, g_ref, k_ref, v_ref,
    dq_ref, dk_ref, dv_ref, dbq_ref,
    lists_smem, count_smem, bias_buf,
    kbuf, vbuf, kall, vall, qbuf, gbuf, dqbuf, weights_buf, chain_k, chain_v, own_k, own_v,
    rs_send, rs_recv, final, bias_acc, rep_slots, z_slots, bias_sums,
    enc_ref, prev_ref, last_ref,
    table_sem, local_sem, plane_send, plane_recv, rows_send, rows_recv, z_send, z_recv,
    gate, rs_sem, dq_sem, out_sem, rep_send, rep_recv, zb_sem, pb_sem,
):
    me = lax.axis_index("seq")
    n = lax.axis_size("seq")
    reps, rep = lax.axis_size("rep"), lax.axis_index("rep")
    lines = n // PLANE
    z, p = me // PLANE, me % PLANE
    rows, width = kall.shape[1:]
    pairs = PLANE * group

    def near(s):
        return (p // 2 + s // 2) % 2 * 2 + (p % 2 + s % 2) % 2

    def seq(zz, pp):
        return {"seq": zz * PLANE + pp}

    def remote(src, dst, send, recv, target):
        return pltpu.make_async_remote_copy(
            src_ref=src, dst_ref=dst, send_sem=send, recv_sem=recv,
            device_id=target, device_id_type=MESH,
        )

    def cols(start, size):
        return pl.ds(pl.multiple_of(start * width, width), size * width)

    barrier = pltpu.get_barrier_semaphore()
    z_others = [lax.rem(z + d, lines) for d in range(1, lines)]
    rep_others = [lax.rem(rep + d, reps) for d in range(1, reps)]
    for s in range(1, PLANE):
        pl.semaphore_signal(barrier, inc=1, device_id=seq(z, near(s)), device_id_type=MESH)
    for zz in z_others:
        pl.semaphore_signal(barrier, inc=1, device_id=seq(zz, p), device_id_type=MESH)
    for rr in rep_others:
        pl.semaphore_signal(barrier, inc=1, device_id={"rep": rr}, device_id_type=MESH)
    own_kv = [
        pltpu.make_async_copy(src.at[:, cols(p, 1)], dst.at[me], local_sem.at[a])
        for a, (src, dst) in enumerate([(k_ref, kall), (v_ref, vall)])
    ]
    own_rows = [
        pltpu.make_async_copy(src.at[:, cols(p * group, group)], dst.at[0], local_sem.at[2 + a])
        for a, (src, dst) in enumerate([(q_ref, qbuf), (g_ref, gbuf)])
    ]
    tables = [
        pltpu.make_async_copy(lists_ref, lists_smem, table_sem.at[0]),
        pltpu.make_async_copy(count_ref, count_smem, table_sem.at[1]),
    ]
    bias_copy = pltpu.make_async_copy(bias_ref, bias_buf, table_sem.at[2])
    ahead = [
        pltpu.make_async_copy(src, dst, local_sem.at[4 + a])
        for a, (src, dst) in enumerate([(k_ref, kbuf), (v_ref, vbuf)])
    ]
    for copy in ahead + own_kv + tables + own_rows + [bias_copy]:
        copy.start()

    pl.semaphore_wait(barrier, PLANE - 1 + lines - 1 + reps - 1)

    def plane_copy(a, s):
        src, dst = [(kbuf, kall), (vbuf, vall)][a]
        return remote(
            src.at[:, cols(near(s), 1)], dst.at[me],
            plane_send.at[a], plane_recv.at[a, s - 1], seq(z, near(s)),
        )

    def plane_sent(a):
        blocks = [kall, vall][a].at[pl.ds(0, PLANE - 1)]
        return remote(blocks, blocks, plane_send.at[a], plane_recv.at[a, 0], seq(z, p))

    lead = rep % 2 == 0
    follow = rep % 2 == 1

    def tell_partner():
        pl.semaphore_signal(
            gate, inc=1, device_id={"rep": rep // 2 * 2 + 1 - rep % 2}, device_id_type=MESH
        )

    for copy in ahead:
        copy.wait()

    def plane_start():
        for a in range(2):
            for s in range(1, PLANE):
                plane_copy(a, s).start()

    pl.when(lead)(plane_start)

    def rows_copy(a, s, first=0, count=group):
        src, dst = [(q_ref, qbuf), (g_ref, gbuf)][a]
        which = s - 1 if first == 0 else PLANE - 1
        return remote(
            src.at[:, cols(near(s) * group + first, count)],
            dst.at[s, :, first * width : (first + count) * width],
            rows_send.at[a if s < PLANE - 1 or a == 0 else 2], rows_recv.at[a, which],
            seq(z, near(s)),
        )

    def rows_sent(which):
        block = [
            qbuf.at[pl.ds(1, PLANE - 1)], gbuf.at[pl.ds(1, PLANE - 2)], gbuf.at[PLANE - 1]
        ][which]
        remote(block, block, rows_send.at[which], rows_recv.at[0, 0], seq(z, p)).wait_send()

    half_group = group // 2
    last_rows = [(0, half_group), (half_group, group - half_group)]
    def rows_start():
        for s in range(1, PLANE - 1):
            rows_copy(0, s).start()
        for s in range(1, PLANE - 1):
            rows_copy(1, s).start()
        rows_copy(0, PLANE - 1).start()
        for first, count in last_rows:
            rows_copy(1, PLANE - 1, first, count).start()

    def z_block(a, place, s):
        return [kall, vall][a].at[place * PLANE + near(s)]

    def z_copy(a, way, d, s):
        block = z_block(a, z - d if way == 0 else z + d, s)
        return remote(
            block, block, z_send.at[a, way, d], z_recv.at[a, way, d, s],
            seq(z + 1 if way == 0 else z - 1, p),
        )

    def goes(way, d):
        if way == 0:
            return (z + 1 < lines) & (z - d >= 0)
        return (z - 1 >= 0) & (z + d < lines)

    def z_start(a, d, s):
        for way in range(2):
            @pl.when(goes(way, d))
            def _():
                z_copy(a, way, d, s).start()

    def z_relay(a, d):
        for s in range(PLANE):
            for way in range(2):
                @pl.when(z - d >= 0 if way == 0 else z + d < lines)
                def _():
                    block = z_block(a, z - d if way == 0 else z + d, s)
                    remote(
                        block, block, z_send.at[a, way, d - 1], z_recv.at[a, way, d - 1, s],
                        seq(z, p),
                    ).wait_recv()

            if d < lines - 1:
                z_start(a, d, s)

    def z_own(a, s, who, which=None):
        for way in range(2):
            wanted = goes(way, 0) & who
            if which is not None:
                wanted = wanted & (goes(way, 1) if which else jnp.logical_not(goes(way, 1)))

            @pl.when(wanted)
            def _():
                z_copy(a, way, 0, s).start()

    own_kv[0].wait()
    z_own(0, 0, lead)

    for copy in tables:
        copy.wait()

    def read_table(t, _):
        position = z * PLANE + near(t // group)
        head = p * group + t % group
        other = jnp.clip(lists_smem[position, 1, head], 0, n - 1)
        enc_ref[t] = jnp.where(count_smem[position, head] != 1, other, n)
        return 0

    lax.fori_loop(0, pairs, read_table, 0)
    pl.when(lead)(rows_start)

    def link_pair(t, _):
        code = enc_ref[t]
        found = jnp.int32(0)
        for u in range(pairs):
            same = (enc_ref[u] == code) & (u < t)
            found = jnp.where(same, u + 1, found)
        prev_ref[t] = found
        return 0

    def link_block(j, _):
        found = jnp.int32(0)
        for u in range(pairs):
            found = jnp.where(enc_ref[u] == j, u + 1, found)
        last_ref[j] = found
        return 0

    lax.fori_loop(0, pairs, link_pair, 0)
    pl.when(follow)(plane_start)
    for s in range(1, PLANE):
        plane_copy(0, s).wait_recv()
        z_own(0, s, lead)
    own_kv[1].wait()
    for s in range(PLANE):
        if s:
            plane_copy(1, s).wait_recv()
        z_own(1, s, lead, False)
    lax.fori_loop(0, n, link_block, 0)
    chain_k[0] = jnp.zeros((rows, width), jnp.float32)
    chain_v[0] = jnp.zeros((rows, width), jnp.float32)
    own_k[...] = jnp.zeros_like(own_k)
    own_v[...] = jnp.zeros_like(own_v)
    bias_acc[...] = jnp.zeros_like(bias_acc)

    @pl.when(follow)
    def _():
        pl.semaphore_wait(gate, 1)
        rows_start()

    for s in range(PLANE):
        z_own(0, s, follow)
    for s in range(PLANE):
        z_own(1, s, follow, False)
    for d in range(1, lines):
        if d == lines - 1:
            @pl.when(lead)
            def _():
                rows_sent(0)
                rows_sent(1)
                tell_partner()

        z_relay(0, d)
        if d == 1:
            for s in range(PLANE):
                z_own(1, s, True, True)
        elif d < lines - 1:
            z_relay(1, d - 1)

    for copy in own_rows:
        copy.wait()
    bias_copy.wait()

    def both(ref, s, t):
        code = enc_ref[t]
        other = jnp.where(code < n, code, 0)
        return jnp.concatenate([ref[z * PLANE + near(s)], ref[other]], axis=0), code

    def lanes_of(h):
        return slice(h * width, (h + 1) * width)

    def soften(s):
        for h in range(group):
            t, lanes = s * group + h, lanes_of(h)
            queries = (
                qbuf[s, :, lanes].astype(jnp.float32) + bias_buf[pl.ds(p * group + h, 1), :]
            ).astype(jnp.bfloat16)
            qbuf[s, :, lanes] = queries
            keys, code = both(kall, s, t)
            scores = dot(keys, queries, NT) * scaling
            first = scores[:rows]
            second = scores[rows:] + jnp.where(code < n, 0.0, -1.0e30)
            top = jnp.maximum(
                jnp.max(first, axis=0, keepdims=True), jnp.max(second, axis=0, keepdims=True)
            )
            first, second = jnp.exp(first - top), jnp.exp(second - top)
            total = jnp.sum(first, axis=0, keepdims=True) + jnp.sum(second, axis=0, keepdims=True)
            scale_to = 1.0 / total
            weights_buf[t, :rows] = first * scale_to
            weights_buf[t, rows:] = second * scale_to

    def dq_copy(s):
        return remote(
            dqbuf.at[s], dq_ref.at[:, cols(p * group, group)],
            dq_sem.at[0], dq_sem.at[1], seq(z, near(s)),
        )

    dq_stay = pltpu.make_async_copy(dqbuf.at[0], dq_ref.at[:, cols(p * group, group)], dq_sem.at[2])
    others = dqbuf.at[pl.ds(1, PLANE - 1)]
    dq_all = remote(others, others, dq_sem.at[0], dq_sem.at[1], seq(z, p))

    def grad_values(s, heads):
        more_v = None
        for h in heads:
            t = s * group + h
            part_v = dot(weights_buf[t].astype(jnp.bfloat16), gbuf[s, :, lanes_of(h)], NN)
            chain_v[t + 1] = part_v[rows:] + chain_v[prev_ref[t]]
            more_v = part_v[:rows] if more_v is None else more_v + part_v[:rows]
        own_v[s] += more_v

    def grad_keys(s, heads):
        more_k = None
        held = []
        for h in heads:
            values, _ = both(vall, s, s * group + h)
            held.append(dot(values, gbuf[s, :, lanes_of(h)], NT))
        for h, weight_grads in zip(heads, held):
            t, lanes = s * group + h, lanes_of(h)
            keys, _ = both(kall, s, t)
            weights = weights_buf[t]
            half = weights.astype(jnp.bfloat16)
            row_dots = jnp.sum(half.astype(jnp.float32) * weight_grads, axis=0, keepdims=True)
            score_grads = (weights * (weight_grads - row_dots)).astype(jnp.bfloat16)
            grad_q = scaling * dot(score_grads, keys, TN)
            dqbuf[s, :, lanes] = grad_q.astype(jnp.bfloat16)
            bias_acc[h : h + 1, :] += jnp.sum(grad_q, axis=0, keepdims=True)
            part_k = dot(score_grads, qbuf[s, :, lanes], NN)
            chain_k[t + 1] = part_k[rows:] + chain_k[prev_ref[t]]
            more_k = part_k[:rows] if more_k is None else more_k + part_k[:rows]
        own_k[s] += more_k

    every = list(range(group))
    early = []
    for s in range(PLANE - 1):
        early.append((0, s))
        early.append((1, s))
    early.append((0, PLANE - 1))

    def run(kind, s):
        if s:
            rows_copy(kind, s).wait_recv()
        if kind == 0:
            soften(s)
        else:
            grad_values(s, every)

    for kind, s in early[:2]:
        run(kind, s)
    z_relay(1, lines - 2)
    for kind, s in early[2:5]:
        run(kind, s)
    z_relay(1, lines - 1)

    def dq_start(s):
        @pl.when(follow)
        def _():
            dq_copy(s).start()

    for s in range(PLANE - 1):
        if s == PLANE - 2:
            run(*early[5])
        grad_keys(s, every)
        if s:
            dq_start(s)
        else:
            dq_stay.start()
    run(*early[6])
    for first, count in last_rows:
        heads = list(range(first, first + count))
        rows_copy(1, PLANE - 1, first, count).wait_recv()
        grad_values(PLANE - 1, heads)
        grad_keys(PLANE - 1, heads)
    dq_start(PLANE - 1)
    rows_sent(2)

    @pl.when(follow)
    def _():
        rows_sent(0)
        rows_sent(1)
        tell_partner()

    rep_slots[rep] = bias_acc[...]

    def sent(a, way, d):
        blocks = [kall, vall][a].at[pl.ds(0, PLANE)]
        return remote(blocks, blocks, z_send.at[a, way, d], z_recv.at[a, way, d, 0], seq(z, p))

    for a in range(2):
        for way in range(2):
            for d in range(lines - 1):
                @pl.when(goes(way, d))
                def _():
                    sent(a, way, d).wait_send()

    def rep_copy(d):
        return remote(
            bias_acc, rep_slots.at[rep], rep_send.at[d - 1], rep_recv.at[d - 1],
            {"rep": rep_others[d - 1]},
        )

    for d in range(1, reps):
        rep_copy(d).start()

    factors = [scaling, 1.0]
    chains = [chain_k, chain_v]
    owns = [own_k, own_v]
    order = range(PLANE - PAIR, -1, -PAIR)

    def rs_copy(a, way, d, first):
        pair = pl.ds(first, PAIR)
        return remote(
            rs_send.at[a, way, d - 1, pair], rs_recv.at[a, way, d - 1, pair],
            z_send.at[a, way, d - 1], rs_sem.at[a, way, d - 1, first // PAIR],
            seq(z + 1 if way == 0 else z - 1, p),
        )

    def rs_inner(way):
        return z >= 1 if way == 0 else z + 1 < lines

    def rs_step(a, way, d, first):
        target = z + d if way == 0 else z - d
        inside = target < lines if way == 0 else target >= 0

        def part(s):
            return chains[a][last_ref[target * PLANE + near(s)]] * factors[a]

        if d < lines - 1:
            @pl.when(inside & rs_inner(way))
            def _():
                rs_copy(a, way, d + 1, first).wait_recv()
                for s in range(first, first + PAIR):
                    rs_send[a, way, d - 1, s] = (
                        part(s) + rs_recv[a, way, d, s].astype(jnp.float32)
                    ).astype(jnp.bfloat16)
                rs_copy(a, way, d, first).start()

            inside = inside & jnp.logical_not(rs_inner(way))

        @pl.when(inside)
        def _():
            for s in range(first, first + PAIR):
                rs_send[a, way, d - 1, s] = part(s).astype(jnp.bfloat16)
            rs_copy(a, way, d, first).start()

    def out_copy(a, s):
        return remote(
            final.at[a, s], [dk_ref, dv_ref][a].at[:, cols(p, 1)],
            out_sem.at[0, a], out_sem.at[1, a], seq(z, near(s)),
        )

    def out_all(a):
        blocks = final.at[a, pl.ds(1, PLANE - 1)]
        return remote(blocks, blocks, out_sem.at[0, a], out_sem.at[1, a], seq(z, p))

    def out_stay(a):
        return pltpu.make_async_copy(
            final.at[a, 0], [dk_ref, dv_ref][a].at[:, cols(p, 1)], out_sem.at[2, a]
        )

    def zb_copy(d):
        return remote(
            bias_sums.at[0], z_slots.at[z], zb_sem.at[0], zb_sem.at[1],
            seq(z_others[d - 1], p),
        )

    slots = z_slots.at[pl.ds(0, lines - 1)]
    zb_all = remote(slots, slots, zb_sem.at[0], zb_sem.at[1], seq(z, p))

    for d in range(lines - 1, 0, -1):
        for a in (1, 0):
            for first in order:
                rs_step(a, 0, d, first)
                rs_step(a, 1, d, first)

    for e in range(1, reps):
        rep_copy(e).wait_recv()
    summed = rep_slots[0]
    for e in range(1, reps):
        summed = summed + rep_slots[e]
    bias_sums[0] = summed
    z_slots[z] = summed
    for e in range(1, lines):
        zb_copy(e).start()

    @pl.when(lead)
    def _():
        pl.semaphore_wait(gate, 1)
        for s in range(1, PLANE):
            dq_copy(s).start()

    def finish(a, first):
        block = range(first, first + PAIR)
        for s in block:
            owns[a][s] = (owns[a][s] + chains[a][last_ref[z * PLANE + near(s)]]) * factors[a]
        for way in range(2):
            @pl.when(rs_inner(way))
            def _():
                rs_copy(a, way, 1, first).wait_recv()
                for s in block:
                    owns[a][s] += rs_recv[a, way, 0, s].astype(jnp.float32)

        for s in reversed(block):
            final[a, s] = owns[a][s].astype(jnp.bfloat16)
            if s:
                out_copy(a, s).start()
            else:
                out_stay(a).start()

    for s in order:
        finish(1, s)

    zb_all.wait_recv()
    summed = z_slots[0]
    for d in range(1, lines):
        summed = summed + z_slots[d]
    bias_sums[1] = summed

    def bias_rows(chip):
        return dbq_ref.at[pl.ds(pl.multiple_of(chip * group, group), group)]

    bias_stay = pltpu.make_async_copy(bias_sums.at[1], bias_rows(p), table_sem.at[0])
    bias_stay.start()

    def pb_copy(s):
        return remote(
            bias_sums.at[1], bias_rows(p), pb_sem.at[0], pb_sem.at[1], seq(z, near(s))
        )

    shares = bias_buf.at[pl.ds(0, (PLANE - 1) * group)]
    pb_all = remote(shares, shares, pb_sem.at[0], pb_sem.at[1], seq(z, p))
    for s in range(1, PLANE):
        pb_copy(s).start()

    for s in order:
        finish(0, s)

    for a in range(2):
        plane_sent(a).wait_send()
        for way in range(2):
            for d in range(1, lines):
                @pl.when(z + d < lines if way == 0 else z - d >= 0)
                def _():
                    sent(a, way, d - 1).wait_send()
    dq_stay.wait()
    dq_all.wait()
    for d in range(1, reps):
        rep_copy(d).wait_send()
    zb_all.wait_send()
    for a in range(2):
        out_stay(a).wait()
        out_all(a).wait()
    bias_stay.wait()
    pb_all.wait()


def fused(lists, counts, bias, q, g, k, v):
    n, reps = lax.axis_size("seq"), lax.axis_size("rep")
    rows, total = q.shape
    heads, width = bias.shape
    kv_count = k.shape[1] // width
    group = heads // kv_count
    assert reps % 2 == 0 and n % PLANE == 0 and kv_count == PLANE and group % 2 == 0
    lines = n // PLANE
    pairs = PLANE * group
    half, full = jnp.bfloat16, jnp.float32
    free = pl.BlockSpec(memory_space=pl.ANY)
    dma = pltpu.SemaphoreType.DMA
    block = rows * width
    need = 2 * block * (2 * n + 3 * pairs + 32 * (lines - 1) + 8 + 2 * kv_count)
    need += 4 * block * (2 * pairs + 2 * (pairs + 1) + 2 * PLANE)
    need += 8 * heads * width * (reps + lines)
    return pl.pallas_call(
        functools.partial(fused_kernel, group, width ** (-0.5)),
        in_specs=[pl.BlockSpec(memory_space=pltpu.HBM)] * 7,
        out_specs=[free] * 4,
        out_shape=[
            jax.ShapeDtypeStruct(q.shape, half),
            jax.ShapeDtypeStruct(k.shape, half),
            jax.ShapeDtypeStruct(v.shape, half),
            jax.ShapeDtypeStruct(bias.shape, full),
        ],
        scratch_shapes=[
            pltpu.SMEM(lists.shape, lists.dtype),
            pltpu.SMEM(counts.shape, counts.dtype),
            pltpu.VMEM(bias.shape, full),
            pltpu.VMEM(k.shape, half),
            pltpu.VMEM(v.shape, half),
            pltpu.VMEM((n, rows, width), half),
            pltpu.VMEM((n, rows, width), half),
            pltpu.VMEM((PLANE, rows, group * width), half),
            pltpu.VMEM((PLANE, rows, group * width), half),
            pltpu.VMEM((PLANE, rows, group * width), half),
            pltpu.VMEM((pairs, 2 * rows, rows), full),
            pltpu.VMEM((pairs + 1, rows, width), full),
            pltpu.VMEM((pairs + 1, rows, width), full),
            pltpu.VMEM((PLANE, rows, width), full),
            pltpu.VMEM((PLANE, rows, width), full),
            pltpu.VMEM((2, 2, lines - 1, PLANE, rows, width), half),
            pltpu.VMEM((2, 2, lines - 1, PLANE, rows, width), half),
            pltpu.VMEM((2, PLANE, rows, width), half),
            pltpu.VMEM((group, width), full),
            pltpu.VMEM((reps, group, width), full),
            pltpu.VMEM((lines, group, width), full),
            pltpu.VMEM((2, group, width), full),
            pltpu.SMEM((pairs,), jnp.int32),
            pltpu.SMEM((pairs,), jnp.int32),
            pltpu.SMEM((n,), jnp.int32),
            dma((3,)), dma((6,)),
            dma((2,)), dma((2, PLANE - 1)),
            dma((3,)), dma((2, PLANE)),
            dma((2, 2, lines - 1)), dma((2, 2, lines - 1, PLANE)),
            pltpu.SemaphoreType.REGULAR,
            dma((2, 2, lines - 1, PLANE // PAIR)), dma((3,)), dma((3, 2)),
            dma((reps - 1,)), dma((reps - 1,)),
            dma((2,)), dma((2,)),
        ],
        compiler_params=pltpu.CompilerParams(
            collective_id=1, has_side_effects=True, vmem_limit_bytes=need + 4 * 2**20
        ),
        name="fused",
    )(lists, counts, bias, q, g, k, v)


def place_kernel(*refs):
    count = len(refs) // 2
    sem = refs[-1]
    copies = [
        pltpu.make_async_copy(refs[a], refs[count + a], sem.at[a]) for a in range(count)
    ]
    for copy in copies:
        copy.start()
    for copy in copies:
        copy.wait()


def place(*arrays):
    spec = pl.BlockSpec(memory_space=pl.ANY)
    return pl.pallas_call(
        place_kernel,
        in_specs=[spec] * len(arrays),
        out_specs=[spec] * len(arrays),
        out_shape=[jax.ShapeDtypeStruct(one.shape, one.dtype) for one in arrays],
        scratch_shapes=[pltpu.SemaphoreType.DMA((len(arrays),))],
        compiler_params=pltpu.CompilerParams(vmem_limit_bytes=2**20),
        name="place",
    )(*arrays)


def body(q_lin, k_lin, value_projection, grad_out, q_bias, block_lists, block_counts):
    assert block_lists.shape[1] == lax.axis_size("seq") and block_lists.shape[2] == 2
    heads = block_lists.shape[0]
    args = (jnp.transpose(block_lists, (1, 2, 0)), block_counts.T, q_bias.reshape(heads, -1),
        q_lin[0], grad_out[0], k_lin[0], value_projection[0])
    args = [pltpu.with_memory_space_constraint(a, pltpu.HBM) for a in args]
    dq, dk, dv, dbq = fused(*args)
    dq, dk, dv, dbq = place(dq, dk, dv, dbq)
    return (dq[None], dk[None], dv[None], dbq.reshape(-1))


def solution(mesh):
    placed = (P("rep", "seq", None),) * 4 + (P(),) * 3
    return jax.shard_map(
        body,
        mesh=mesh,
        in_specs=placed,
        out_specs=(P("rep", "seq", None),) * 3 + (P(),),
        check_vma=False,
    )
```

```python
import functools

import jax
import jax.numpy as jnp
from jax import lax
from jax.experimental import pallas as pl
from jax.experimental.pallas import tpu as pltpu
from jax.sharding import PartitionSpec as P

NT = (((1,), (1,)), ((), ()))
TN = (((0,), (0,)), ((), ()))
NN = (((1,), (0,)), ((), ()))
MESH = pl.DeviceIdType.MESH
PLANE = 4
PAIR = 2


def dot(a, b, dims):
    return lax.dot_general(a, b, dims, preferred_element_type=jnp.float32)


def fused_kernel(
    group, scaling,
    lists_ref, count_ref, bias_ref, q_ref, g_ref, k_ref, v_ref,
    dq_ref, dk_ref, dv_ref, dbq_ref,
    lists_smem, count_smem, bias_buf,
    kbuf, vbuf, kall, vall, qbuf, gbuf, dqbuf, weights_buf, chain_k, chain_v, own_k, own_v,
    rs_send, rs_recv, final, bias_acc, rep_slots, z_slots, bias_sums,
    enc_ref, prev_ref, last_ref,
    table_sem, local_sem, plane_send, plane_recv, rows_send, rows_recv, z_send, z_recv,
    gate, rs_sem, dq_sem, out_sem, rep_send, rep_recv, zb_sem, pb_sem,
):
    me = lax.axis_index("seq")
    n = lax.axis_size("seq")
    reps, rep = lax.axis_size("rep"), lax.axis_index("rep")
    lines = n // PLANE
    z, p = me // PLANE, me % PLANE
    rows, width = kall.shape[1:]
    pairs = PLANE * group

    def near(s):
        return (p // 2 + s // 2) % 2 * 2 + (p % 2 + s % 2) % 2

    def seq(zz, pp):
        return {"seq": zz * PLANE + pp}

    def remote(src, dst, send, recv, target):
        return pltpu.make_async_remote_copy(
            src_ref=src, dst_ref=dst, send_sem=send, recv_sem=recv,
            device_id=target, device_id_type=MESH,
        )

    def cols(start, size):
        return pl.ds(pl.multiple_of(start * width, width), size * width)

    barrier = pltpu.get_barrier_semaphore()
    z_others = [lax.rem(z + d, lines) for d in range(1, lines)]
    rep_others = [lax.rem(rep + d, reps) for d in range(1, reps)]
    for s in range(1, PLANE):
        pl.semaphore_signal(barrier, inc=1, device_id=seq(z, near(s)), device_id_type=MESH)
    for zz in z_others:
        pl.semaphore_signal(barrier, inc=1, device_id=seq(zz, p), device_id_type=MESH)
    for rr in rep_others:
        pl.semaphore_signal(barrier, inc=1, device_id={"rep": rr}, device_id_type=MESH)
    own_kv = [
        pltpu.make_async_copy(src.at[:, cols(p, 1)], dst.at[me], local_sem.at[a])
        for a, (src, dst) in enumerate([(k_ref, kall), (v_ref, vall)])
    ]
    own_rows = [
        pltpu.make_async_copy(src.at[:, cols(p * group, group)], dst.at[0], local_sem.at[2 + a])
        for a, (src, dst) in enumerate([(q_ref, qbuf), (g_ref, gbuf)])
    ]
    tables = [
        pltpu.make_async_copy(lists_ref, lists_smem, table_sem.at[0]),
        pltpu.make_async_copy(count_ref, count_smem, table_sem.at[1]),
    ]
    bias_copy = pltpu.make_async_copy(bias_ref, bias_buf, table_sem.at[2])
    ahead = [
        pltpu.make_async_copy(src, dst, local_sem.at[4 + a])
        for a, (src, dst) in enumerate([(k_ref, kbuf), (v_ref, vbuf)])
    ]
    for copy in ahead + own_kv + tables + own_rows + [bias_copy]:
        copy.start()

    pl.semaphore_wait(barrier, PLANE - 1 + lines - 1 + reps - 1)

    def plane_copy(a, s):
        src, dst = [(kbuf, kall), (vbuf, vall)][a]
        return remote(
            src.at[:, cols(near(s), 1)], dst.at[me],
            plane_send.at[a], plane_recv.at[a, s - 1], seq(z, near(s)),
        )

    def plane_sent(a):
        blocks = [kall, vall][a].at[pl.ds(0, PLANE - 1)]
        return remote(blocks, blocks, plane_send.at[a], plane_recv.at[a, 0], seq(z, p))

    lead = rep % 2 == 0
    follow = rep % 2 == 1

    def tell_partner():
        pl.semaphore_signal(
            gate, inc=1, device_id={"rep": rep // 2 * 2 + 1 - rep % 2}, device_id_type=MESH
        )

    for copy in ahead:
        copy.wait()

    def plane_start():
        for a in range(2):
            for s in range(1, PLANE):
                plane_copy(a, s).start()

    pl.when(lead)(plane_start)

    def rows_copy(a, s, first=0, count=group):
        src, dst = [(q_ref, qbuf), (g_ref, gbuf)][a]
        which = s - 1 if first == 0 else PLANE - 1
        return remote(
            src.at[:, cols(near(s) * group + first, count)],
            dst.at[s, :, first * width : (first + count) * width],
            rows_send.at[a if s < PLANE - 1 or a == 0 else 2], rows_recv.at[a, which],
            seq(z, near(s)),
        )

    def rows_sent(which):
        block = [
            qbuf.at[pl.ds(1, PLANE - 1)], gbuf.at[pl.ds(1, PLANE - 2)], gbuf.at[PLANE - 1]
        ][which]
        remote(block, block, rows_send.at[which], rows_recv.at[0, 0], seq(z, p)).wait_send()

    half_group = group // 2
    last_rows = [(0, half_group), (half_group, group - half_group)]
    def rows_start():
        for s in range(1, PLANE - 1):
            rows_copy(0, s).start()
        for s in range(1, PLANE - 1):
            rows_copy(1, s).start()
        rows_copy(0, PLANE - 1).start()
        for first, count in last_rows:
            rows_copy(1, PLANE - 1, first, count).start()

    def z_block(a, place, s):
        return [kall, vall][a].at[place * PLANE + near(s)]

    def z_copy(a, way, d, s):
        block = z_block(a, z - d if way == 0 else z + d, s)
        return remote(
            block, block, z_send.at[a, way, d], z_recv.at[a, way, d, s],
            seq(z + 1 if way == 0 else z - 1, p),
        )

    def goes(way, d):
        if way == 0:
            return (z + 1 < lines) & (z - d >= 0)
        return (z - 1 >= 0) & (z + d < lines)

    def z_start(a, d, s):
        for way in range(2):
            @pl.when(goes(way, d))
            def _():
                z_copy(a, way, d, s).start()

    def z_relay(a, d):
        for s in range(PLANE):
            for way in range(2):
                @pl.when(z - d >= 0 if way == 0 else z + d < lines)
                def _():
                    block = z_block(a, z - d if way == 0 else z + d, s)
                    remote(
                        block, block, z_send.at[a, way, d - 1], z_recv.at[a, way, d - 1, s],
                        seq(z, p),
                    ).wait_recv()

            if d < lines - 1:
                z_start(a, d, s)

    def z_own(a, s, who, which=None):
        for way in range(2):
            wanted = goes(way, 0) & who
            if which is not None:
                wanted = wanted & (goes(way, 1) if which else jnp.logical_not(goes(way, 1)))

            @pl.when(wanted)
            def _():
                z_copy(a, way, 0, s).start()

    own_kv[0].wait()
    z_own(0, 0, lead)

    for copy in tables:
        copy.wait()

    def read_table(t, _):
        position = z * PLANE + near(t // group)
        head = p * group + t % group
        other = jnp.clip(lists_smem[position, 1, head], 0, n - 1)
        enc_ref[t] = jnp.where(count_smem[position, head] != 1, other, n)
        return 0

    lax.fori_loop(0, pairs, read_table, 0)
    pl.when(lead)(rows_start)

    def link_pair(t, _):
        code = enc_ref[t]
        found = jnp.int32(0)
        for u in range(pairs):
            same = (enc_ref[u] == code) & (u < t)
            found = jnp.where(same, u + 1, found)
        prev_ref[t] = found
        return 0

    def link_block(j, _):
        found = jnp.int32(0)
        for u in range(pairs):
            found = jnp.where(enc_ref[u] == j, u + 1, found)
        last_ref[j] = found
        return 0

    lax.fori_loop(0, pairs, link_pair, 0)
    pl.when(follow)(plane_start)
    for s in range(1, PLANE):
        plane_copy(0, s).wait_recv()
        z_own(0, s, lead)
    own_kv[1].wait()
    for s in range(PLANE):
        if s:
            plane_copy(1, s).wait_recv()
        z_own(1, s, lead, False)
    lax.fori_loop(0, n, link_block, 0)
    chain_k[0] = jnp.zeros((rows, width), jnp.float32)
    chain_v[0] = jnp.zeros((rows, width), jnp.float32)
    own_k[...] = jnp.zeros_like(own_k)
    own_v[...] = jnp.zeros_like(own_v)
    bias_acc[...] = jnp.zeros_like(bias_acc)

    @pl.when(follow)
    def _():
        pl.semaphore_wait(gate, 1)
        rows_start()

    for s in range(PLANE):
        z_own(0, s, follow)
    for s in range(PLANE):
        z_own(1, s, follow, False)
    for d in range(1, lines):
        if d == lines - 1:
            @pl.when(lead)
            def _():
                rows_sent(0)
                rows_sent(1)
                tell_partner()

        z_relay(0, d)
        if d == 1:
            for s in range(PLANE):
                z_own(1, s, True, True)
        elif d < lines - 1:
            z_relay(1, d - 1)

    for copy in own_rows:
        copy.wait()
    bias_copy.wait()

    def both(ref, s, t):
        code = enc_ref[t]
        other = jnp.where(code < n, code, 0)
        return jnp.concatenate([ref[z * PLANE + near(s)], ref[other]], axis=0), code

    def lanes_of(h):
        return slice(h * width, (h + 1) * width)

    def soften(s):
        for h in range(group):
            t, lanes = s * group + h, lanes_of(h)
            queries = (
                qbuf[s, :, lanes].astype(jnp.float32) + bias_buf[pl.ds(p * group + h, 1), :]
            ).astype(jnp.bfloat16)
            qbuf[s, :, lanes] = queries
            keys, code = both(kall, s, t)
            scores = dot(keys, queries, NT) * scaling
            first = scores[:rows]
            second = scores[rows:] + jnp.where(code < n, 0.0, -1.0e30)
            top = jnp.maximum(
                jnp.max(first, axis=0, keepdims=True), jnp.max(second, axis=0, keepdims=True)
            )
            first, second = jnp.exp(first - top), jnp.exp(second - top)
            total = jnp.sum(first, axis=0, keepdims=True) + jnp.sum(second, axis=0, keepdims=True)
            scale_to = 1.0 / total
            weights_buf[t, :rows] = first * scale_to
            weights_buf[t, rows:] = second * scale_to

    def dq_copy(s):
        return remote(
            dqbuf.at[s], dq_ref.at[:, cols(p * group, group)],
            dq_sem.at[0], dq_sem.at[1], seq(z, near(s)),
        )

    dq_stay = pltpu.make_async_copy(dqbuf.at[0], dq_ref.at[:, cols(p * group, group)], dq_sem.at[2])
    others = dqbuf.at[pl.ds(1, PLANE - 1)]
    dq_all = remote(others, others, dq_sem.at[0], dq_sem.at[1], seq(z, p))

    def grad_values(s, heads):
        more_v = None
        for h in heads:
            t = s * group + h
            part_v = dot(weights_buf[t].astype(jnp.bfloat16), gbuf[s, :, lanes_of(h)], NN)
            chain_v[t + 1] = part_v[rows:] + chain_v[prev_ref[t]]
            more_v = part_v[:rows] if more_v is None else more_v + part_v[:rows]
        own_v[s] += more_v

    def grad_keys(s, heads):
        more_k = None
        held = []
        for h in heads:
            values, _ = both(vall, s, s * group + h)
            held.append(dot(values, gbuf[s, :, lanes_of(h)], NT))
        for h, weight_grads in zip(heads, held):
            t, lanes = s * group + h, lanes_of(h)
            keys, _ = both(kall, s, t)
            weights = weights_buf[t]
            half = weights.astype(jnp.bfloat16)
            row_dots = jnp.sum(half.astype(jnp.float32) * weight_grads, axis=0, keepdims=True)
            score_grads = (weights * (weight_grads - row_dots)).astype(jnp.bfloat16)
            grad_q = scaling * dot(score_grads, keys, TN)
            dqbuf[s, :, lanes] = grad_q.astype(jnp.bfloat16)
            bias_acc[h : h + 1, :] += jnp.sum(grad_q, axis=0, keepdims=True)
            part_k = dot(score_grads, qbuf[s, :, lanes], NN)
            chain_k[t + 1] = part_k[rows:] + chain_k[prev_ref[t]]
            more_k = part_k[:rows] if more_k is None else more_k + part_k[:rows]
        own_k[s] += more_k

    every = list(range(group))
    early = []
    for s in range(PLANE - 1):
        early.append((0, s))
        early.append((1, s))
    early.append((0, PLANE - 1))

    def run(kind, s):
        if s:
            rows_copy(kind, s).wait_recv()
        if kind == 0:
            soften(s)
        else:
            grad_values(s, every)

    for kind, s in early[:2]:
        run(kind, s)
    z_relay(1, lines - 2)
    for kind, s in early[2:5]:
        run(kind, s)
    z_relay(1, lines - 1)

    def dq_start(s):
        @pl.when(follow)
        def _():
            dq_copy(s).start()

    for s in range(PLANE - 1):
        if s == PLANE - 2:
            run(*early[5])
        grad_keys(s, every)
        if s:
            dq_start(s)
        else:
            dq_stay.start()
    run(*early[6])
    def sent(a, way, d):
        blocks = [kall, vall][a].at[pl.ds(0, PLANE)]
        return remote(blocks, blocks, z_send.at[a, way, d], z_recv.at[a, way, d, 0], seq(z, p))

    for a in range(2):
        for way in range(2):
            for d in range(lines - 1):
                @pl.when(goes(way, d))
                def _():
                    sent(a, way, d).wait_send()

    factors = [scaling, 1.0]
    chains = [chain_k, chain_v]
    owns = [own_k, own_v]
    order = range(PLANE - PAIR, -1, -PAIR)

    def rs_copy(a, way, d, first):
        pair = pl.ds(first, PAIR)
        return remote(
            rs_send.at[a, way, d - 1, pair], rs_recv.at[a, way, d - 1, pair],
            z_send.at[a, way, d - 1], rs_sem.at[a, way, d - 1, first // PAIR],
            seq(z + 1 if way == 0 else z - 1, p),
        )

    def rs_inner(way):
        return z >= 1 if way == 0 else z + 1 < lines

    def rs_step(a, way, d, first):
        target = z + d if way == 0 else z - d
        inside = target < lines if way == 0 else target >= 0

        def part(s):
            return chains[a][last_ref[target * PLANE + near(s)]] * factors[a]

        if d < lines - 1:
            @pl.when(inside & rs_inner(way))
            def _():
                rs_copy(a, way, d + 1, first).wait_recv()
                for s in range(first, first + PAIR):
                    rs_send[a, way, d - 1, s] = (
                        part(s) + rs_recv[a, way, d, s].astype(jnp.float32)
                    ).astype(jnp.bfloat16)
                rs_copy(a, way, d, first).start()

            inside = inside & jnp.logical_not(rs_inner(way))

        @pl.when(inside)
        def _():
            for s in range(first, first + PAIR):
                rs_send[a, way, d - 1, s] = part(s).astype(jnp.bfloat16)
            rs_copy(a, way, d, first).start()

    for part, (first, count) in enumerate(last_rows):
        heads = range(first, first + count)
        rows_copy(1, PLANE - 1, first, count).wait_recv()
        grad_values(PLANE - 1, heads)
        if part == len(last_rows) - 1:
            for block in order:
                for way in range(2):
                    rs_step(1, way, lines - 1, block)
        grad_keys(PLANE - 1, heads)
    dq_start(PLANE - 1)
    rows_sent(2)

    @pl.when(follow)
    def _():
        rows_sent(0)
        rows_sent(1)
        tell_partner()

    rep_slots[rep] = bias_acc[...]

    def rep_copy(d):
        return remote(
            bias_acc, rep_slots.at[rep], rep_send.at[d - 1], rep_recv.at[d - 1],
            {"rep": rep_others[d - 1]},
        )

    for d in range(1, reps):
        rep_copy(d).start()

    def out_copy(a, s):
        return remote(
            final.at[a, s], [dk_ref, dv_ref][a].at[:, cols(p, 1)],
            out_sem.at[0, a], out_sem.at[1, a], seq(z, near(s)),
        )

    def out_all(a):
        blocks = final.at[a, pl.ds(1, PLANE - 1)]
        return remote(blocks, blocks, out_sem.at[0, a], out_sem.at[1, a], seq(z, p))

    def out_stay(a):
        return pltpu.make_async_copy(
            final.at[a, 0], [dk_ref, dv_ref][a].at[:, cols(p, 1)], out_sem.at[2, a]
        )

    def zb_copy(d):
        return remote(
            bias_sums.at[0], z_slots.at[z], zb_sem.at[0], zb_sem.at[1],
            seq(z_others[d - 1], p),
        )

    slots = z_slots.at[pl.ds(0, lines - 1)]
    zb_all = remote(slots, slots, zb_sem.at[0], zb_sem.at[1], seq(z, p))

    for d in range(lines - 1, 0, -1):
        for a in (1, 0):
            for first in order if d < lines - 1 or a == 0 else ():
                rs_step(a, 0, d, first)
                rs_step(a, 1, d, first)

    for e in range(1, reps):
        rep_copy(e).wait_recv()
    summed = rep_slots[0]
    for e in range(1, reps):
        summed = summed + rep_slots[e]
    bias_sums[0] = summed
    z_slots[z] = summed
    for e in range(1, lines):
        zb_copy(e).start()

    @pl.when(lead)
    def _():
        pl.semaphore_wait(gate, 1)
        for s in range(1, PLANE):
            dq_copy(s).start()

    def finish(a, first):
        block = range(first, first + PAIR)
        for s in block:
            owns[a][s] = (owns[a][s] + chains[a][last_ref[z * PLANE + near(s)]]) * factors[a]
        for way in range(2):
            @pl.when(rs_inner(way))
            def _():
                rs_copy(a, way, 1, first).wait_recv()
                for s in block:
                    owns[a][s] += rs_recv[a, way, 0, s].astype(jnp.float32)

        for s in reversed(block):
            final[a, s] = owns[a][s].astype(jnp.bfloat16)
            if s:
                out_copy(a, s).start()
            else:
                out_stay(a).start()

    for s in order:
        finish(1, s)

    zb_all.wait_recv()
    summed = z_slots[0]
    for d in range(1, lines):
        summed = summed + z_slots[d]
    bias_sums[1] = summed

    def bias_rows(chip):
        return dbq_ref.at[pl.ds(pl.multiple_of(chip * group, group), group)]

    bias_stay = pltpu.make_async_copy(bias_sums.at[1], bias_rows(p), table_sem.at[0])
    bias_stay.start()

    def pb_copy(s):
        return remote(
            bias_sums.at[1], bias_rows(p), pb_sem.at[0], pb_sem.at[1], seq(z, near(s))
        )

    shares = bias_buf.at[pl.ds(0, (PLANE - 1) * group)]
    pb_all = remote(shares, shares, pb_sem.at[0], pb_sem.at[1], seq(z, p))
    for s in range(1, PLANE):
        pb_copy(s).start()

    for s in order:
        finish(0, s)

    for a in range(2):
        plane_sent(a).wait_send()
        for way in range(2):
            for d in range(1, lines):
                @pl.when(z + d < lines if way == 0 else z - d >= 0)
                def _():
                    sent(a, way, d - 1).wait_send()
    dq_stay.wait()
    dq_all.wait()
    for d in range(1, reps):
        rep_copy(d).wait_send()
    zb_all.wait_send()
    for a in range(2):
        out_stay(a).wait()
        out_all(a).wait()
    bias_stay.wait()
    pb_all.wait()


def fused(lists, counts, bias, q, g, k, v):
    n, reps = lax.axis_size("seq"), lax.axis_size("rep")
    rows, total = q.shape
    heads, width = bias.shape
    kv_count = k.shape[1] // width
    group = heads // kv_count
    assert reps % 2 == 0 and n % PLANE == 0 and kv_count == PLANE and group % 2 == 0
    lines = n // PLANE
    pairs = PLANE * group
    half, full = jnp.bfloat16, jnp.float32
    free = pl.BlockSpec(memory_space=pl.ANY)
    dma = pltpu.SemaphoreType.DMA
    block = rows * width
    need = 2 * block * (2 * n + 3 * pairs + 32 * (lines - 1) + 8 + 2 * kv_count)
    need += 4 * block * (2 * pairs + 2 * (pairs + 1) + 2 * PLANE)
    need += 8 * heads * width * (reps + lines)
    return pl.pallas_call(
        functools.partial(fused_kernel, group, width ** (-0.5)),
        in_specs=[pl.BlockSpec(memory_space=pltpu.HBM)] * 7,
        out_specs=[free] * 4,
        out_shape=[
            jax.ShapeDtypeStruct(q.shape, half),
            jax.ShapeDtypeStruct(k.shape, half),
            jax.ShapeDtypeStruct(v.shape, half),
            jax.ShapeDtypeStruct(bias.shape, full),
        ],
        scratch_shapes=[
            pltpu.SMEM(lists.shape, lists.dtype),
            pltpu.SMEM(counts.shape, counts.dtype),
            pltpu.VMEM(bias.shape, full),
            pltpu.VMEM(k.shape, half),
            pltpu.VMEM(v.shape, half),
            pltpu.VMEM((n, rows, width), half),
            pltpu.VMEM((n, rows, width), half),
            pltpu.VMEM((PLANE, rows, group * width), half),
            pltpu.VMEM((PLANE, rows, group * width), half),
            pltpu.VMEM((PLANE, rows, group * width), half),
            pltpu.VMEM((pairs, 2 * rows, rows), full),
            pltpu.VMEM((pairs + 1, rows, width), full),
            pltpu.VMEM((pairs + 1, rows, width), full),
            pltpu.VMEM((PLANE, rows, width), full),
            pltpu.VMEM((PLANE, rows, width), full),
            pltpu.VMEM((2, 2, lines - 1, PLANE, rows, width), half),
            pltpu.VMEM((2, 2, lines - 1, PLANE, rows, width), half),
            pltpu.VMEM((2, PLANE, rows, width), half),
            pltpu.VMEM((group, width), full),
            pltpu.VMEM((reps, group, width), full),
            pltpu.VMEM((lines, group, width), full),
            pltpu.VMEM((2, group, width), full),
            pltpu.SMEM((pairs,), jnp.int32),
            pltpu.SMEM((pairs,), jnp.int32),
            pltpu.SMEM((n,), jnp.int32),
            dma((3,)), dma((6,)),
            dma((2,)), dma((2, PLANE - 1)),
            dma((3,)), dma((2, PLANE)),
            dma((2, 2, lines - 1)), dma((2, 2, lines - 1, PLANE)),
            pltpu.SemaphoreType.REGULAR,
            dma((2, 2, lines - 1, PLANE // PAIR)), dma((3,)), dma((3, 2)),
            dma((reps - 1,)), dma((reps - 1,)),
            dma((2,)), dma((2,)),
        ],
        compiler_params=pltpu.CompilerParams(
            collective_id=1, has_side_effects=True, vmem_limit_bytes=need + 4 * 2**20
        ),
        name="fused",
    )(lists, counts, bias, q, g, k, v)


def place_kernel(*refs):
    count = len(refs) // 2
    sem = refs[-1]
    copies = [
        pltpu.make_async_copy(refs[a], refs[count + a], sem.at[a]) for a in range(count)
    ]
    for copy in copies:
        copy.start()
    for copy in copies:
        copy.wait()


def place(*arrays):
    spec = pl.BlockSpec(memory_space=pl.ANY)
    return pl.pallas_call(
        place_kernel,
        in_specs=[spec] * len(arrays),
        out_specs=[spec] * len(arrays),
        out_shape=[jax.ShapeDtypeStruct(one.shape, one.dtype) for one in arrays],
        scratch_shapes=[pltpu.SemaphoreType.DMA((len(arrays),))],
        compiler_params=pltpu.CompilerParams(vmem_limit_bytes=2**20),
        name="place",
    )(*arrays)


def body(q_lin, k_lin, value_projection, grad_out, q_bias, block_lists, block_counts):
    assert block_lists.shape[1] == lax.axis_size("seq") and block_lists.shape[2] == 2
    heads = block_lists.shape[0]
    args = (jnp.transpose(block_lists, (1, 2, 0)), block_counts.T, q_bias.reshape(heads, -1),
        q_lin[0], grad_out[0], k_lin[0], value_projection[0])
    args = [pltpu.with_memory_space_constraint(a, pltpu.HBM) for a in args]
    dq, dk, dv, dbq = fused(*args)
    dq, dk, dv, dbq = place(dq, dk, dv, dbq)
    return (dq[None], dk[None], dv[None], dbq.reshape(-1))


def solution(mesh):
    placed = (P("rep", "seq", None),) * 4 + (P(),) * 3
    return jax.shard_map(
        body,
        mesh=mesh,
        in_specs=placed,
        out_specs=(P("rep", "seq", None),) * 3 + (P(),),
        check_vma=False,
    )
```

```python
import functools

import jax
import jax.numpy as jnp
from jax import lax
from jax.experimental import pallas as pl
from jax.experimental.pallas import tpu as pltpu
from jax.sharding import PartitionSpec as P

NT = (((1,), (1,)), ((), ()))
TN = (((0,), (0,)), ((), ()))
NN = (((1,), (0,)), ((), ()))
MESH = pl.DeviceIdType.MESH
PLANE = 4
PAIR = 2


def dot(a, b, dims):
    return lax.dot_general(a, b, dims, preferred_element_type=jnp.float32)


def fused_kernel(
    group, scaling,
    lists_ref, count_ref, bias_ref, q_ref, g_ref, k_ref, v_ref,
    dq_ref, dk_ref, dv_ref, dbq_ref,
    lists_smem, count_smem, bias_buf,
    kbuf, vbuf, kall, vall, qbuf, gbuf, dqbuf, weights_buf, chain_k, chain_v, own_k, own_v,
    rs_send, rs_recv, final, bias_acc, rep_slots, z_slots, bias_sums,
    enc_ref, prev_ref, last_ref,
    table_sem, local_sem, plane_send, plane_recv, rows_send, rows_recv, z_send, z_recv,
    gate, rs_sem, dq_sem, out_sem, rep_send, rep_recv, zb_sem, pb_sem,
):
    me = lax.axis_index("seq")
    n = lax.axis_size("seq")
    reps, rep = lax.axis_size("rep"), lax.axis_index("rep")
    lines = n // PLANE
    z, p = me // PLANE, me % PLANE
    rows, width = kall.shape[1:]
    pairs = PLANE * group

    def near(s):
        return (p // 2 + s // 2) % 2 * 2 + (p % 2 + s % 2) % 2

    def seq(zz, pp):
        return {"seq": zz * PLANE + pp}

    def remote(src, dst, send, recv, target):
        return pltpu.make_async_remote_copy(
            src_ref=src, dst_ref=dst, send_sem=send, recv_sem=recv,
            device_id=target, device_id_type=MESH,
        )

    def cols(start, size):
        return pl.ds(pl.multiple_of(start * width, width), size * width)

    barrier = pltpu.get_barrier_semaphore()
    z_others = [lax.rem(z + d, lines) for d in range(1, lines)]
    rep_others = [lax.rem(rep + d, reps) for d in range(1, reps)]
    for s in range(1, PLANE):
        pl.semaphore_signal(barrier, inc=1, device_id=seq(z, near(s)), device_id_type=MESH)
    for zz in z_others:
        pl.semaphore_signal(barrier, inc=1, device_id=seq(zz, p), device_id_type=MESH)
    for rr in rep_others:
        pl.semaphore_signal(barrier, inc=1, device_id={"rep": rr}, device_id_type=MESH)
    own_kv = [
        pltpu.make_async_copy(src.at[:, cols(p, 1)], dst.at[me], local_sem.at[a])
        for a, (src, dst) in enumerate([(k_ref, kall), (v_ref, vall)])
    ]
    own_rows = [
        pltpu.make_async_copy(src.at[:, cols(p * group, group)], dst.at[0], local_sem.at[2 + a])
        for a, (src, dst) in enumerate([(q_ref, qbuf), (g_ref, gbuf)])
    ]
    tables = [
        pltpu.make_async_copy(lists_ref, lists_smem, table_sem.at[0]),
        pltpu.make_async_copy(count_ref, count_smem, table_sem.at[1]),
    ]
    bias_copy = pltpu.make_async_copy(bias_ref, bias_buf, table_sem.at[2])
    ahead = [
        pltpu.make_async_copy(src, dst, local_sem.at[4 + a])
        for a, (src, dst) in enumerate([(k_ref, kbuf), (v_ref, vbuf)])
    ]
    for copy in ahead + own_kv + tables + own_rows + [bias_copy]:
        copy.start()

    pl.semaphore_wait(barrier, PLANE - 1 + lines - 1 + reps - 1)

    def plane_copy(a, s):
        src, dst = [(kbuf, kall), (vbuf, vall)][a]
        return remote(
            src.at[:, cols(near(s), 1)], dst.at[me],
            plane_send.at[a], plane_recv.at[a, s - 1], seq(z, near(s)),
        )

    def plane_sent(a):
        blocks = [kall, vall][a].at[pl.ds(0, PLANE - 1)]
        return remote(blocks, blocks, plane_send.at[a], plane_recv.at[a, 0], seq(z, p))

    lead = rep % 2 == 0
    follow = rep % 2 == 1

    def tell_partner():
        pl.semaphore_signal(
            gate, inc=1, device_id={"rep": rep // 2 * 2 + 1 - rep % 2}, device_id_type=MESH
        )

    for copy in ahead:
        copy.wait()

    def plane_start():
        for a in range(2):
            for s in range(1, PLANE):
                plane_copy(a, s).start()

    pl.when(lead)(plane_start)

    def rows_copy(a, s, first=0, count=group):
        src, dst = [(q_ref, qbuf), (g_ref, gbuf)][a]
        which = s - 1 if first == 0 else PLANE - 1
        return remote(
            src.at[:, cols(near(s) * group + first, count)],
            dst.at[s, :, first * width : (first + count) * width],
            rows_send.at[a if s < PLANE - 1 or a == 0 else 2], rows_recv.at[a, which],
            seq(z, near(s)),
        )

    def rows_sent(which):
        block = [
            qbuf.at[pl.ds(1, PLANE - 1)], gbuf.at[pl.ds(1, PLANE - 2)], gbuf.at[PLANE - 1]
        ][which]
        remote(block, block, rows_send.at[which], rows_recv.at[0, 0], seq(z, p)).wait_send()

    half_group = group // 2
    last_rows = [(0, half_group), (half_group, group - half_group)]
    def rows_start():
        for s in range(1, PLANE - 1):
            rows_copy(0, s).start()
        for s in range(1, PLANE - 1):
            rows_copy(1, s).start()
        rows_copy(0, PLANE - 1).start()
        for first, count in last_rows:
            rows_copy(1, PLANE - 1, first, count).start()

    def z_block(a, place, s):
        return [kall, vall][a].at[place * PLANE + near(s)]

    def z_slot(d, s):
        return d * PLANE + (s if d < lines - 2 else 0)

    def z_copy(a, way, d, s):
        block = z_block(a, z - d if way == 0 else z + d, s)
        return remote(
            block, block, z_send.at[a, way, d], z_recv.at[a, way, z_slot(d, s)],
            seq(z + 1 if way == 0 else z - 1, p),
        )

    def goes(way, d):
        if way == 0:
            return (z + 1 < lines) & (z - d >= 0)
        return (z - 1 >= 0) & (z + d < lines)

    def z_start(a, d, s):
        for way in range(2):
            @pl.when(goes(way, d))
            def _():
                z_copy(a, way, d, s).start()

    def z_relay(a, d):
        if d == lines - 1:
            for way in range(2):
                @pl.when(z - d >= 0 if way == 0 else z + d < lines)
                def _():
                    where = z - d if way == 0 else z + d
                    shard = [kall, vall][a].at[pl.ds(where * PLANE, PLANE)]
                    remote(
                        shard, shard, z_send.at[a, way, d - 1], z_recv.at[a, way, z_slot(d - 1, 0)],
                        seq(z, p),
                    ).wait_recv()

            return
        for s in range(PLANE):
            for way in range(2):
                @pl.when(z - d >= 0 if way == 0 else z + d < lines)
                def _():
                    block = z_block(a, z - d if way == 0 else z + d, s)
                    remote(
                        block, block, z_send.at[a, way, d - 1], z_recv.at[a, way, z_slot(d - 1, s)],
                        seq(z, p),
                    ).wait_recv()

            z_start(a, d, s)

    def z_own(a, s, who, which=None):
        for way in range(2):
            wanted = goes(way, 0) & who
            if which is not None:
                wanted = wanted & (goes(way, 1) if which else jnp.logical_not(goes(way, 1)))

            @pl.when(wanted)
            def _():
                z_copy(a, way, 0, s).start()

    own_kv[0].wait()
    z_own(0, 0, lead)

    for copy in tables:
        copy.wait()

    def read_table(t, _):
        position = z * PLANE + near(t // group)
        head = p * group + t % group
        other = jnp.clip(lists_smem[position, 1, head], 0, n - 1)
        enc_ref[t] = jnp.where(count_smem[position, head] != 1, other, n)
        return 0

    lax.fori_loop(0, pairs, read_table, 0)
    pl.when(lead)(rows_start)

    def link_pair(t, _):
        code = enc_ref[t]
        found = jnp.int32(0)
        for u in range(pairs):
            same = (enc_ref[u] == code) & (u < t)
            found = jnp.where(same, u + 1, found)
        prev_ref[t] = found
        return 0

    def link_block(j, _):
        found = jnp.int32(0)
        for u in range(pairs):
            found = jnp.where(enc_ref[u] == j, u + 1, found)
        last_ref[j] = found
        return 0

    lax.fori_loop(0, pairs, link_pair, 0)
    pl.when(follow)(plane_start)
    for s in range(1, PLANE):
        plane_copy(0, s).wait_recv()
        z_own(0, s, lead)
    own_kv[1].wait()
    for s in range(PLANE):
        if s:
            plane_copy(1, s).wait_recv()
        z_own(1, s, lead)
    lax.fori_loop(0, n, link_block, 0)
    chain_k[0] = jnp.zeros((rows, width), jnp.float32)
    chain_v[0] = jnp.zeros((rows, width), jnp.float32)
    own_k[...] = jnp.zeros_like(own_k)
    own_v[...] = jnp.zeros_like(own_v)
    bias_acc[...] = jnp.zeros_like(bias_acc)

    @pl.when(follow)
    def _():
        pl.semaphore_wait(gate, 1)
        rows_start()
        pl.semaphore_wait(gate, 1)

    for s in range(PLANE):
        z_own(0, s, follow)
    for s in range(PLANE):
        z_own(1, s, follow, False)
    for d in range(1, lines):
        if d == lines - 1:
            @pl.when(lead)
            def _():
                rows_sent(0)
                rows_sent(1)
                tell_partner()

        z_relay(0, d)
        if d == 1:
            for s in range(PLANE):
                z_own(1, s, follow, True)
        elif d < lines - 1:
            z_relay(1, d - 1)

    for copy in own_rows:
        copy.wait()
    bias_copy.wait()

    def both(ref, s, t):
        code = enc_ref[t]
        other = jnp.where(code < n, code, 0)
        return jnp.concatenate([ref[z * PLANE + near(s)], ref[other]], axis=0), code

    def lanes_of(h):
        return slice(h * width, (h + 1) * width)

    def soften(s):
        for h in range(group):
            t, lanes = s * group + h, lanes_of(h)
            queries = (
                qbuf[s, :, lanes].astype(jnp.float32) + bias_buf[pl.ds(p * group + h, 1), :]
            ).astype(jnp.bfloat16)
            qbuf[s, :, lanes] = queries
            keys, code = both(kall, s, t)
            scores = dot(keys, queries, NT) * scaling
            first = scores[:rows]
            second = scores[rows:] + jnp.where(code < n, 0.0, -1.0e30)
            top = jnp.maximum(
                jnp.max(first, axis=0, keepdims=True), jnp.max(second, axis=0, keepdims=True)
            )
            first, second = jnp.exp(first - top), jnp.exp(second - top)
            total = jnp.sum(first, axis=0, keepdims=True) + jnp.sum(second, axis=0, keepdims=True)
            scale_to = 1.0 / total
            weights_buf[t, :rows] = first * scale_to
            weights_buf[t, rows:] = second * scale_to

    def dq_copy(s):
        return remote(
            dqbuf.at[s], dq_ref.at[:, cols(p * group, group)],
            dq_sem.at[0], dq_sem.at[1], seq(z, near(s)),
        )

    dq_stay = pltpu.make_async_copy(dqbuf.at[0], dq_ref.at[:, cols(p * group, group)], dq_sem.at[2])
    others = dqbuf.at[pl.ds(1, PLANE - 1)]
    dq_all = remote(others, others, dq_sem.at[0], dq_sem.at[1], seq(z, p))

    def grad_values(s, heads):
        more_v = None
        for h in heads:
            t = s * group + h
            part_v = dot(weights_buf[t].astype(jnp.bfloat16), gbuf[s, :, lanes_of(h)], NN)
            chain_v[t + 1] = part_v[rows:] + chain_v[prev_ref[t]]
            more_v = part_v[:rows] if more_v is None else more_v + part_v[:rows]
        own_v[s] += more_v

    def grad_keys(s, heads):
        more_k = None
        held = []
        for h in heads:
            values, _ = both(vall, s, s * group + h)
            held.append(dot(values, gbuf[s, :, lanes_of(h)], NT))
        for h, weight_grads in zip(heads, held):
            t, lanes = s * group + h, lanes_of(h)
            keys, _ = both(kall, s, t)
            weights = weights_buf[t]
            half = weights.astype(jnp.bfloat16)
            row_dots = jnp.sum(half.astype(jnp.float32) * weight_grads, axis=0, keepdims=True)
            score_grads = (weights * (weight_grads - row_dots)).astype(jnp.bfloat16)
            grad_q = scaling * dot(score_grads, keys, TN)
            dqbuf[s, :, lanes] = grad_q.astype(jnp.bfloat16)
            bias_acc[h : h + 1, :] += jnp.sum(grad_q, axis=0, keepdims=True)
            part_k = dot(score_grads, qbuf[s, :, lanes], NN)
            chain_k[t + 1] = part_k[rows:] + chain_k[prev_ref[t]]
            more_k = part_k[:rows] if more_k is None else more_k + part_k[:rows]
        own_k[s] += more_k

    every = list(range(group))
    early = []
    for s in range(PLANE - 1):
        early.append((0, s))
        early.append((1, s))
    early.append((0, PLANE - 1))

    def run(kind, s):
        if s:
            rows_copy(kind, s).wait_recv()
        if kind == 0:
            soften(s)
        else:
            grad_values(s, every)

    pl.when(lead)(tell_partner)
    for kind, s in early[:2]:
        run(kind, s)
    z_relay(1, lines - 2)
    for kind, s in early[2:5]:
        run(kind, s)
    z_relay(1, lines - 1)

    def dq_start(s):
        @pl.when(follow)
        def _():
            dq_copy(s).start()

    for s in range(PLANE - 1):
        if s == PLANE - 2:
            run(*early[5])
        grad_keys(s, every)
        if s:
            dq_start(s)
        else:
            dq_stay.start()
    run(*early[6])
    def sent(a, way, d):
        blocks = [kall, vall][a].at[pl.ds(0, PLANE)]
        return remote(blocks, blocks, z_send.at[a, way, d], z_recv.at[a, way, 0], seq(z, p))

    for a in range(2):
        for way in range(2):
            for d in range(lines - 1):
                @pl.when(goes(way, d))
                def _():
                    sent(a, way, d).wait_send()

    factors = [scaling, 1.0]
    chains = [chain_k, chain_v]
    owns = [own_k, own_v]
    order = range(PLANE - PAIR, -1, -PAIR)

    def rs_copy(a, way, d, first):
        pair = pl.ds(first, PAIR)
        return remote(
            rs_send.at[a, way, d - 1, pair], rs_recv.at[a, way, d - 1, pair],
            z_send.at[a, way, d - 1], rs_sem.at[a, way, d - 1, first // PAIR],
            seq(z + 1 if way == 0 else z - 1, p),
        )

    def rs_inner(way):
        return z >= 1 if way == 0 else z + 1 < lines

    def rs_step(a, way, d, first):
        target = z + d if way == 0 else z - d
        inside = target < lines if way == 0 else target >= 0

        def part(s):
            return chains[a][last_ref[target * PLANE + near(s)]] * factors[a]

        if d < lines - 1:
            @pl.when(inside & rs_inner(way))
            def _():
                rs_copy(a, way, d + 1, first).wait_recv()
                for s in range(first, first + PAIR):
                    rs_send[a, way, d - 1, s] = (
                        part(s) + rs_recv[a, way, d, s].astype(jnp.float32)
                    ).astype(jnp.bfloat16)
                rs_copy(a, way, d, first).start()

            inside = inside & jnp.logical_not(rs_inner(way))

        @pl.when(inside)
        def _():
            for s in range(first, first + PAIR):
                rs_send[a, way, d - 1, s] = part(s).astype(jnp.bfloat16)
            rs_copy(a, way, d, first).start()

    for part, (first, count) in enumerate(last_rows):
        heads = range(first, first + count)
        rows_copy(1, PLANE - 1, first, count).wait_recv()
        if part == len(last_rows) - 1:
            @pl.when(follow)
            def _():
                for which in range(3):
                    rows_sent(which)
                tell_partner()

        grad_values(PLANE - 1, heads)
        if part == len(last_rows) - 1:
            for block in order:
                for way in range(2):
                    rs_step(1, way, lines - 1, block)
        grad_keys(PLANE - 1, heads)
    dq_start(PLANE - 1)
    pl.when(lead)(functools.partial(rows_sent, 2))

    rep_slots[rep] = bias_acc[...]

    def rep_copy(d):
        return remote(
            bias_acc, rep_slots.at[rep], rep_send.at[d - 1], rep_recv.at[d - 1],
            {"rep": rep_others[d - 1]},
        )

    for d in range(1, reps):
        rep_copy(d).start()

    def out_copy(a, s):
        return remote(
            final.at[a, s], [dk_ref, dv_ref][a].at[:, cols(p, 1)],
            out_sem.at[0, a], out_sem.at[1, a], seq(z, near(s)),
        )

    def out_all(a):
        blocks = final.at[a, pl.ds(1, PLANE - 1)]
        return remote(blocks, blocks, out_sem.at[0, a], out_sem.at[1, a], seq(z, p))

    def out_stay(a):
        return pltpu.make_async_copy(
            final.at[a, 0], [dk_ref, dv_ref][a].at[:, cols(p, 1)], out_sem.at[2, a]
        )

    def zb_copy(d):
        return remote(
            bias_sums.at[0], z_slots.at[z], zb_sem.at[0], zb_sem.at[1],
            seq(z_others[d - 1], p),
        )

    slots = z_slots.at[pl.ds(0, lines - 1)]
    zb_all = remote(slots, slots, zb_sem.at[0], zb_sem.at[1], seq(z, p))

    for d in range(lines - 1, 0, -1):
        for a in (1, 0):
            for first in order if d < lines - 1 or a == 0 else ():
                rs_step(a, 1, d, first)
                rs_step(a, 0, d, first)

    for e in range(1, reps):
        rep_copy(e).wait_recv()
    summed = rep_slots[0]
    for e in range(1, reps):
        summed = summed + rep_slots[e]
    bias_sums[0] = summed
    z_slots[z] = summed
    for e in range(1, lines):
        zb_copy(e).start()

    @pl.when(lead)
    def _():
        pl.semaphore_wait(gate, 1)
        for s in range(1, PLANE):
            dq_copy(s).start()

    def finish(a, first):
        block = range(first, first + PAIR)
        for s in block:
            owns[a][s] = (owns[a][s] + chains[a][last_ref[z * PLANE + near(s)]]) * factors[a]
        for way in range(2):
            @pl.when(rs_inner(way))
            def _():
                rs_copy(a, way, 1, first).wait_recv()
                for s in block:
                    owns[a][s] += rs_recv[a, way, 0, s].astype(jnp.float32)

        for s in reversed(block):
            final[a, s] = owns[a][s].astype(jnp.bfloat16)
            if s:
                out_copy(a, s).start()
            else:
                out_stay(a).start()

    for s in order:
        finish(1, s)

    zb_all.wait_recv()
    summed = z_slots[0]
    for d in range(1, lines):
        summed = summed + z_slots[d]
    bias_sums[1] = summed

    def bias_rows(chip):
        return dbq_ref.at[pl.ds(pl.multiple_of(chip * group, group), group)]

    bias_stay = pltpu.make_async_copy(bias_sums.at[1], bias_rows(p), table_sem.at[0])
    bias_stay.start()

    def pb_copy(s):
        return remote(
            bias_sums.at[1], bias_rows(p), pb_sem.at[0], pb_sem.at[1], seq(z, near(s))
        )

    shares = bias_buf.at[pl.ds(0, (PLANE - 1) * group)]
    pb_all = remote(shares, shares, pb_sem.at[0], pb_sem.at[1], seq(z, p))
    for s in range(1, PLANE):
        pb_copy(s).start()

    for s in order:
        finish(0, s)

    for a in range(2):
        plane_sent(a).wait_send()
        for way in range(2):
            for d in range(1, lines):
                @pl.when(z + d < lines if way == 0 else z - d >= 0)
                def _():
                    sent(a, way, d - 1).wait_send()
    dq_stay.wait()
    dq_all.wait()
    for d in range(1, reps):
        rep_copy(d).wait_send()
    zb_all.wait_send()
    for a in range(2):
        out_stay(a).wait()
        out_all(a).wait()
    bias_stay.wait()
    pb_all.wait()


def fused(lists, counts, bias, q, g, k, v):
    n, reps = lax.axis_size("seq"), lax.axis_size("rep")
    rows, total = q.shape
    heads, width = bias.shape
    kv_count = k.shape[1] // width
    group = heads // kv_count
    assert reps % 2 == 0 and n % PLANE == 0 and kv_count == PLANE and group % 2 == 0
    lines = n // PLANE
    pairs = PLANE * group
    half, full = jnp.bfloat16, jnp.float32
    free = pl.BlockSpec(memory_space=pl.ANY)
    dma = pltpu.SemaphoreType.DMA
    block = rows * width
    need = 2 * block * (2 * n + 3 * pairs + 32 * (lines - 1) + 8 + 2 * kv_count)
    need += 4 * block * (2 * pairs + 2 * (pairs + 1) + 2 * PLANE)
    need += 8 * heads * width * (reps + lines)
    return pl.pallas_call(
        functools.partial(fused_kernel, group, width ** (-0.5)),
        in_specs=[pl.BlockSpec(memory_space=pltpu.HBM)] * 7,
        out_specs=[free] * 4,
        out_shape=[
            jax.ShapeDtypeStruct(q.shape, half),
            jax.ShapeDtypeStruct(k.shape, half),
            jax.ShapeDtypeStruct(v.shape, half),
            jax.ShapeDtypeStruct(bias.shape, full),
        ],
        scratch_shapes=[
            pltpu.SMEM(lists.shape, lists.dtype),
            pltpu.SMEM(counts.shape, counts.dtype),
            pltpu.VMEM(bias.shape, full),
            pltpu.VMEM(k.shape, half),
            pltpu.VMEM(v.shape, half),
            pltpu.VMEM((n, rows, width), half),
            pltpu.VMEM((n, rows, width), half),
            pltpu.VMEM((PLANE, rows, group * width), half),
            pltpu.VMEM((PLANE, rows, group * width), half),
            pltpu.VMEM((PLANE, rows, group * width), half),
            pltpu.VMEM((pairs, 2 * rows, rows), full),
            pltpu.VMEM((pairs + 1, rows, width), full),
            pltpu.VMEM((pairs + 1, rows, width), full),
            pltpu.VMEM((PLANE, rows, width), full),
            pltpu.VMEM((PLANE, rows, width), full),
            pltpu.VMEM((2, 2, lines - 1, PLANE, rows, width), half),
            pltpu.VMEM((2, 2, lines - 1, PLANE, rows, width), half),
            pltpu.VMEM((2, PLANE, rows, width), half),
            pltpu.VMEM((group, width), full),
            pltpu.VMEM((reps, group, width), full),
            pltpu.VMEM((lines, group, width), full),
            pltpu.VMEM((2, group, width), full),
            pltpu.SMEM((pairs,), jnp.int32),
            pltpu.SMEM((pairs,), jnp.int32),
            pltpu.SMEM((n,), jnp.int32),
            dma((3,)), dma((6,)),
            dma((2,)), dma((2, PLANE - 1)),
            dma((3,)), dma((2, PLANE)),
            dma((2, 2, lines - 1)), dma((2, 2, (lines - 2) * PLANE + 1)),
            pltpu.SemaphoreType.REGULAR,
            dma((2, 2, lines - 1, PLANE // PAIR)), dma((3,)), dma((3, 2)),
            dma((reps - 1,)), dma((reps - 1,)),
            dma((2,)), dma((2,)),
        ],
        compiler_params=pltpu.CompilerParams(
            collective_id=1, has_side_effects=True, vmem_limit_bytes=need + 4 * 2**20
        ),
        name="fused",
    )(lists, counts, bias, q, g, k, v)


def place_kernel(*refs):
    count = len(refs) // 2
    sem = refs[-1]
    copies = [
        pltpu.make_async_copy(refs[a], refs[count + a], sem.at[a]) for a in range(count)
    ]
    for copy in copies:
        copy.start()
    for copy in copies:
        copy.wait()


def place(*arrays):
    spec = pl.BlockSpec(memory_space=pl.ANY)
    return pl.pallas_call(
        place_kernel,
        in_specs=[spec] * len(arrays),
        out_specs=[spec] * len(arrays),
        out_shape=[jax.ShapeDtypeStruct(one.shape, one.dtype) for one in arrays],
        scratch_shapes=[pltpu.SemaphoreType.DMA((len(arrays),))],
        compiler_params=pltpu.CompilerParams(vmem_limit_bytes=2**20),
        name="place",
    )(*arrays)


def body(q_lin, k_lin, value_projection, grad_out, q_bias, block_lists, block_counts):
    assert block_lists.shape[1] == lax.axis_size("seq") and block_lists.shape[2] == 2
    heads = block_lists.shape[0]
    args = (jnp.transpose(block_lists, (1, 2, 0)), block_counts.T, q_bias.reshape(heads, -1),
        q_lin[0], grad_out[0], k_lin[0], value_projection[0])
    args = [pltpu.with_memory_space_constraint(a, pltpu.HBM) for a in args]
    dq, dk, dv, dbq = fused(*args)
    dq, dk, dv, dbq = place(dq, dk, dv, dbq)
    return (dq[None], dk[None], dv[None], dbq.reshape(-1))


def solution(mesh):
    placed = (P("rep", "seq", None),) * 4 + (P(),) * 3
    return jax.shard_map(
        body,
        mesh=mesh,
        in_specs=placed,
        out_specs=(P("rep", "seq", None),) * 3 + (P(),),
        check_vma=False,
    )
```

```python
import functools

import jax
import jax.numpy as jnp
from jax import lax
from jax.experimental import pallas as pl
from jax.experimental.pallas import tpu as pltpu
from jax.sharding import PartitionSpec as P

NT = (((1,), (1,)), ((), ()))
TN = (((0,), (0,)), ((), ()))
NN = (((1,), (0,)), ((), ()))
MESH = pl.DeviceIdType.MESH
PLANE = 4
PAIR = 2


def dot(a, b, dims):
    return lax.dot_general(a, b, dims, preferred_element_type=jnp.float32)


def fused_kernel(
    group, scaling,
    lists_ref, count_ref, bias_ref, q_ref, g_ref, k_ref, v_ref,
    dq_ref, dk_ref, dv_ref, dbq_ref,
    lists_smem, count_smem, bias_buf,
    kbuf, vbuf, kall, vall, qbuf, gbuf, dqbuf, weights_buf, chain_k, chain_v, own_k, own_v,
    rs_send, rs_recv, final, bias_acc, rep_slots, z_slots, bias_sums,
    enc_ref, prev_ref, last_ref,
    table_sem, local_sem, plane_send, plane_recv, rows_send, rows_recv, z_send, z_recv,
    gate, rs_sem, dq_sem, out_sem, rep_send, rep_recv, zb_sem, pb_sem,
):
    me = lax.axis_index("seq")
    n = lax.axis_size("seq")
    reps, rep = lax.axis_size("rep"), lax.axis_index("rep")
    lines = n // PLANE
    z, p = me // PLANE, me % PLANE
    rows, width = kall.shape[1:]
    pairs = PLANE * group

    def near(s):
        return (p // 2 + s // 2) % 2 * 2 + (p % 2 + s % 2) % 2

    def seq(zz, pp):
        return {"seq": zz * PLANE + pp}

    def remote(src, dst, send, recv, target):
        return pltpu.make_async_remote_copy(
            src_ref=src, dst_ref=dst, send_sem=send, recv_sem=recv,
            device_id=target, device_id_type=MESH,
        )

    def cols(start, size):
        return pl.ds(pl.multiple_of(start * width, width), size * width)

    barrier = pltpu.get_barrier_semaphore()
    z_others = [lax.rem(z + d, lines) for d in range(1, lines)]
    rep_others = [lax.rem(rep + d, reps) for d in range(1, reps)]
    for s in range(1, PLANE):
        pl.semaphore_signal(barrier, inc=1, device_id=seq(z, near(s)), device_id_type=MESH)
    for zz in z_others:
        pl.semaphore_signal(barrier, inc=1, device_id=seq(zz, p), device_id_type=MESH)
    for rr in rep_others:
        pl.semaphore_signal(barrier, inc=1, device_id={"rep": rr}, device_id_type=MESH)
    own_kv = [
        pltpu.make_async_copy(src.at[:, cols(p, 1)], dst.at[me], local_sem.at[a])
        for a, (src, dst) in enumerate([(k_ref, kall), (v_ref, vall)])
    ]
    own_rows = [
        pltpu.make_async_copy(src.at[:, cols(p * group, group)], dst.at[0], local_sem.at[2 + a])
        for a, (src, dst) in enumerate([(q_ref, qbuf), (g_ref, gbuf)])
    ]
    tables = [
        pltpu.make_async_copy(lists_ref, lists_smem, table_sem.at[0]),
        pltpu.make_async_copy(count_ref, count_smem, table_sem.at[1]),
    ]
    bias_copy = pltpu.make_async_copy(bias_ref, bias_buf, table_sem.at[2])
    ahead = [
        pltpu.make_async_copy(src, dst, local_sem.at[4 + a])
        for a, (src, dst) in enumerate([(k_ref, kbuf), (v_ref, vbuf)])
    ]
    for copy in ahead + own_kv + tables + own_rows + [bias_copy]:
        copy.start()

    pl.semaphore_wait(barrier, PLANE - 1 + lines - 1 + reps - 1)

    def plane_copy(a, s):
        src, dst = [(kbuf, kall), (vbuf, vall)][a]
        return remote(
            src.at[:, cols(near(s), 1)], dst.at[me],
            plane_send.at[a], plane_recv.at[a, s - 1], seq(z, near(s)),
        )

    def plane_sent(a):
        blocks = [kall, vall][a].at[pl.ds(0, PLANE - 1)]
        return remote(blocks, blocks, plane_send.at[a], plane_recv.at[a, 0], seq(z, p))

    lead = rep % 2 == 0
    follow = rep % 2 == 1

    def tell_partner():
        pl.semaphore_signal(
            gate, inc=1, device_id={"rep": rep // 2 * 2 + 1 - rep % 2}, device_id_type=MESH
        )

    for copy in ahead:
        copy.wait()

    def plane_start():
        for a in range(2):
            for s in range(1, PLANE):
                plane_copy(a, s).start()

    pl.when(lead)(plane_start)

    def rows_copy(a, s, first=0, count=group):
        src, dst = [(q_ref, qbuf), (g_ref, gbuf)][a]
        which = s - 1 if first == 0 else PLANE - 1
        return remote(
            src.at[:, cols(near(s) * group + first, count)],
            dst.at[s, :, first * width : (first + count) * width],
            rows_send.at[a if s < PLANE - 1 or a == 0 else 2], rows_recv.at[a, which],
            seq(z, near(s)),
        )

    def rows_sent(which):
        block = [
            qbuf.at[pl.ds(1, PLANE - 1)], gbuf.at[pl.ds(1, PLANE - 2)], gbuf.at[PLANE - 1]
        ][which]
        remote(block, block, rows_send.at[which], rows_recv.at[0, 0], seq(z, p)).wait_send()

    half_group = group * 3 // 4
    last_rows = [(0, half_group), (half_group, group - half_group)]
    def rows_start():
        for s in range(1, PLANE - 1):
            rows_copy(0, s).start()
        for s in range(1, PLANE - 1):
            rows_copy(1, s).start()
        rows_copy(0, PLANE - 1).start()
        for first, count in last_rows:
            rows_copy(1, PLANE - 1, first, count).start()

    def z_block(a, place, s):
        return [kall, vall][a].at[place * PLANE + near(s)]

    def z_slot(d, s):
        return d * PLANE + (s if d < lines - 2 else 0)

    def z_copy(a, way, d, s):
        block = z_block(a, z - d if way == 0 else z + d, s)
        return remote(
            block, block, z_send.at[a, way, d], z_recv.at[a, way, z_slot(d, s)],
            seq(z + 1 if way == 0 else z - 1, p),
        )

    def goes(way, d):
        if way == 0:
            return (z + 1 < lines) & (z - d >= 0)
        return (z - 1 >= 0) & (z + d < lines)

    def z_start(a, d, s):
        for way in range(2):
            @pl.when(goes(way, d))
            def _():
                z_copy(a, way, d, s).start()

    def z_relay(a, d):
        if d == lines - 1:
            for way in range(2):
                @pl.when(z - d >= 0 if way == 0 else z + d < lines)
                def _():
                    where = z - d if way == 0 else z + d
                    shard = [kall, vall][a].at[pl.ds(where * PLANE, PLANE)]
                    remote(
                        shard, shard, z_send.at[a, way, d - 1], z_recv.at[a, way, z_slot(d - 1, 0)],
                        seq(z, p),
                    ).wait_recv()

            return
        for s in range(PLANE):
            for way in range(2):
                @pl.when(z - d >= 0 if way == 0 else z + d < lines)
                def _():
                    block = z_block(a, z - d if way == 0 else z + d, s)
                    remote(
                        block, block, z_send.at[a, way, d - 1], z_recv.at[a, way, z_slot(d - 1, s)],
                        seq(z, p),
                    ).wait_recv()

            z_start(a, d, s)

    def z_own(a, s, who, which=None):
        for way in range(2):
            wanted = goes(way, 0) & who
            if which is not None:
                wanted = wanted & (goes(way, 1) if which else jnp.logical_not(goes(way, 1)))

            @pl.when(wanted)
            def _():
                z_copy(a, way, 0, s).start()

    own_kv[0].wait()
    z_own(0, 0, lead)

    for copy in tables:
        copy.wait()

    def read_table(t, _):
        position = z * PLANE + near(t // group)
        head = p * group + t % group
        other = jnp.clip(lists_smem[position, 1, head], 0, n - 1)
        enc_ref[t] = jnp.where(count_smem[position, head] != 1, other, n)
        return 0

    lax.fori_loop(0, pairs, read_table, 0)
    pl.when(lead)(rows_start)

    def link_pair(t, _):
        code = enc_ref[t]
        found = jnp.int32(0)
        for u in range(pairs):
            same = (enc_ref[u] == code) & (u < t)
            found = jnp.where(same, u + 1, found)
        prev_ref[t] = found
        return 0

    def link_block(j, _):
        found = jnp.int32(0)
        for u in range(pairs):
            found = jnp.where(enc_ref[u] == j, u + 1, found)
        last_ref[j] = found
        return 0

    lax.fori_loop(0, pairs, link_pair, 0)
    pl.when(follow)(plane_start)
    for s in range(1, PLANE):
        plane_copy(0, s).wait_recv()
        z_own(0, s, lead)
    own_kv[1].wait()
    for s in range(PLANE):
        if s:
            plane_copy(1, s).wait_recv()
        z_own(1, s, lead)
    lax.fori_loop(0, n, link_block, 0)
    chain_k[0] = jnp.zeros((rows, width), jnp.float32)
    chain_v[0] = jnp.zeros((rows, width), jnp.float32)
    own_k[...] = jnp.zeros_like(own_k)
    own_v[...] = jnp.zeros_like(own_v)
    bias_acc[...] = jnp.zeros_like(bias_acc)

    @pl.when(follow)
    def _():
        pl.semaphore_wait(gate, 1)
        rows_start()
        pl.semaphore_wait(gate, 1)

    for s in range(PLANE):
        z_own(0, s, follow)
    for s in range(PLANE):
        z_own(1, s, follow, False)
    for d in range(1, lines):
        if d == lines - 1:
            @pl.when(lead)
            def _():
                rows_sent(0)
                rows_sent(1)
                tell_partner()

        z_relay(0, d)
        if d == 1:
            for s in range(PLANE):
                z_own(1, s, follow, True)
        elif d < lines - 1:
            z_relay(1, d - 1)

    for copy in own_rows:
        copy.wait()
    bias_copy.wait()

    def both(ref, s, t):
        code = enc_ref[t]
        other = jnp.where(code < n, code, 0)
        return jnp.concatenate([ref[z * PLANE + near(s)], ref[other]], axis=0), code

    def lanes_of(h):
        return slice(h * width, (h + 1) * width)

    def soften(s):
        for h in range(group):
            t, lanes = s * group + h, lanes_of(h)
            queries = (
                qbuf[s, :, lanes].astype(jnp.float32) + bias_buf[pl.ds(p * group + h, 1), :]
            ).astype(jnp.bfloat16)
            qbuf[s, :, lanes] = queries
            keys, code = both(kall, s, t)
            scores = dot(keys, queries, NT) * scaling
            first = scores[:rows]
            second = scores[rows:] + jnp.where(code < n, 0.0, -1.0e30)
            top = jnp.maximum(
                jnp.max(first, axis=0, keepdims=True), jnp.max(second, axis=0, keepdims=True)
            )
            first, second = jnp.exp(first - top), jnp.exp(second - top)
            total = jnp.sum(first, axis=0, keepdims=True) + jnp.sum(second, axis=0, keepdims=True)
            scale_to = 1.0 / total
            weights_buf[t, :rows] = first * scale_to
            weights_buf[t, rows:] = second * scale_to

    def dq_copy(s):
        return remote(
            dqbuf.at[s], dq_ref.at[:, cols(p * group, group)],
            dq_sem.at[0], dq_sem.at[1], seq(z, near(s)),
        )

    dq_stay = pltpu.make_async_copy(dqbuf.at[0], dq_ref.at[:, cols(p * group, group)], dq_sem.at[2])
    others = dqbuf.at[pl.ds(1, PLANE - 1)]
    dq_all = remote(others, others, dq_sem.at[0], dq_sem.at[1], seq(z, p))

    def grad_values(s, heads):
        more_v = None
        for h in heads:
            t = s * group + h
            part_v = dot(weights_buf[t].astype(jnp.bfloat16), gbuf[s, :, lanes_of(h)], NN)
            chain_v[t + 1] = part_v[rows:] + chain_v[prev_ref[t]]
            more_v = part_v[:rows] if more_v is None else more_v + part_v[:rows]
        own_v[s] += more_v

    def grad_keys(s, heads):
        more_k = None
        held = []
        for h in heads:
            values, _ = both(vall, s, s * group + h)
            held.append(dot(values, gbuf[s, :, lanes_of(h)], NT))
        for h, weight_grads in zip(heads, held):
            t, lanes = s * group + h, lanes_of(h)
            keys, _ = both(kall, s, t)
            weights = weights_buf[t]
            half = weights.astype(jnp.bfloat16)
            row_dots = jnp.sum(half.astype(jnp.float32) * weight_grads, axis=0, keepdims=True)
            score_grads = (weights * (weight_grads - row_dots)).astype(jnp.bfloat16)
            grad_q = scaling * dot(score_grads, keys, TN)
            dqbuf[s, :, lanes] = grad_q.astype(jnp.bfloat16)
            bias_acc[h : h + 1, :] += jnp.sum(grad_q, axis=0, keepdims=True)
            part_k = dot(score_grads, qbuf[s, :, lanes], NN)
            chain_k[t + 1] = part_k[rows:] + chain_k[prev_ref[t]]
            more_k = part_k[:rows] if more_k is None else more_k + part_k[:rows]
        own_k[s] += more_k

    every = list(range(group))
    early = []
    for s in range(PLANE - 1):
        early.append((0, s))
        early.append((1, s))
    early.append((0, PLANE - 1))

    def run(kind, s):
        if s:
            rows_copy(kind, s).wait_recv()
        if kind == 0:
            soften(s)
        else:
            grad_values(s, every)

    pl.when(lead)(tell_partner)
    for kind, s in early[:2]:
        run(kind, s)
    z_relay(1, lines - 2)
    for kind, s in early[2:5]:
        run(kind, s)
    z_relay(1, lines - 1)

    def dq_start(s):
        @pl.when(follow)
        def _():
            dq_copy(s).start()

    for s in range(PLANE - 1):
        if s == PLANE - 2:
            run(*early[5])
        grad_keys(s, every)
        if s:
            dq_start(s)
        else:
            dq_stay.start()
    run(*early[6])
    def sent(a, way, d):
        blocks = [kall, vall][a].at[pl.ds(0, PLANE)]
        return remote(blocks, blocks, z_send.at[a, way, d], z_recv.at[a, way, 0], seq(z, p))

    for a in range(2):
        for way in range(2):
            for d in range(lines - 1):
                @pl.when(goes(way, d))
                def _():
                    sent(a, way, d).wait_send()

    factors = [scaling, 1.0]
    chains = [chain_k, chain_v]
    owns = [own_k, own_v]
    order = range(PLANE - PAIR, -1, -PAIR)

    def rs_copy(a, way, d, first):
        pair = pl.ds(first, PAIR)
        return remote(
            rs_send.at[a, way, d - 1, pair], rs_recv.at[a, way, d - 1, pair],
            z_send.at[a, way, d - 1], rs_sem.at[a, way, d - 1, first // PAIR],
            seq(z + 1 if way == 0 else z - 1, p),
        )

    def rs_inner(way):
        return z >= 1 if way == 0 else z + 1 < lines

    def rs_step(a, way, d, first):
        target = z + d if way == 0 else z - d
        inside = target < lines if way == 0 else target >= 0

        def part(s):
            return chains[a][last_ref[target * PLANE + near(s)]] * factors[a]

        if d < lines - 1:
            @pl.when(inside & rs_inner(way))
            def _():
                rs_copy(a, way, d + 1, first).wait_recv()
                for s in range(first, first + PAIR):
                    rs_send[a, way, d - 1, s] = (
                        part(s) + rs_recv[a, way, d, s].astype(jnp.float32)
                    ).astype(jnp.bfloat16)
                rs_copy(a, way, d, first).start()

            inside = inside & jnp.logical_not(rs_inner(way))

        @pl.when(inside)
        def _():
            for s in range(first, first + PAIR):
                rs_send[a, way, d - 1, s] = part(s).astype(jnp.bfloat16)
            rs_copy(a, way, d, first).start()

    for part, (first, count) in enumerate(last_rows):
        heads = range(first, first + count)
        rows_copy(1, PLANE - 1, first, count).wait_recv()
        if part == len(last_rows) - 1:
            @pl.when(follow)
            def _():
                for which in range(3):
                    rows_sent(which)
                tell_partner()

        grad_values(PLANE - 1, heads)
        if part == len(last_rows) - 1:
            for block in order:
                for way in range(2):
                    rs_step(1, way, lines - 1, block)
        grad_keys(PLANE - 1, heads)
    dq_start(PLANE - 1)
    pl.when(lead)(functools.partial(rows_sent, 2))

    rep_slots[rep] = bias_acc[...]

    def rep_copy(d):
        return remote(
            bias_acc, rep_slots.at[rep], rep_send.at[d - 1], rep_recv.at[d - 1],
            {"rep": rep_others[d - 1]},
        )

    for d in range(1, reps):
        rep_copy(d).start()

    def out_copy(a, s):
        return remote(
            final.at[a, s], [dk_ref, dv_ref][a].at[:, cols(p, 1)],
            out_sem.at[0, a], out_sem.at[1, a], seq(z, near(s)),
        )

    def out_all(a):
        blocks = final.at[a, pl.ds(1, PLANE - 1)]
        return remote(blocks, blocks, out_sem.at[0, a], out_sem.at[1, a], seq(z, p))

    def out_stay(a):
        return pltpu.make_async_copy(
            final.at[a, 0], [dk_ref, dv_ref][a].at[:, cols(p, 1)], out_sem.at[2, a]
        )

    def zb_copy(d):
        return remote(
            bias_sums.at[0], z_slots.at[z], zb_sem.at[0], zb_sem.at[1],
            seq(z_others[d - 1], p),
        )

    slots = z_slots.at[pl.ds(0, lines - 1)]
    zb_all = remote(slots, slots, zb_sem.at[0], zb_sem.at[1], seq(z, p))

    for d in range(lines - 1, 0, -1):
        for a in (1, 0):
            for first in order if d < lines - 1 or a == 0 else ():
                rs_step(a, 1, d, first)
                rs_step(a, 0, d, first)

    for e in range(1, reps):
        rep_copy(e).wait_recv()
    summed = rep_slots[0]
    for e in range(1, reps):
        summed = summed + rep_slots[e]
    bias_sums[0] = summed
    z_slots[z] = summed
    for e in range(1, lines):
        zb_copy(e).start()

    @pl.when(lead)
    def _():
        pl.semaphore_wait(gate, 1)
        for s in range(1, PLANE):
            dq_copy(s).start()

    def finish(a, first):
        block = range(first, first + PAIR)
        for s in block:
            owns[a][s] = (owns[a][s] + chains[a][last_ref[z * PLANE + near(s)]]) * factors[a]
        for way in range(2):
            @pl.when(rs_inner(way))
            def _():
                rs_copy(a, way, 1, first).wait_recv()
                for s in block:
                    owns[a][s] += rs_recv[a, way, 0, s].astype(jnp.float32)

        for s in reversed(block):
            final[a, s] = owns[a][s].astype(jnp.bfloat16)
            if s:
                out_copy(a, s).start()
            else:
                out_stay(a).start()

    for s in order:
        finish(1, s)

    zb_all.wait_recv()
    summed = z_slots[0]
    for d in range(1, lines):
        summed = summed + z_slots[d]
    bias_sums[1] = summed

    def bias_rows(chip):
        return dbq_ref.at[pl.ds(pl.multiple_of(chip * group, group), group)]

    bias_stay = pltpu.make_async_copy(bias_sums.at[1], bias_rows(p), table_sem.at[0])
    bias_stay.start()

    def pb_copy(s):
        return remote(
            bias_sums.at[1], bias_rows(p), pb_sem.at[0], pb_sem.at[1], seq(z, near(s))
        )

    shares = bias_buf.at[pl.ds(0, (PLANE - 1) * group)]
    pb_all = remote(shares, shares, pb_sem.at[0], pb_sem.at[1], seq(z, p))
    for s in range(1, PLANE):
        pb_copy(s).start()

    for s in order:
        finish(0, s)

    for a in range(2):
        plane_sent(a).wait_send()
        for way in range(2):
            for d in range(1, lines):
                @pl.when(z + d < lines if way == 0 else z - d >= 0)
                def _():
                    sent(a, way, d - 1).wait_send()
    dq_stay.wait()
    dq_all.wait()
    for d in range(1, reps):
        rep_copy(d).wait_send()
    zb_all.wait_send()
    for a in range(2):
        out_stay(a).wait()
        out_all(a).wait()
    bias_stay.wait()
    pb_all.wait()


def fused(lists, counts, bias, q, g, k, v):
    n, reps = lax.axis_size("seq"), lax.axis_size("rep")
    rows, total = q.shape
    heads, width = bias.shape
    kv_count = k.shape[1] // width
    group = heads // kv_count
    assert reps % 2 == 0 and n % PLANE == 0 and kv_count == PLANE and group % 4 == 0
    lines = n // PLANE
    pairs = PLANE * group
    half, full = jnp.bfloat16, jnp.float32
    free = pl.BlockSpec(memory_space=pl.ANY)
    dma = pltpu.SemaphoreType.DMA
    block = rows * width
    need = 2 * block * (2 * n + 3 * pairs + 32 * (lines - 1) + 8 + 2 * kv_count)
    need += 4 * block * (2 * pairs + 2 * (pairs + 1) + 2 * PLANE)
    need += 8 * heads * width * (reps + lines)
    return pl.pallas_call(
        functools.partial(fused_kernel, group, width ** (-0.5)),
        in_specs=[pl.BlockSpec(memory_space=pltpu.HBM)] * 7,
        out_specs=[free] * 4,
        out_shape=[
            jax.ShapeDtypeStruct(q.shape, half),
            jax.ShapeDtypeStruct(k.shape, half),
            jax.ShapeDtypeStruct(v.shape, half),
            jax.ShapeDtypeStruct(bias.shape, full),
        ],
        scratch_shapes=[
            pltpu.SMEM(lists.shape, lists.dtype),
            pltpu.SMEM(counts.shape, counts.dtype),
            pltpu.VMEM(bias.shape, full),
            pltpu.VMEM(k.shape, half),
            pltpu.VMEM(v.shape, half),
            pltpu.VMEM((n, rows, width), half),
            pltpu.VMEM((n, rows, width), half),
            pltpu.VMEM((PLANE, rows, group * width), half),
            pltpu.VMEM((PLANE, rows, group * width), half),
            pltpu.VMEM((PLANE, rows, group * width), half),
            pltpu.VMEM((pairs, 2 * rows, rows), full),
            pltpu.VMEM((pairs + 1, rows, width), full),
            pltpu.VMEM((pairs + 1, rows, width), full),
            pltpu.VMEM((PLANE, rows, width), full),
            pltpu.VMEM((PLANE, rows, width), full),
            pltpu.VMEM((2, 2, lines - 1, PLANE, rows, width), half),
            pltpu.VMEM((2, 2, lines - 1, PLANE, rows, width), half),
            pltpu.VMEM((2, PLANE, rows, width), half),
            pltpu.VMEM((group, width), full),
            pltpu.VMEM((reps, group, width), full),
            pltpu.VMEM((lines, group, width), full),
            pltpu.VMEM((2, group, width), full),
            pltpu.SMEM((pairs,), jnp.int32),
            pltpu.SMEM((pairs,), jnp.int32),
            pltpu.SMEM((n,), jnp.int32),
            dma((3,)), dma((6,)),
            dma((2,)), dma((2, PLANE - 1)),
            dma((3,)), dma((2, PLANE)),
            dma((2, 2, lines - 1)), dma((2, 2, (lines - 2) * PLANE + 1)),
            pltpu.SemaphoreType.REGULAR,
            dma((2, 2, lines - 1, PLANE // PAIR)), dma((3,)), dma((3, 2)),
            dma((reps - 1,)), dma((reps - 1,)),
            dma((2,)), dma((2,)),
        ],
        compiler_params=pltpu.CompilerParams(
            collective_id=1, has_side_effects=True, vmem_limit_bytes=need + 4 * 2**20
        ),
        name="fused",
    )(lists, counts, bias, q, g, k, v)


def place_kernel(*refs):
    count = len(refs) // 2
    sem = refs[-1]
    copies = [
        pltpu.make_async_copy(refs[a], refs[count + a], sem.at[a]) for a in range(count)
    ]
    for copy in copies:
        copy.start()
    for copy in copies:
        copy.wait()


def place(*arrays):
    spec = pl.BlockSpec(memory_space=pl.ANY)
    return pl.pallas_call(
        place_kernel,
        in_specs=[spec] * len(arrays),
        out_specs=[spec] * len(arrays),
        out_shape=[jax.ShapeDtypeStruct(one.shape, one.dtype) for one in arrays],
        scratch_shapes=[pltpu.SemaphoreType.DMA((len(arrays),))],
        compiler_params=pltpu.CompilerParams(vmem_limit_bytes=2**20),
        name="place",
    )(*arrays)


def body(q_lin, k_lin, value_projection, grad_out, q_bias, block_lists, block_counts):
    assert block_lists.shape[1] == lax.axis_size("seq") and block_lists.shape[2] == 2
    heads = block_lists.shape[0]
    args = (jnp.transpose(block_lists, (1, 2, 0)), block_counts.T, q_bias.reshape(heads, -1),
        q_lin[0], grad_out[0], k_lin[0], value_projection[0])
    args = [pltpu.with_memory_space_constraint(a, pltpu.HBM) for a in args]
    dq, dk, dv, dbq = fused(*args)
    dq, dk, dv, dbq = place(dq, dk, dv, dbq)
    return (dq[None], dk[None], dv[None], dbq.reshape(-1))


def solution(mesh):
    placed = (P("rep", "seq", None),) * 4 + (P(),) * 3
    return jax.shard_map(
        body,
        mesh=mesh,
        in_specs=placed,
        out_specs=(P("rep", "seq", None),) * 3 + (P(),),
        check_vma=False,
    )
```
